32 devices in a mesh: slab: 8 (over y, x, core), probe: 4 (over z).
Axes of the slice: x: 2, y: 2, z: 4, core: 2. Of those that a mesh axis runs over, the one named last changes fastest.
Arguments:
- probe_fields: bfloat16 [256, 32, 8192], P('probe', 'slab'), may hold values from -6 to 6
- sensor_rows: int32 [4096], replicated, may hold values from 0 to 30, as said below
- sensor_cols: int32 [4096], replicated, may hold values from 0 to 8190
- row_frac: float32 [4096], replicated, may hold values from 0 to 1
- col_frac: float32 [4096], replicated, may hold values from 0 to 1
- sensor_weights: float32 [4096], replicated, may hold values from 0.05 to 1
- owner_order: int32 [4096], replicated, may hold values from 0 to 4095, as said below
Outputs:
- adjoint_sources: bfloat16 [256, 32, 8192], P('probe', 'slab')
- observed: float32 [256, 4096], P('probe', 'slab')
- trace_mean: float32 [], replicated
The draws below stay inside these ranges and needn't reach their ends.
Inputs may be any that keep to these rules, and one draw needn't show every extreme that they name: `sensor_rows`: rows run from 0 to 30. The sensors whose row lies in one slab of 4 rows number at most 2048, and some slab holds exactly 2048. `owner_order`: A permutation. The 4096 // 8 slots of one owner name at most 256 sensors whose row lies in any one slab, and every owner reaches 256 for some slab.
All inputs are finite; a program needn't handle non-finite values.
Results may differ from the reference program's by a relative error of at most 0.0068.
Values sent between devices are 32-bit elements; how exact they have to be, the bound alone decides.
A program may use at most 64 MiB of HBM per device.

```python
import math
import jax
import jax.numpy as jnp
from jax import lax

ROWS_DEV = 4
NCOL = 8192
SENSORS = 4096
NX = 32
PROBES = 256


def sensor_layout(key):
    slab_total = NX // ROWS_DEV
    slab_most = 4 * SENSORS // slab_total
    own_count = SENSORS // slab_total
    busiest = jax.random.randint(jax.random.fold_in(key, 11), (), 0, slab_total)
    position = jnp.arange(SENSORS, dtype=jnp.int32)
    others = (position - slab_most) % (slab_total - 1)
    others = others + (others >= busiest).astype(jnp.int32)
    slab_seq = jnp.sort(jnp.where(position < slab_most, busiest, others))
    row_inside = jax.random.randint(jax.random.fold_in(key, 12), (SENSORS,), 0, ROWS_DEV)
    row_inside = jnp.where((slab_seq == slab_total - 1) & (row_inside == ROWS_DEV - 1), row_inside - 1, row_inside)
    rows_seq = (slab_seq * ROWS_DEV + row_inside).astype(jnp.int32)
    sensor_ids = jax.random.permutation(jax.random.fold_in(key, 13), SENSORS).astype(jnp.int32)
    sensor_rows = jnp.zeros((SENSORS,), jnp.int32).at[sensor_ids].set(rows_seq)
    owner_perm = jax.random.permutation(jax.random.fold_in(key, 14), slab_total).astype(jnp.int32)
    shuffle = jax.random.permutation(jax.random.fold_in(key, 15), own_count).astype(jnp.int32)
    rotate = jax.random.randint(jax.random.fold_in(key, 16), (slab_total,), 0, own_count)
    owner_of = owner_perm[position % slab_total]
    inside = (shuffle[position // slab_total] + rotate[owner_of]) % own_count
    slot_of = (owner_of * own_count + inside).astype(jnp.int32)
    owner_order = jnp.zeros((SENSORS,), jnp.int32).at[slot_of].set(sensor_ids)
    return (sensor_rows, owner_order)


def draw_sensor_rows(key, part):
    return sensor_layout(key)[0]


def draw_owner_order(key, part):
    return sensor_layout(key)[1]


def with_ends(result, key, low, top_value):
    longest = result.shape.index(max(result.shape))
    spots = []
    for shift in (0, 1):
        where = [jax.random.randint(jax.random.fold_in(key, axis), (), 0, length) for axis, length in enumerate(result.shape)]
        where[longest] = (where[longest] + shift) % result.shape[longest]
        spots.append(tuple(where))
    return result.at[spots[0]].set(low).at[spots[1]].set(top_value)


def block_levels(rng, dims, split, least, high):
    def one(dim, shards_of):
        steps = jax.random.uniform(jax.random.fold_in(jax.random.fold_in(rng, 6), dim), (shards_of,), jnp.float32, least / len(split), high / len(split))
        return jnp.repeat(jnp.exp(steps), dims[dim] // shards_of).reshape((-1,) + (1,) * (len(dims) - dim - 1))

    loudness = one(*split[0])
    for cut in split[1:]:
        loudness = loudness * one(*cut)
    return loudness


def bell_draw(rng, extent, scale, most, pieces=(), kind=jnp.bfloat16):
    level = block_levels(rng, extent, pieces, -0.22, 0.18) if pieces else 1.0
    entries = jax.random.normal(rng, extent, jnp.float32) * scale * level
    return jnp.minimum(jnp.maximum(entries, -most), most).astype(kind)


def setup_inputs(seed: int = 0) -> dict:
    keys = jax.random.split(jax.random.key(seed), 8)
    return {
        "probe_fields": bell_draw(keys[0], (PROBES, NX, NCOL), 1.0, 6.0, ((0, 4), (1, 8))),
        "sensor_rows": draw_sensor_rows(jax.random.fold_in(keys[7], 71), 0),
        "sensor_cols": with_ends(jax.random.randint(keys[2], (SENSORS,), 0, NCOL - 1), jax.random.fold_in(keys[2], 1), 0, (NCOL - 1) - 1).astype(jnp.int32),
        "row_frac": jnp.clip(jax.random.uniform(keys[3], (SENSORS,), jnp.float32, 0.0, 1.0), 0.0, 1.0),
        "col_frac": jnp.clip(jax.random.uniform(keys[4], (SENSORS,), jnp.float32, 0.0, 1.0), 0.0, 1.0),
        "sensor_weights": jnp.clip(jnp.exp(jax.random.uniform(keys[5], (SENSORS,), jnp.float32, math.log(0.05), math.log(1.0))), 0.05, 1.0),
        "owner_order": draw_owner_order(jax.random.fold_in(keys[7], 71), 0),
    }


def reference(probe_fields, sensor_rows, sensor_cols, row_frac, col_frac, sensor_weights, owner_order):
    rlow = 1.0 - row_frac
    rhigh = row_frac
    clow = lax.optimization_barrier((1.0 - col_frac).astype(jnp.bfloat16)).astype(jnp.float32)
    chigh = lax.optimization_barrier(col_frac.astype(jnp.bfloat16)).astype(jnp.float32)
    rows_next = sensor_rows + 1
    cols_next = sensor_cols + 1

    def sample(field):
        field = field.astype(jnp.float32)
        top = clow * field[sensor_rows, sensor_cols] + chigh * field[sensor_rows, cols_next]
        bottom = clow * field[rows_next, sensor_cols] + chigh * field[rows_next, cols_next]
        return rlow * top + rhigh * bottom

    values = lax.map(sample, probe_fields)
    observed = values[:, owner_order]
    weights = sensor_weights[owner_order]
    spread = observed * weights[None, :]
    trace_mean = jnp.sum(spread * observed) / (PROBES * SENSORS)
    owned_rows = sensor_rows[owner_order]
    owned_cols = sensor_cols[owner_order]
    owned_low = rlow[owner_order]
    owned_high = rhigh[owner_order]
    clow_owned = clow[owner_order]
    chigh_owned = chigh[owner_order]

    def place(spread_row):
        lower = (spread_row * owned_low).astype(jnp.bfloat16).astype(jnp.float32)
        upper = (spread_row * owned_high).astype(jnp.bfloat16).astype(jnp.float32)
        grid = jnp.zeros((NX, NCOL), jnp.float32)
        grid = grid.at[owned_rows, owned_cols].add(lower * clow_owned)
        grid = grid.at[owned_rows, owned_cols + 1].add(lower * chigh_owned)
        grid = grid.at[owned_rows + 1, owned_cols].add(upper * clow_owned)
        grid = grid.at[owned_rows + 1, owned_cols + 1].add(upper * chigh_owned)
        return grid.astype(jnp.bfloat16)

    adjoint_sources = lax.map(place, spread)
    return adjoint_sources, observed, trace_mean
```

```python
import functools
import typing

import jax
import jax.numpy as jnp
from jax import lax
from jax.experimental import pallas as pl
from jax.experimental.pallas import tpu as pltpu
from jax.sharding import PartitionSpec as P

LANES = 128
BLOCK = 1024
HALF = 256
FIELDS = 11
F32 = jnp.float32
BF16 = jnp.bfloat16
NT = (((1,), (1,)), ((), ()))
VMEM = pltpu.VMEM
SMEM = pltpu.SMEM
LIMIT = pltpu.CompilerParams(vmem_limit_bytes=60 * 1024 * 1024)


def iota(shape, dim):
    return lax.broadcasted_iota(jnp.int32, shape, dim)


def nt_dot(a, b):
    return lax.dot_general(a, b, NT, preferred_element_type=F32)


def plan_kernel(rows, cap_chunks, blocks, slabs, pair_lines, me_ref, r_ref, c_ref, rf_ref, cf_ref, w_ref, order_ref, plan_ref, marks_ref, places_ref, peak_ref):
    lines = r_ref.shape[0]
    sensors = lines * LANES
    step = min(4, lines)
    me = me_ref[0]
    first = me * rows
    owned = lines * LANES // slabs
    keys_group = 2 * blocks
    keys = 3 * keys_group
    chunks = 3 * cap_chunks

    def wide(x, i):
        return jnp.concatenate([x[i + j : i + j + 1, :] for j in range(step)], axis=1)

    order = order_ref[...]
    slot = iota((lines, LANES), 0) * LANES + iota((lines, LANES), 1)
    found = jnp.zeros((2 * lines, LANES), F32)
    for i in range(0, lines, step):
        target = wide(order, i)
        mine = wide(slot, i)
        here = iota((lines, step * LANES), 0) == (target >> 7)
        stack = jnp.concatenate(
            [jnp.where(here, (mine >> 7).astype(F32), 0.0), jnp.where(here, (mine & 127).astype(F32), 0.0)], axis=0
        ).astype(BF16)
        place = jnp.where(iota((LANES, step * LANES), 0) == (target & 127), 1.0, 0.0).astype(BF16)
        found = found + nt_dot(stack, place)
    slot_hi = found[:lines, :]
    slot_lo = found[lines:, :]

    r = r_ref[...]
    c = c_ref[...]
    rel = r - first + 1
    valid = (rel >= 0) & (rel <= rows)
    group = jnp.where(rel == 0, 0, jnp.where(rel == rows, 2, 1))
    block = c // BLOCK
    inner = c - block * BLOCK
    half = c // HALF
    slot_of = (slot_hi * LANES + slot_lo).astype(jnp.int32)
    owner = slot_of // owned
    home = r // rows
    send_key = jnp.where(home == me, owner, -1)
    recv_key = jnp.where(owner == me, home, -1)
    edge = jnp.where(r - home * rows == rows - 1, home, -1)
    edges = jnp.zeros((slabs, LANES), F32)
    for i in range(lines):
        edges = edges + jnp.where(iota((slabs, LANES), 0) == edge[i : i + 1, :], 1.0, 0.0)
    peak_ref[0] = jnp.max(jnp.sum(edges, axis=1, keepdims=True)).astype(jnp.int32)
    key = group * keys_group + 2 * block + jnp.where(inner == BLOCK - 1, 1, 0)
    key = jnp.where(valid, key, -1)

    count = jnp.zeros((keys, 1), F32)
    for i in range(lines):
        count = count + jnp.sum(jnp.where(iota((keys, LANES), 0) == key[i : i + 1, :], 1.0, 0.0), axis=1, keepdims=True)
    big = jnp.floor(count * (1.0 / 64.0))
    small = count - 64.0 * big
    ka, kb = iota((keys, keys), 0), iota((keys, keys), 1)
    below = jnp.where((kb < ka) & (kb // keys_group == ka // keys_group), 1.0, 0.0).astype(BF16)
    start = 64.0 * jnp.dot(below, jnp.broadcast_to(big, (keys, LANES)).astype(BF16), preferred_element_type=F32)
    start = start + jnp.dot(below, jnp.broadcast_to(small, (keys, LANES)).astype(BF16), preferred_element_type=F32)
    start = start + ((iota((keys, LANES), 0) // keys_group) * (cap_chunks * LANES)).astype(F32)
    wide_keys = marks_ref.shape[1]
    diagonal = iota((keys, wide_keys), 0) == iota((keys, wide_keys), 1)
    marks_ref[...] = jnp.concatenate(
        [jnp.sum(jnp.where(diagonal, x, 0.0), axis=0, keepdims=True) for x in (start[:, :1], start[:, :1] + count)], axis=0
    ).astype(jnp.int32)

    upper = jnp.where(iota((LANES, LANES), 0) < iota((LANES, LANES), 1), 1.0, 0.0).astype(BF16)
    carry = jnp.concatenate([start[:, :1], jnp.zeros((2 * slabs, 1), F32)], axis=0)
    spots, sends, recvs = [], [], []
    for i in range(lines):
        hot = jnp.concatenate(
            [
                jnp.where(iota((keys, LANES), 0) == key[i : i + 1, :], 1.0, 0.0),
                jnp.where(iota((slabs, LANES), 0) == send_key[i : i + 1, :], 1.0, 0.0),
                jnp.where(iota((slabs, LANES), 0) == recv_key[i : i + 1, :], 1.0, 0.0),
            ],
            axis=0,
        )
        before = jnp.dot(hot.astype(BF16), upper, preferred_element_type=F32)
        ranks = hot * (before + carry)
        spots.append(jnp.sum(ranks[:keys], axis=0, keepdims=True))
        sends.append(jnp.sum(ranks[keys : keys + slabs], axis=0, keepdims=True))
        recvs.append(jnp.sum(ranks[keys + slabs :], axis=0, keepdims=True))
        carry = carry + jnp.sum(hot, axis=1, keepdims=True)
    spot = jnp.concatenate(spots, axis=0).astype(jnp.int32)
    spot = jnp.where(valid, spot, -1)
    send = jnp.concatenate(sends, axis=0).astype(jnp.int32)
    recv = jnp.concatenate(recvs, axis=0).astype(jnp.int32)
    send_line = jnp.where(send_key >= 0, owner * pair_lines + (send >> 7), 200)
    recv_line = jnp.where(recv_key >= 0, home * pair_lines + (recv >> 7), -1)

    rf = rf_ref[...]
    cf = cf_ref[...]
    w = w_ref[...]
    rf_top = rf.astype(BF16).astype(F32)
    w_top = w.astype(BF16).astype(F32)
    values = [
        half.astype(F32),
        (c - half * HALF).astype(F32),
        (1.0 - cf).astype(BF16).astype(F32),
        cf.astype(BF16).astype(F32),
        rf_top,
        rf - rf_top,
        w_top,
        w - w_top,
        rel.astype(F32),
        send_line.astype(F32),
        (send & 127).astype(F32),
    ]
    total = jnp.zeros((FIELDS * chunks, LANES), F32)
    for i in range(0, lines, step):
        target = wide(spot, i)
        here = iota((chunks, step * LANES), 0) == (target >> 7)
        stack = jnp.concatenate([jnp.where(here, wide(v, i), 0.0) for v in values], axis=0).astype(BF16)
        place = jnp.where(iota((LANES, step * LANES), 0) == (target & 127), 1.0, 0.0).astype(BF16)
        total = total + nt_dot(stack, place)
    for f in range(FIELDS):
        plan_ref[f] = total[f * chunks : (f + 1) * chunks, :]

    slot_here = slot_of - me * owned
    received = slabs * pair_lines
    found = jnp.zeros((2 * received, LANES), F32)
    for i in range(0, lines, step):
        here = iota((received, step * LANES), 0) == wide(recv_line, i)
        target = wide(slot_here, i)
        stack = jnp.concatenate(
            [jnp.where(here, (target >> 7).astype(F32), 0.0), jnp.where(here, (target & 127).astype(F32), 0.0)], axis=0
        ).astype(BF16)
        place = jnp.where(iota((LANES, step * LANES), 0) == (wide(recv, i) & 127), 1.0, 0.0).astype(BF16)
        found = found + nt_dot(stack, place)
    places_ref[...] = (found[:received] * LANES + found[received:]).astype(jnp.int32)


def column_table(plan_ref, chunk, number):
    line = pl.ds(chunk, 1)
    column = plan_ref[0, line, :] * HALF + plan_ref[1, line, :] - (number * BLOCK).astype(F32)
    low = plan_ref[2, line, :].astype(BF16)
    high = plan_ref[3, line, :].astype(BF16)
    cells = iota((HALF, LANES), 0).astype(F32).astype(BF16)
    pieces = []
    for begin in range(0, BLOCK, HALF):
        near = jnp.clip(column - begin, -2.0, HALF).astype(BF16)
        after = jnp.clip(column - (begin - 1), -2.0, HALF).astype(BF16)
        pieces.append(jnp.where(cells == near, low, jnp.where(cells == after, high, jnp.zeros((), BF16))))
    return jnp.concatenate(pieces, axis=0)


def row_pattern(plan_ref, chunk, rows, depth):
    line = pl.ds(chunk, 1)
    rf = plan_ref[4, line, :] + plan_ref[5, line, :]
    rel = plan_ref[8, line, :].astype(jnp.int32)
    row = iota((depth, LANES), 0) % rows + 1
    return jnp.where(row == rel, 1.0 - rf, jnp.where(row == rel + 1, rf, 0.0))


def group_chunks(marks_ref, group, keys_group, base):
    count = (marks_ref[1, (group + 1) * keys_group - 1] - base + LANES - 1) // LANES
    return jnp.maximum(count, 1)


def chunk_range(marks_ref, group, number, keys_group, cap_chunks):
    at = group * keys_group + 2 * number
    begin = marks_ref[0, jnp.maximum(at - 1, group * keys_group)]
    end = marks_ref[1, at + 1]
    base = group * cap_chunks
    last = base + group_chunks(marks_ref, group, keys_group, base * LANES) - 1
    return jnp.minimum(begin // LANES, last), jnp.where(end > begin, (end + LANES - 1) // LANES, 0)


def forward_kernel(cap_chunks, blocks, field_ref, plan_ref, marks_ref, value_ref, sums, flat):
    probes, rows, _ = field_ref.shape
    depth = probes * rows
    keys_group = 2 * blocks
    number = pl.program_id(0)
    counts = [group_chunks(marks_ref, g, keys_group, g * cap_chunks * LANES) for g in range(3)]

    @pl.when(number == 0)
    def _():
        for g in range(3):

            @pl.loop(0, counts[g])
            def _(k):
                sums[g * cap_chunks + k] = jnp.zeros((depth, LANES), F32)

    block = field_ref[...].reshape(depth, BLOCK)
    flat[...] = block
    ranges = [chunk_range(marks_ref, g, number, keys_group, cap_chunks) for g in range(3)]
    table = jnp.concatenate([column_table(plan_ref, begin, number) for begin, _ in ranges], axis=1)
    part = jnp.dot(block, table, preferred_element_type=F32)
    for g in range(3):
        sums[ranges[g][0]] += part[:, g * LANES : (g + 1) * LANES]
    for g in range(3):

        @pl.loop(ranges[g][0] + 1, ranges[g][1])
        def _(chunk):
            sums[chunk] += jnp.dot(flat[...], column_table(plan_ref, chunk, number), preferred_element_type=F32)

    @pl.when(number == blocks - 1)
    def _():
        fold = jnp.where(iota((probes, depth), 1) // rows == iota((probes, depth), 0), 1.0, 0.0).astype(BF16)
        for g in range(3):

            @pl.loop(0, counts[g])
            def _(k):
                chunk = g * cap_chunks + k
                scaled = (sums[chunk] * row_pattern(plan_ref, chunk, rows, depth)).astype(BF16)
                value_ref[chunk] = jnp.dot(fold, scaled, preferred_element_type=F32)


def swap_kernel(slabs, top, value_ref, above_ref, below_ref, send_sem, recv_sem):
    probe, me = lax.axis_index("probe"), lax.axis_index("slab")
    width = above_ref.shape[0]
    down, up = lax.rem(me + slabs - 1, slabs), lax.rem(me + 1, slabs)
    barrier = pltpu.get_barrier_semaphore()
    for peer in (down, up):
        pl.semaphore_signal(barrier, inc=1, device_id=(peer, probe), device_id_type=pl.DeviceIdType.MESH)
    pl.semaphore_wait(barrier, 2)
    copies = []
    for k, (peer, begin, target) in enumerate(((down, 0, above_ref), (up, top, below_ref))):
        copies.append(
            pltpu.make_async_remote_copy(
                src_ref=value_ref.at[begin : begin + width],
                dst_ref=target,
                send_sem=send_sem.at[k],
                recv_sem=recv_sem.at[k],
                device_id=(peer, probe),
                device_id_type=pl.DeviceIdType.MESH,
            )
        )
    for copy in copies:
        copy.start()
    for copy in copies:
        copy.wait()


def swap(slabs, cap_chunks, width, number, value):
    part = (width, *value.shape[1:])
    any_space = pl.BlockSpec(memory_space=pl.ANY)
    above, below = pl.pallas_call(
        functools.partial(swap_kernel, slabs, 2 * cap_chunks),
        out_shape=(jax.ShapeDtypeStruct(part, F32), jax.ShapeDtypeStruct(part, F32)),
        in_specs=[any_space],
        out_specs=(any_space, any_space),
        scratch_shapes=[pltpu.SemaphoreType.DMA((2,)), pltpu.SemaphoreType.DMA((2,))],
        compiler_params=pltpu.CompilerParams(collective_id=number, has_side_effects=True),
        name="swap",
    )(value)
    return above, below


def merge_kernel(cap_chunks, blocks, value_ref, above_ref, below_ref, plan_ref, marks_ref, spread_ref, packed_ref, squares, parts):
    slabs = packed_ref.shape[0]
    outgoing, probes, _ = parts.shape
    lines = outgoing // slabs
    keys_group = 2 * blocks
    squares[...] = jnp.zeros_like(squares)
    parts[...] = jnp.zeros_like(parts)
    for g in range(3):
        count = group_chunks(marks_ref, g, keys_group, g * cap_chunks * LANES)

        @pl.loop(0, count)
        def _(k):
            chunk = g * cap_chunks + k
            value = value_ref[chunk]
            if g == 0:
                value = value + below_ref[k]
            if g == 2:
                value = value + above_ref[k]
            line = pl.ds(chunk, 1)
            spread = value * (plan_ref[6, line, :] + plan_ref[7, line, :])
            spread_ref[chunk] = spread.astype(BF16)
            if g > 0:
                squares[...] += spread * value
                high = plan_ref[9, line, :].astype(jnp.int32)
                low = plan_ref[10, line, :].astype(jnp.int32)
                place = jnp.where(iota((LANES, LANES), 0) == low, 1.0, 0.0).astype(BF16)
                stack = jnp.concatenate([jnp.where(high == d, value, 0.0) for d in range(outgoing)], axis=0).astype(BF16)
                parts[...] += nt_dot(stack, place).reshape(outgoing, probes, LANES)

    folded = squares[:8, :]
    for d in range(8, probes, 8):
        folded = folded + squares[d : d + 8, :]
    for d in range(slabs):
        for e in range(lines):
            packed_ref[d, e * probes : (e + 1) * probes, :] = parts[d * lines + e]
        packed_ref[d, lines * probes :, :] = folded


def unpack_kernel(groups, scale, packed_ref, places_ref, observed_ref, mean_ref, traces, send_sem, recv_sem):
    slab, me = lax.axis_index("slab"), lax.axis_index("probe")
    slabs = packed_ref.shape[0]
    probes, owned = observed_ref.shape
    lines = places_ref.shape[0] // slabs
    barrier = pltpu.get_barrier_semaphore()
    for k in range(1, groups):
        peer = lax.rem(me + k, groups)
        pl.semaphore_signal(barrier, inc=1, device_id=(slab, peer), device_id_type=pl.DeviceIdType.MESH)
    own = packed_ref[0, lines * probes :, :]
    for d in range(1, slabs):
        own = own + packed_ref[d, lines * probes :, :]
    traces[me] = own
    pl.semaphore_wait(barrier, groups - 1)

    def tile(k, source, peer):
        return pltpu.make_async_remote_copy(
            src_ref=traces.at[me],
            dst_ref=traces.at[source],
            send_sem=send_sem.at[k],
            recv_sem=recv_sem.at[k],
            device_id=(slab, peer),
            device_id_type=pl.DeviceIdType.MESH,
        )

    for k in range(1, groups):
        tile(k, me, lax.rem(me + k, groups)).start()
    total = jnp.zeros((probes, owned), F32)
    for d in range(slabs):
        for e in range(lines):
            at = d * lines + e
            place = jnp.where(iota((owned, LANES), 0) == places_ref[at : at + 1, :], 1.0, 0.0).astype(BF16)
            total = total + nt_dot(packed_ref[d, e * probes : (e + 1) * probes, :].astype(BF16), place)
    observed_ref[...] = total
    for k in range(1, groups):
        source = lax.rem(me + groups - k, groups)
        tile(k, source, source).wait()
    summed = jnp.sum(jnp.sum(traces[...], axis=0), axis=0, keepdims=True)
    mean_ref[...] = jnp.broadcast_to(jnp.sum(summed, axis=1, keepdims=True) * scale, mean_ref.shape)


def adjoint_kernel(cap_chunks, blocks, spread_ref, plan_ref, marks_ref, out_ref, sources, total):
    probes, rows, _ = out_ref.shape
    depth = probes * rows
    keys_group = 2 * blocks
    number = pl.program_id(0)

    @pl.when(number == 0)
    def _():
        raise_rows = jnp.where(iota((depth, probes), 0) // rows == iota((depth, probes), 1), 1.0, 0.0).astype(BF16)
        for g in range(3):
            count = group_chunks(marks_ref, g, keys_group, g * cap_chunks * LANES)

            @pl.loop(0, count)
            def _(k):
                chunk = g * cap_chunks + k
                raised = jnp.dot(raise_rows, spread_ref[chunk], preferred_element_type=F32)
                sources[chunk] = (raised * row_pattern(plan_ref, chunk, rows, depth)).astype(BF16)

    ranges = [chunk_range(marks_ref, g, number, keys_group, cap_chunks) for g in range(3)]
    table = jnp.concatenate([column_table(plan_ref, begin, number) for begin, _ in ranges], axis=1)
    source = jnp.concatenate([sources[begin] for begin, _ in ranges], axis=1)
    total[...] = nt_dot(source, table)
    for g in range(3):

        @pl.loop(ranges[g][0] + 1, ranges[g][1])
        def _(chunk):
            total[...] += nt_dot(sources[chunk], column_table(plan_ref, chunk, number))

    out_ref[...] = total[...].astype(BF16).reshape(probes, rows, BLOCK)


def general(slab_count, probe_groups, probe_fields, sensor_rows, sensor_cols, row_frac, col_frac, sensor_weights, owner_order):
    probes, rows, width = probe_fields.shape
    sensors = sensor_rows.shape[0]
    depth = probes * rows
    lines = sensors // LANES
    blocks = width // BLOCK
    keys = 6 * blocks
    most = min(sensors, 4 * sensors // slab_count)
    cap_chunks = -(-most // (8 * LANES)) * 8
    chunks = 3 * cap_chunks
    pair_lines = -(-most // (slab_count * LANES))
    outgoing = slab_count * pair_lines
    me = jnp.reshape(lax.axis_index("slab"), (1,)).astype(jnp.int32)
    boxed = [x.reshape(lines, LANES) for x in (sensor_rows, sensor_cols, row_frac, col_frac, sensor_weights, owner_order)]
    vmem = pl.BlockSpec(memory_space=VMEM)
    smem = pl.BlockSpec(memory_space=SMEM)
    plan, marks, places, peak = pl.pallas_call(
        functools.partial(plan_kernel, rows, cap_chunks, blocks, slab_count, pair_lines),
        out_shape=(
            jax.ShapeDtypeStruct((FIELDS, chunks, LANES), F32),
            jax.ShapeDtypeStruct((2, -(-keys // LANES) * LANES), jnp.int32),
            jax.ShapeDtypeStruct((outgoing, LANES), jnp.int32),
            jax.ShapeDtypeStruct((1,), jnp.int32),
        ),
        in_specs=[smem] + [vmem] * 6,
        out_specs=(vmem, vmem, vmem, smem),
        compiler_params=LIMIT,
        name="plan",
    )(me, *boxed)
    value = pl.pallas_call(
        functools.partial(forward_kernel, cap_chunks, blocks),
        out_shape=jax.ShapeDtypeStruct((chunks, probes, LANES), F32),
        grid=(blocks,),
        in_specs=[pl.BlockSpec((probes, rows, BLOCK), lambda n: (0, 0, n)), vmem, smem],
        out_specs=vmem,
        scratch_shapes=[VMEM((chunks, depth, LANES), F32), VMEM((depth, BLOCK), BF16)],
        compiler_params=LIMIT,
        name="forward",
    )(probe_fields, plan, marks)
    few = min(cap_chunks, -(-5 * most // (4 * rows * LANES)))

    def merged(above, below):
        return pl.pallas_call(
            functools.partial(merge_kernel, cap_chunks, blocks),
            out_shape=(
                jax.ShapeDtypeStruct((chunks, probes, LANES), BF16),
                jax.ShapeDtypeStruct((slab_count, pair_lines * probes + 8, LANES), F32),
            ),
            in_specs=[vmem, vmem, vmem, vmem, smem],
            out_specs=(vmem, vmem),
            scratch_shapes=[VMEM((probes, LANES), F32), VMEM((outgoing, probes, LANES), F32)],
            compiler_params=LIMIT,
            name="merge",
        )(value, above, below, plan, marks)

    spread, packed = lax.cond(
        peak[0] <= few * LANES,
        lambda: merged(*swap(slab_count, cap_chunks, few, 0, value)),
        lambda: merged(*swap(slab_count, cap_chunks, cap_chunks, 1, value)),
    )
    arrived = lax.all_to_all(packed, "slab", 0, 0, tiled=True)
    adjoint = pl.pallas_call(
        functools.partial(adjoint_kernel, cap_chunks, blocks),
        out_shape=jax.ShapeDtypeStruct((probes, rows, width), BF16),
        grid=(blocks,),
        in_specs=[vmem, vmem, smem],
        out_specs=pl.BlockSpec((probes, rows, BLOCK), lambda n: (0, 0, n)),
        scratch_shapes=[
            VMEM((chunks, depth, LANES), BF16),
            VMEM((depth, BLOCK), F32),
        ],
        compiler_params=LIMIT,
        cost_estimate=pl.CostEstimate(flops=4 * 10**9, bytes_accessed=8 * 10**6, transcendentals=0),
        name="adjoint",
    )(spread, plan, marks)
    observed, mean = pl.pallas_call(
        functools.partial(unpack_kernel, probe_groups, 1.0 / (probes * probe_groups * sensors)),
        out_shape=(
            jax.ShapeDtypeStruct((probes, sensors // slab_count), F32),
            jax.ShapeDtypeStruct((1, LANES), F32),
        ),
        in_specs=[vmem, vmem],
        out_specs=(vmem, vmem),
        scratch_shapes=[
            VMEM((probe_groups, 8, LANES), F32),
            pltpu.SemaphoreType.DMA((probe_groups,)),
            pltpu.SemaphoreType.DMA((probe_groups,)),
        ],
        compiler_params=pltpu.CompilerParams(collective_id=2, has_side_effects=True, vmem_limit_bytes=40 * 1024 * 1024),
        name="unpack",
    )(arrived, places)
    return adjoint, observed, mean[0, 0]


COLS = 256
FAST = 11
ROOM = 28 * 1024 * 1024
SMALL = pltpu.CompilerParams(vmem_limit_bytes=ROOM)


class Geo(typing.NamedTuple):
    rows: int
    probes: int
    slabs: int
    groups: int
    buckets: int
    tiles: int
    lines: int
    owned: int
    quarter: int
    edge_lines: int
    kinds: int


def bf(x):
    return x.astype(BF16)


def cells(rows, width):
    return bf(iota((rows, width), 0).astype(F32))


def match(rows, target):
    grid = cells(min(rows, COLS), target.shape[1])
    pieces = []
    for begin in range(0, rows, COLS):
        size = min(COLS, rows - begin)
        near = bf(jnp.clip(target - begin, -1.0, float(COLS)))
        pieces.append(jnp.where(grid[:size] == near, jnp.ones((), BF16), jnp.zeros((), BF16)))
    return pieces[0] if len(pieces) == 1 else jnp.concatenate(pieces, axis=0)


def observe_kernel(geo, me_ref, r_ref, c_ref, rf_ref, cf_ref, w_ref, order_ref, field_ref, plan_ref, slot_ref, flag_ref, value_ref, tiles, hots, ranks, fold, sem):
    lines, slabs, buckets, owned = geo.lines, geo.slabs, geo.buckets, geo.owned
    loads = 8
    rounds = geo.tiles // loads

    def load(g, j):
        t = g * loads + j
        return pltpu.make_async_copy(field_ref.at[:, t], tiles.at[t], sem.at[g])

    for g in reversed(range(rounds)):
        for j in range(loads):
            load(g, j).start()

    me = me_ref[0]
    step = min(4, lines)
    kinds = geo.kinds

    def wide(x, i):
        return jnp.concatenate([x[i + j : i + j + 1, :] for j in range(step)], axis=1)

    order = order_ref[...]
    slot = iota((lines, LANES), 0) * LANES + iota((lines, LANES), 1)
    order_hi, order_lo = bf((order >> 7).astype(F32)), bf((order & 127).astype(F32))
    order_hi, order_lo = order_hi.astype(F32), order_lo.astype(F32)
    mine_hi, mine_lo = (slot >> 7).astype(F32), (slot & 127).astype(F32)
    found = jnp.zeros((2 * lines, LANES), F32)
    line_cells, lane_cells = cells(lines, step * LANES), cells(LANES, step * LANES)
    zero, one = jnp.zeros((), BF16), jnp.ones((), BF16)
    for i in range(0, lines, step):
        here = line_cells == bf(wide(order_hi, i))
        stack = jnp.concatenate([jnp.where(here, bf(wide(mine_hi, i)), zero), jnp.where(here, bf(wide(mine_lo, i)), zero)], axis=0)
        place = jnp.where(lane_cells == bf(wide(order_lo, i)), one, zero)
        found = found + nt_dot(stack, place)
    slot_of = (found[:lines] * LANES + found[lines:]).astype(jnp.int32)

    r = r_ref[...]
    c = c_ref[...]
    rel = r - me * geo.rows + 1
    valid = (rel >= 0) & (rel <= geo.rows)
    bucket = c // COLS
    owner = slot_of // owned
    home = r // geo.rows
    edge = r - home * geo.rows == geo.rows - 1
    key = jnp.where(valid, bucket, -1)
    send_key = jnp.where(valid, owner, -1)
    first_key = jnp.where(owner == me, home, -1)
    second_key = jnp.where((owner == me) & edge, home + 1, -1)
    edge_key = jnp.where(valid & (rel == 0), 0, jnp.where(valid & (rel == geo.rows), 1, -1))

    def hot_of(i):
        line = slice(i, i + 1)
        recv = iota((slabs, LANES), 0)
        return (
            iota((buckets, LANES), 0) == key[line],
            recv == send_key[line],
            recv == first_key[line],
            recv == second_key[line],
            iota((16, LANES), 0) == edge_key[line],
        )

    for i in range(lines):
        a, b, c1, c2, d = hot_of(i)
        hot = jnp.concatenate([jnp.where(x, 1.0, 0.0) for x in (a, b, c1 | c2, d)], axis=0)
        hots[i * kinds : (i + 1) * kinds, :] = bf(hot)
    upper = iota((LANES, 2 * LANES), 0) < iota((LANES, 2 * LANES), 1)
    upper = bf(jnp.where(upper, 1.0, 0.0))
    before = jnp.dot(hots[...], upper, preferred_element_type=F32)
    carry = jnp.zeros((kinds, LANES), F32)
    for i in range(lines):
        part = before[i * kinds : (i + 1) * kinds]
        rank = part[:, :LANES] + carry
        a, b, c1, c2, d = hot_of(i)
        recv = rank[buckets + slabs : buckets + 2 * slabs]
        picks = (
            (a, rank[:buckets]),
            (b, rank[buckets : buckets + slabs]),
            (c1, recv),
            (c2, recv),
            (d, rank[buckets + 2 * slabs :]),
        )
        for k, (mask, value) in enumerate(picks):
            ranks[k, i : i + 1, :] = jnp.sum(jnp.where(mask, value, 0.0), axis=0, keepdims=True)
        carry = carry + part[:, LANES:]
    capacity = 4.0 * geo.quarter
    row = iota((kinds, LANES), 0)
    limit = jnp.where(row < buckets, float(LANES), jnp.where(row < buckets + 2 * slabs, capacity, float(geo.edge_lines * LANES)))
    over = jnp.sum(jnp.where(carry > limit, 1.0, 0.0), axis=0, keepdims=True)
    flag_ref[...] = jnp.broadcast_to(over, flag_ref.shape)

    spot, send, recv1, recv2, swap = (ranks[k] for k in range(5))
    rf, cf, w = rf_ref[...], cf_ref[...], w_ref[...]
    rf_top, w_top = bf(rf).astype(F32), bf(w).astype(F32)
    send_quarter = jnp.floor((send + 0.5) * (1.0 / geo.quarter))
    swap_line = jnp.floor((swap + 0.5) * (1.0 / LANES))
    values = (
        (c - bucket * COLS).astype(F32),
        bf(1.0 - cf).astype(F32),
        bf(cf).astype(F32),
        rf_top,
        rf - rf_top,
        w_top,
        w - w_top,
        (rel + 1 + 8 * owner).astype(F32),
        send - send_quarter * geo.quarter,
        jnp.minimum(send_quarter, 15.0) + 16.0 * jnp.minimum(jnp.where(edge_key >= 0, swap_line, 0.0), 15.0),
        swap - swap_line * LANES,
    )
    key_value = jnp.where(valid & (spot < LANES), bucket, -1).astype(F32)
    bucket_cells = cells(buckets, step * LANES)
    total = jnp.zeros((FAST * buckets, LANES), F32)
    for i in range(0, lines, step):
        here = bucket_cells == bf(wide(key_value, i))
        stack = jnp.concatenate([jnp.where(here, bf(wide(v, i)), zero) for v in values], axis=0)
        place = jnp.where(lane_cells == bf(jnp.minimum(wide(spot, i), 255.0)), one, zero)
        total = total + nt_dot(stack, place)
    for f in range(FAST):
        plan_ref[f] = total[f * buckets : (f + 1) * buckets, :]

    sent = slabs * geo.quarter

    def position(rank, source, use):
        quarter = jnp.floor((rank + 0.5) * (1.0 / geo.quarter))
        place = quarter * sent + source.astype(F32) * geo.quarter + (rank - quarter * geo.quarter)
        return jnp.where(use, place, 4.0 * sent + 8.0)

    here_slot = slot_of - me * owned
    owned_lines = owned // LANES
    slot_line = jnp.where(owner == me, here_slot >> 7, -1).astype(F32)
    slot_lane = (here_slot & 127).astype(F32)
    fields = []
    for place in (position(recv1, home, owner == me), position(recv2, home + 1, edge)):
        high = jnp.floor(place * (1.0 / 64.0))
        fields += [high, place - 64.0 * high]
    slot_cells = cells(owned_lines, step * LANES)
    pad = -(4 * owned_lines) % 16
    placed = jnp.zeros((4 * owned_lines + pad, LANES), F32)
    for i in range(0, lines, step):
        here = jnp.broadcast_to(wide(slot_line, i), (owned_lines, step * LANES)) == iota((owned_lines, step * LANES), 0).astype(F32)
        stack = [jnp.where(here, wide(v, i), 0.0) for v in fields]
        if pad:
            stack.append(jnp.zeros((pad, step * LANES), F32))
        place = jnp.where(lane_cells == bf(wide(slot_lane, i)), one, zero)
        placed = placed + nt_dot(bf(jnp.concatenate(stack, axis=0)), place)
    for f in range(2):
        at = 2 * f * owned_lines
        slot_ref[f] = placed[at : at + owned_lines] * 64.0 + placed[at + owned_lines : at + 2 * owned_lines]

    depth = geo.rows * geo.probes
    spill = None
    batch = loads // 2
    for g in reversed(range(rounds)):
        for j in range(loads):
            load(g, j).wait()
        group = list(reversed(range(g * batch, (g + 1) * batch)))
        parts = []
        for b in group:
            block = jnp.concatenate([tiles[2 * b].reshape(depth, LANES), tiles[2 * b + 1].reshape(depth, LANES)], axis=1)
            parts.append(jnp.dot(block, bucket_table(plan_ref, b), preferred_element_type=F32))
        for b, part in zip(group, parts):
            value = part[:, :LANES]
            if spill is not None:
                value = value + spill
            spill = part[:, LANES:]
            fold[b] = value
            terms = [fold[b, pl.ds(k, geo.probes, stride=geo.rows), :] * x for k, x in enumerate(row_weights(geo, plan_ref, b))]
            value_ref[b] = functools.reduce(jnp.add, terms)


def bucket_table(plan_ref, b):
    near, low, high = (plan_ref[f, pl.ds(b, 1), :] for f in range(3))
    grid = cells(COLS, LANES)
    zero = jnp.zeros((), BF16)
    main = jnp.where(grid == bf(near), bf(low), jnp.where(grid == bf(near + 1.0), bf(high), zero))
    if isinstance(b, int) and b == 0:
        return jnp.concatenate([main, jnp.zeros((COLS, LANES), BF16)], axis=1)
    before = b - 1 if isinstance(b, int) else jnp.maximum(b - 1, 0)
    last, spill = (plan_ref[f, pl.ds(before, 1), :] for f in (0, 2))
    spill = jnp.where(last == COLS - 1.0, spill, 0.0)
    over = bf(jnp.where(iota((16, LANES), 0) == 0, spill, 0.0))
    over = jnp.concatenate([over, jnp.zeros((COLS - 16, LANES), BF16)], axis=0)
    return jnp.concatenate([main, over], axis=1)


def place_code(plan_ref, b):
    code = plan_ref[7, pl.ds(b, 1), :]
    owner = jnp.floor(code * 0.125)
    return owner, code - 8.0 * owner


def row_weights(geo, plan_ref, b):
    rf = plan_ref[3, pl.ds(b, 1), :] + plan_ref[4, pl.ds(b, 1), :]
    _, rel = place_code(plan_ref, b)
    return [jnp.where(rel == k + 2.0, 1.0 - rf, jnp.where(rel == k + 1.0, rf, 0.0)) for k in range(geo.rows)]


def exchange_kernel(geo, value_ref, plan_ref, flag_ref, adjoint_ref, arrived_ref, total_ref, ok_ref, edges, places, inbox, packed, sources, raised, tiles, sums, swap_send, swap_recv, owner_send, owner_recv, tile_send, tile_recv, sum_send, sum_recv):
    slabs, groups, probes, rows, quarter, buckets = geo.slabs, geo.groups, geo.probes, geo.rows, geo.quarter, geo.buckets
    me, mine = lax.axis_index("slab"), lax.axis_index("probe")
    lines = geo.edge_lines
    zero = jnp.zeros((), BF16)
    batch = 8

    def at(slab, probe):
        return dict(device_id=(slab, probe), device_id_type=pl.DeviceIdType.MESH)

    barrier = pltpu.get_barrier_semaphore()
    for k in range(1, slabs):
        pl.semaphore_signal(barrier, inc=1, **at(lax.rem(me + k, slabs), mine))
    for k in range(1, groups):
        pl.semaphore_signal(barrier, inc=1, **at(me, lax.rem(mine + k, groups)))

    def columns(j):
        return slice(j * LANES, (j + 1) * LANES)

    def edge_fields(b):
        _, rel = place_code(plan_ref, b)
        line = jnp.floor(plan_ref[9, pl.ds(b, 1), :] * (1.0 / 16.0))
        lane = plan_ref[10, pl.ds(b, 1), :]
        return rel, line, lane

    edges[...] = jnp.zeros_like(edges)

    @pl.loop(0, buckets // batch)
    def _(g):
        stacks, spots = [], []
        for j in range(batch):
            b = g * batch + j
            rel, line, lane = edge_fields(b)
            low, high = rel == 1.0, rel == rows + 1.0
            spot = match(2 * LANES, jnp.where(low, lane, jnp.where(high, lane + LANES, -1.0)))
            value = value_ref[b]
            stacks.append(jnp.concatenate([bf(jnp.where(line == float(l), value, 0.0)) for l in range(lines)], axis=0))
            spots.append(spot)
            places[b] = spot
        part = nt_dot(jnp.concatenate(stacks, axis=1), jnp.concatenate(spots, axis=1))
        for side in range(2):
            edges[side] += part[:, columns(side)]

    pl.semaphore_wait(barrier, slabs + groups - 2)
    down, up = lax.rem(me + slabs - 1, slabs), lax.rem(me + 1, slabs)
    swaps = [
        pltpu.make_async_remote_copy(
            src_ref=edges.at[side], dst_ref=inbox.at[1 - side], send_sem=swap_send.at[side], recv_sem=swap_recv.at[side], **at(peer, mine)
        )
        for side, peer in ((0, down), (1, up))
    ]
    for copy in swaps:
        copy.start()

    packed[...] = jnp.zeros_like(packed)

    @pl.loop(0, buckets // batch)
    def _(g):
        hots, quads = [], []
        for j in range(batch):
            b = g * batch + j
            owner, rel = place_code(plan_ref, b)
            code = plan_ref[9, pl.ds(b, 1), :]
            fourth = code - 16.0 * jnp.floor(code * (1.0 / 16.0))
            row = jnp.where(rel > 0.0, owner * quarter + plan_ref[8, pl.ds(b, 1), :], -1.0)
            hots.append(match(slabs * quarter, row))
            value = value_ref[b]
            quads.append(jnp.concatenate([bf(jnp.where(fourth == float(k), value, 0.0)) for k in range(4)], axis=0))
        part = nt_dot(jnp.concatenate(hots, axis=1), jnp.concatenate(quads, axis=1))
        packed[...] += part.reshape(packed.shape)

    def owner_copy(k, source, peer):
        return pltpu.make_async_remote_copy(
            src_ref=packed.at[peer], dst_ref=arrived_ref.at[source], send_sem=owner_send.at[k], recv_sem=owner_recv.at[k], **at(peer, mine)
        )

    for k in range(1, slabs):
        owner_copy(k, me, lax.rem(me + k, slabs)).start()
    arrived_ref[me] = packed[me]

    for copy in swaps:
        copy.wait()
    both = bf(jnp.concatenate([inbox[0], inbox[1]], axis=1))
    sources[0] = jnp.zeros_like(sources[0])
    squares = jnp.zeros((probes, LANES), F32)

    def merge(g, squares):
        spots = jnp.concatenate([places[g * batch + j] for j in range(batch)], axis=1)
        extra = jnp.dot(both, spots, preferred_element_type=F32)
        for j in range(batch):
            b = g * batch + j
            rel, line, _ = edge_fields(b)
            full = value_ref[b]
            for l in range(lines):
                full = full + jnp.where(line == float(l), extra[l * probes : (l + 1) * probes, columns(j)], 0.0)
            spread = full * (plan_ref[5, pl.ds(b, 1), :] + plan_ref[6, pl.ds(b, 1), :])
            squares = squares + jnp.where(rel >= 2.0, spread * full, 0.0)
            for k, weight in enumerate(row_weights(geo, plan_ref, b)):
                raised[j, pl.ds(k, probes, stride=rows), :] = spread * weight
            sources[b + 1] = bf(raised[j])
        return squares

    squares = lax.fori_loop(0, buckets // batch, merge, squares)
    folded = squares[:8]
    for d in range(8, probes, 8):
        folded = folded + squares[d : d + 8]
    tiles[mine] = jnp.concatenate([folded, flag_ref[...]], axis=0)

    def tile_copy(k, source, peer):
        return pltpu.make_async_remote_copy(
            src_ref=tiles.at[mine], dst_ref=tiles.at[source], send_sem=tile_send.at[k], recv_sem=tile_recv.at[k], **at(me, peer)
        )

    for k in range(1, groups):
        tile_copy(k, mine, lax.rem(mine + k, groups)).start()

    @pl.loop(0, buckets // batch)
    def _(g):
        parts = []
        for j in range(batch):
            b = g * batch + j
            source = jnp.concatenate([sources[b + 1], sources[b]], axis=1)
            parts.append(nt_dot(source, bucket_table(plan_ref, b)))
        for j in range(batch):
            for t in range(2):
                adjoint_ref[2 * (g * batch + j) + t] = bf(parts[j][:, columns(t)]).reshape(probes, rows, LANES)

    for k in range(1, groups):
        source = lax.rem(mine + groups - k, groups)
        tile_copy(k, source, source).wait()
    sums[me] = jnp.sum(tiles[...], axis=0)

    def sum_copy(k, source, peer):
        return pltpu.make_async_remote_copy(
            src_ref=sums.at[me], dst_ref=sums.at[source], send_sem=sum_send.at[k], recv_sem=sum_recv.at[k], **at(peer, mine)
        )

    for k in range(1, slabs):
        sum_copy(k, me, lax.rem(me + k, slabs)).start()
    for k in range(1, slabs):
        source = lax.rem(me + slabs - k, slabs)
        owner_copy(k, source, source).wait()
    for k in range(1, slabs):
        source = lax.rem(me + slabs - k, slabs)
        sum_copy(k, source, source).wait()
    total = jnp.sum(sums[...], axis=0)
    total_ref[...] = total
    ok_ref[0] = jnp.max(total[8:]).astype(jnp.int32)


def deliver_kernel(geo, scale, adjoint_ref, arrived_ref, slot_ref, total_ref, out_ref, observed_ref, mean_ref, observed, sem):
    slabs, probes, quarter, owned = geo.slabs, geo.probes, geo.quarter, geo.owned
    loads = 8

    def store(t):
        return pltpu.make_async_copy(adjoint_ref.at[t], out_ref.at[:, t], sem.at[0])

    for t in range(geo.tiles):
        store(t).start()
    sent = slabs * quarter
    arrived = jnp.transpose(arrived_ref[...].reshape(sent, 4 * probes))
    lines = owned // LANES
    spots = [jnp.concatenate([slot_ref[f, l : l + 1, :] for l in range(lines)], axis=1) for f in range(2)]
    total = jnp.zeros((probes, owned), F32)
    for k in range(4):
        hot = match(sent, spots[0] - float(k * sent)) + match(sent, spots[1] - float(k * sent))
        total = total + jnp.dot(bf(arrived[k * probes : (k + 1) * probes]), hot, preferred_element_type=F32)
    observed[...] = total
    pltpu.make_async_copy(observed, observed_ref, sem.at[1]).start()
    summed = jnp.sum(total_ref[:8], axis=0, keepdims=True)
    mean_ref[...] = jnp.broadcast_to(jnp.sum(summed, axis=1, keepdims=True) * scale, mean_ref.shape)
    pltpu.make_async_copy(observed, observed_ref, sem.at[1]).wait()
    for t in range(geo.tiles):
        store(t).wait()


def geometry(slabs, groups, probe_fields, sensors):
    probes, rows, width = probe_fields.shape
    most = min(sensors, 4 * sensors // slabs)
    quarter = -(-(most // slabs + 32) // 32) * 8
    edge_lines = -(-5 * most // (4 * rows * LANES))
    buckets = width // COLS
    return Geo(rows, probes, slabs, groups, buckets, width // LANES, sensors // LANES, sensors // slabs, quarter, edge_lines, buckets + 2 * slabs + 16)


def body(slab_count, probe_groups, probe_fields, *vectors):
    sensors = vectors[0].shape[0]
    geo = geometry(slab_count, probe_groups, probe_fields, sensors)
    probes, rows, width = probe_fields.shape
    depth = probes * rows
    lines, buckets, tiles = geo.lines, geo.buckets, geo.tiles
    me = jnp.reshape(lax.axis_index("slab"), (1,)).astype(jnp.int32)
    boxed = [x.reshape(lines, LANES) for x in vectors]
    field = probe_fields.reshape(probes, rows, tiles, LANES).transpose(0, 2, 1, 3)
    vmem = pl.BlockSpec(memory_space=VMEM)
    smem = pl.BlockSpec(memory_space=SMEM)
    hbm = pl.BlockSpec(memory_space=pltpu.HBM)
    dma = pltpu.SemaphoreType.DMA
    shape = jax.ShapeDtypeStruct
    plan, slots, flags, value = pl.pallas_call(
        functools.partial(observe_kernel, geo),
        out_shape=(
            shape((FAST, buckets, LANES), F32),
            shape((2, geo.owned // LANES, LANES), F32),
            shape((8, LANES), F32),
            shape((buckets, probes, LANES), F32),
        ),
        in_specs=[smem] + [vmem] * 6 + [hbm],
        out_specs=(vmem,) * 4,
        scratch_shapes=[
            VMEM((tiles, probes, rows, LANES), BF16),
            VMEM((lines * geo.kinds, LANES), BF16),
            VMEM((5, lines, LANES), F32),
            VMEM((buckets, depth, LANES), F32),
            dma((tiles // 8,)),
        ],
        compiler_params=SMALL,
        name="observe",
    )(me, *boxed, field)
    edge_rows = geo.edge_lines * probes
    adjoint, arrived, total, flag = pl.pallas_call(
        functools.partial(exchange_kernel, geo),
        out_shape=(
            shape((tiles, probes, rows, LANES), BF16),
            shape((slab_count, geo.quarter, 4 * probes), F32),
            shape((16, LANES), F32),
            shape((1,), jnp.int32),
        ),
        in_specs=[vmem] * 3,
        out_specs=(vmem, vmem, vmem, smem),
        scratch_shapes=[
            VMEM((2, edge_rows, LANES), F32),
            VMEM((buckets, 2 * LANES, LANES), BF16),
            VMEM((2, edge_rows, LANES), F32),
            VMEM((slab_count, geo.quarter, 4 * probes), F32),
            VMEM((buckets + 1, depth, LANES), BF16),
            VMEM((8, depth, LANES), F32),
            VMEM((probe_groups, 16, LANES), F32),
            VMEM((slab_count, 16, LANES), F32),
            dma((2,)),
            dma((2,)),
            dma((slab_count,)),
            dma((slab_count,)),
            dma((probe_groups,)),
            dma((probe_groups,)),
            dma((slab_count,)),
            dma((slab_count,)),
        ],
        compiler_params=pltpu.CompilerParams(collective_id=3, has_side_effects=True, vmem_limit_bytes=ROOM),
        name="exchange",
    )(value, plan, flags)

    def deliver():
        out, observed, mean = pl.pallas_call(
            functools.partial(deliver_kernel, geo, 1.0 / (probes * probe_groups * sensors)),
            out_shape=(
                shape((probes, tiles, rows, LANES), BF16),
                shape((probes, geo.owned), F32),
                shape((1, LANES), F32),
            ),
            in_specs=[vmem] * 4,
            out_specs=(hbm, hbm, vmem),
            scratch_shapes=[VMEM((probes, geo.owned), F32), dma((2,))],
            compiler_params=SMALL,
            name="deliver",
        )(adjoint, arrived, slots, total)
        return out.transpose(0, 2, 1, 3).reshape(probes, rows, width), observed, mean[0, 0]

    return lax.cond(flag[0] == 0, deliver, lambda: general(slab_count, probe_groups, probe_fields, *vectors))


def solution(mesh):
    placed = (P("probe", "slab", None), P(), P(), P(), P(), P(), P())
    return jax.shard_map(
        functools.partial(body, mesh.shape["slab"], mesh.shape["probe"]),
        mesh=mesh,
        in_specs=placed,
        out_specs=(P("probe", "slab", None), P("probe", "slab"), P()),
        check_vma=False,
    )
```

```python
import functools
import typing

import jax
import jax.numpy as jnp
from jax import lax
from jax.experimental import pallas as pl
from jax.experimental.pallas import tpu as pltpu
from jax.sharding import PartitionSpec as P

LANES = 128
BLOCK = 1024
HALF = 256
FIELDS = 11
F32 = jnp.float32
BF16 = jnp.bfloat16
NT = (((1,), (1,)), ((), ()))
VMEM = pltpu.VMEM
SMEM = pltpu.SMEM
LIMIT = pltpu.CompilerParams(vmem_limit_bytes=60 * 1024 * 1024)


def iota(shape, dim):
    return lax.broadcasted_iota(jnp.int32, shape, dim)


def nt_dot(a, b):
    return lax.dot_general(a, b, NT, preferred_element_type=F32)


def plan_kernel(rows, cap_chunks, blocks, slabs, pair_lines, me_ref, r_ref, c_ref, rf_ref, cf_ref, w_ref, order_ref, plan_ref, marks_ref, places_ref, peak_ref):
    lines = r_ref.shape[0]
    sensors = lines * LANES
    step = min(4, lines)
    me = me_ref[0]
    first = me * rows
    owned = lines * LANES // slabs
    keys_group = 2 * blocks
    keys = 3 * keys_group
    chunks = 3 * cap_chunks

    def wide(x, i):
        return jnp.concatenate([x[i + j : i + j + 1, :] for j in range(step)], axis=1)

    order = order_ref[...]
    slot = iota((lines, LANES), 0) * LANES + iota((lines, LANES), 1)
    found = jnp.zeros((2 * lines, LANES), F32)
    for i in range(0, lines, step):
        target = wide(order, i)
        mine = wide(slot, i)
        here = iota((lines, step * LANES), 0) == (target >> 7)
        stack = jnp.concatenate(
            [jnp.where(here, (mine >> 7).astype(F32), 0.0), jnp.where(here, (mine & 127).astype(F32), 0.0)], axis=0
        ).astype(BF16)
        place = jnp.where(iota((LANES, step * LANES), 0) == (target & 127), 1.0, 0.0).astype(BF16)
        found = found + nt_dot(stack, place)
    slot_hi = found[:lines, :]
    slot_lo = found[lines:, :]

    r = r_ref[...]
    c = c_ref[...]
    rel = r - first + 1
    valid = (rel >= 0) & (rel <= rows)
    group = jnp.where(rel == 0, 0, jnp.where(rel == rows, 2, 1))
    block = c // BLOCK
    inner = c - block * BLOCK
    half = c // HALF
    slot_of = (slot_hi * LANES + slot_lo).astype(jnp.int32)
    owner = slot_of // owned
    home = r // rows
    send_key = jnp.where(home == me, owner, -1)
    recv_key = jnp.where(owner == me, home, -1)
    edge = jnp.where(r - home * rows == rows - 1, home, -1)
    edges = jnp.zeros((slabs, LANES), F32)
    for i in range(lines):
        edges = edges + jnp.where(iota((slabs, LANES), 0) == edge[i : i + 1, :], 1.0, 0.0)
    peak_ref[0] = jnp.max(jnp.sum(edges, axis=1, keepdims=True)).astype(jnp.int32)
    key = group * keys_group + 2 * block + jnp.where(inner == BLOCK - 1, 1, 0)
    key = jnp.where(valid, key, -1)

    count = jnp.zeros((keys, 1), F32)
    for i in range(lines):
        count = count + jnp.sum(jnp.where(iota((keys, LANES), 0) == key[i : i + 1, :], 1.0, 0.0), axis=1, keepdims=True)
    big = jnp.floor(count * (1.0 / 64.0))
    small = count - 64.0 * big
    ka, kb = iota((keys, keys), 0), iota((keys, keys), 1)
    below = jnp.where((kb < ka) & (kb // keys_group == ka // keys_group), 1.0, 0.0).astype(BF16)
    start = 64.0 * jnp.dot(below, jnp.broadcast_to(big, (keys, LANES)).astype(BF16), preferred_element_type=F32)
    start = start + jnp.dot(below, jnp.broadcast_to(small, (keys, LANES)).astype(BF16), preferred_element_type=F32)
    start = start + ((iota((keys, LANES), 0) // keys_group) * (cap_chunks * LANES)).astype(F32)
    wide_keys = marks_ref.shape[1]
    diagonal = iota((keys, wide_keys), 0) == iota((keys, wide_keys), 1)
    marks_ref[...] = jnp.concatenate(
        [jnp.sum(jnp.where(diagonal, x, 0.0), axis=0, keepdims=True) for x in (start[:, :1], start[:, :1] + count)], axis=0
    ).astype(jnp.int32)

    upper = jnp.where(iota((LANES, LANES), 0) < iota((LANES, LANES), 1), 1.0, 0.0).astype(BF16)
    carry = jnp.concatenate([start[:, :1], jnp.zeros((2 * slabs, 1), F32)], axis=0)
    spots, sends, recvs = [], [], []
    for i in range(lines):
        hot = jnp.concatenate(
            [
                jnp.where(iota((keys, LANES), 0) == key[i : i + 1, :], 1.0, 0.0),
                jnp.where(iota((slabs, LANES), 0) == send_key[i : i + 1, :], 1.0, 0.0),
                jnp.where(iota((slabs, LANES), 0) == recv_key[i : i + 1, :], 1.0, 0.0),
            ],
            axis=0,
        )
        before = jnp.dot(hot.astype(BF16), upper, preferred_element_type=F32)
        ranks = hot * (before + carry)
        spots.append(jnp.sum(ranks[:keys], axis=0, keepdims=True))
        sends.append(jnp.sum(ranks[keys : keys + slabs], axis=0, keepdims=True))
        recvs.append(jnp.sum(ranks[keys + slabs :], axis=0, keepdims=True))
        carry = carry + jnp.sum(hot, axis=1, keepdims=True)
    spot = jnp.concatenate(spots, axis=0).astype(jnp.int32)
    spot = jnp.where(valid, spot, -1)
    send = jnp.concatenate(sends, axis=0).astype(jnp.int32)
    recv = jnp.concatenate(recvs, axis=0).astype(jnp.int32)
    send_line = jnp.where(send_key >= 0, owner * pair_lines + (send >> 7), 200)
    recv_line = jnp.where(recv_key >= 0, home * pair_lines + (recv >> 7), -1)

    rf = rf_ref[...]
    cf = cf_ref[...]
    w = w_ref[...]
    rf_top = rf.astype(BF16).astype(F32)
    w_top = w.astype(BF16).astype(F32)
    values = [
        half.astype(F32),
        (c - half * HALF).astype(F32),
        (1.0 - cf).astype(BF16).astype(F32),
        cf.astype(BF16).astype(F32),
        rf_top,
        rf - rf_top,
        w_top,
        w - w_top,
        rel.astype(F32),
        send_line.astype(F32),
        (send & 127).astype(F32),
    ]
    total = jnp.zeros((FIELDS * chunks, LANES), F32)
    for i in range(0, lines, step):
        target = wide(spot, i)
        here = iota((chunks, step * LANES), 0) == (target >> 7)
        stack = jnp.concatenate([jnp.where(here, wide(v, i), 0.0) for v in values], axis=0).astype(BF16)
        place = jnp.where(iota((LANES, step * LANES), 0) == (target & 127), 1.0, 0.0).astype(BF16)
        total = total + nt_dot(stack, place)
    for f in range(FIELDS):
        plan_ref[f] = total[f * chunks : (f + 1) * chunks, :]

    slot_here = slot_of - me * owned
    received = slabs * pair_lines
    found = jnp.zeros((2 * received, LANES), F32)
    for i in range(0, lines, step):
        here = iota((received, step * LANES), 0) == wide(recv_line, i)
        target = wide(slot_here, i)
        stack = jnp.concatenate(
            [jnp.where(here, (target >> 7).astype(F32), 0.0), jnp.where(here, (target & 127).astype(F32), 0.0)], axis=0
        ).astype(BF16)
        place = jnp.where(iota((LANES, step * LANES), 0) == (wide(recv, i) & 127), 1.0, 0.0).astype(BF16)
        found = found + nt_dot(stack, place)
    places_ref[...] = (found[:received] * LANES + found[received:]).astype(jnp.int32)


def column_table(plan_ref, chunk, number):
    line = pl.ds(chunk, 1)
    column = plan_ref[0, line, :] * HALF + plan_ref[1, line, :] - (number * BLOCK).astype(F32)
    low = plan_ref[2, line, :].astype(BF16)
    high = plan_ref[3, line, :].astype(BF16)
    cells = iota((HALF, LANES), 0).astype(F32).astype(BF16)
    pieces = []
    for begin in range(0, BLOCK, HALF):
        near = jnp.clip(column - begin, -2.0, HALF).astype(BF16)
        after = jnp.clip(column - (begin - 1), -2.0, HALF).astype(BF16)
        pieces.append(jnp.where(cells == near, low, jnp.where(cells == after, high, jnp.zeros((), BF16))))
    return jnp.concatenate(pieces, axis=0)


def row_pattern(plan_ref, chunk, rows, depth):
    line = pl.ds(chunk, 1)
    rf = plan_ref[4, line, :] + plan_ref[5, line, :]
    rel = plan_ref[8, line, :].astype(jnp.int32)
    row = iota((depth, LANES), 0) % rows + 1
    return jnp.where(row == rel, 1.0 - rf, jnp.where(row == rel + 1, rf, 0.0))


def group_chunks(marks_ref, group, keys_group, base):
    count = (marks_ref[1, (group + 1) * keys_group - 1] - base + LANES - 1) // LANES
    return jnp.maximum(count, 1)


def chunk_range(marks_ref, group, number, keys_group, cap_chunks):
    at = group * keys_group + 2 * number
    begin = marks_ref[0, jnp.maximum(at - 1, group * keys_group)]
    end = marks_ref[1, at + 1]
    base = group * cap_chunks
    last = base + group_chunks(marks_ref, group, keys_group, base * LANES) - 1
    return jnp.minimum(begin // LANES, last), jnp.where(end > begin, (end + LANES - 1) // LANES, 0)


def forward_kernel(cap_chunks, blocks, field_ref, plan_ref, marks_ref, value_ref, sums, flat):
    probes, rows, _ = field_ref.shape
    depth = probes * rows
    keys_group = 2 * blocks
    number = pl.program_id(0)
    counts = [group_chunks(marks_ref, g, keys_group, g * cap_chunks * LANES) for g in range(3)]

    @pl.when(number == 0)
    def _():
        for g in range(3):

            @pl.loop(0, counts[g])
            def _(k):
                sums[g * cap_chunks + k] = jnp.zeros((depth, LANES), F32)

    block = field_ref[...].reshape(depth, BLOCK)
    flat[...] = block
    ranges = [chunk_range(marks_ref, g, number, keys_group, cap_chunks) for g in range(3)]
    table = jnp.concatenate([column_table(plan_ref, begin, number) for begin, _ in ranges], axis=1)
    part = jnp.dot(block, table, preferred_element_type=F32)
    for g in range(3):
        sums[ranges[g][0]] += part[:, g * LANES : (g + 1) * LANES]
    for g in range(3):

        @pl.loop(ranges[g][0] + 1, ranges[g][1])
        def _(chunk):
            sums[chunk] += jnp.dot(flat[...], column_table(plan_ref, chunk, number), preferred_element_type=F32)

    @pl.when(number == blocks - 1)
    def _():
        fold = jnp.where(iota((probes, depth), 1) // rows == iota((probes, depth), 0), 1.0, 0.0).astype(BF16)
        for g in range(3):

            @pl.loop(0, counts[g])
            def _(k):
                chunk = g * cap_chunks + k
                scaled = (sums[chunk] * row_pattern(plan_ref, chunk, rows, depth)).astype(BF16)
                value_ref[chunk] = jnp.dot(fold, scaled, preferred_element_type=F32)


def swap_kernel(slabs, top, value_ref, above_ref, below_ref, send_sem, recv_sem):
    probe, me = lax.axis_index("probe"), lax.axis_index("slab")
    width = above_ref.shape[0]
    down, up = lax.rem(me + slabs - 1, slabs), lax.rem(me + 1, slabs)
    barrier = pltpu.get_barrier_semaphore()
    for peer in (down, up):
        pl.semaphore_signal(barrier, inc=1, device_id=(peer, probe), device_id_type=pl.DeviceIdType.MESH)
    pl.semaphore_wait(barrier, 2)
    copies = []
    for k, (peer, begin, target) in enumerate(((down, 0, above_ref), (up, top, below_ref))):
        copies.append(
            pltpu.make_async_remote_copy(
                src_ref=value_ref.at[begin : begin + width],
                dst_ref=target,
                send_sem=send_sem.at[k],
                recv_sem=recv_sem.at[k],
                device_id=(peer, probe),
                device_id_type=pl.DeviceIdType.MESH,
            )
        )
    for copy in copies:
        copy.start()
    for copy in copies:
        copy.wait()


def swap(slabs, cap_chunks, width, number, value):
    part = (width, *value.shape[1:])
    any_space = pl.BlockSpec(memory_space=pl.ANY)
    above, below = pl.pallas_call(
        functools.partial(swap_kernel, slabs, 2 * cap_chunks),
        out_shape=(jax.ShapeDtypeStruct(part, F32), jax.ShapeDtypeStruct(part, F32)),
        in_specs=[any_space],
        out_specs=(any_space, any_space),
        scratch_shapes=[pltpu.SemaphoreType.DMA((2,)), pltpu.SemaphoreType.DMA((2,))],
        compiler_params=pltpu.CompilerParams(collective_id=number, has_side_effects=True),
        name="swap",
    )(value)
    return above, below


def merge_kernel(cap_chunks, blocks, value_ref, above_ref, below_ref, plan_ref, marks_ref, spread_ref, packed_ref, squares, parts):
    slabs = packed_ref.shape[0]
    outgoing, probes, _ = parts.shape
    lines = outgoing // slabs
    keys_group = 2 * blocks
    squares[...] = jnp.zeros_like(squares)
    parts[...] = jnp.zeros_like(parts)
    for g in range(3):
        count = group_chunks(marks_ref, g, keys_group, g * cap_chunks * LANES)

        @pl.loop(0, count)
        def _(k):
            chunk = g * cap_chunks + k
            value = value_ref[chunk]
            if g == 0:
                value = value + below_ref[k]
            if g == 2:
                value = value + above_ref[k]
            line = pl.ds(chunk, 1)
            spread = value * (plan_ref[6, line, :] + plan_ref[7, line, :])
            spread_ref[chunk] = spread.astype(BF16)
            if g > 0:
                squares[...] += spread * value
                high = plan_ref[9, line, :].astype(jnp.int32)
                low = plan_ref[10, line, :].astype(jnp.int32)
                place = jnp.where(iota((LANES, LANES), 0) == low, 1.0, 0.0).astype(BF16)
                stack = jnp.concatenate([jnp.where(high == d, value, 0.0) for d in range(outgoing)], axis=0).astype(BF16)
                parts[...] += nt_dot(stack, place).reshape(outgoing, probes, LANES)

    folded = squares[:8, :]
    for d in range(8, probes, 8):
        folded = folded + squares[d : d + 8, :]
    for d in range(slabs):
        for e in range(lines):
            packed_ref[d, e * probes : (e + 1) * probes, :] = parts[d * lines + e]
        packed_ref[d, lines * probes :, :] = folded


def unpack_kernel(groups, scale, packed_ref, places_ref, observed_ref, mean_ref, traces, send_sem, recv_sem):
    slab, me = lax.axis_index("slab"), lax.axis_index("probe")
    slabs = packed_ref.shape[0]
    probes, owned = observed_ref.shape
    lines = places_ref.shape[0] // slabs
    barrier = pltpu.get_barrier_semaphore()
    for k in range(1, groups):
        peer = lax.rem(me + k, groups)
        pl.semaphore_signal(barrier, inc=1, device_id=(slab, peer), device_id_type=pl.DeviceIdType.MESH)
    own = packed_ref[0, lines * probes :, :]
    for d in range(1, slabs):
        own = own + packed_ref[d, lines * probes :, :]
    traces[me] = own
    pl.semaphore_wait(barrier, groups - 1)

    def tile(k, source, peer):
        return pltpu.make_async_remote_copy(
            src_ref=traces.at[me],
            dst_ref=traces.at[source],
            send_sem=send_sem.at[k],
            recv_sem=recv_sem.at[k],
            device_id=(slab, peer),
            device_id_type=pl.DeviceIdType.MESH,
        )

    for k in range(1, groups):
        tile(k, me, lax.rem(me + k, groups)).start()
    total = jnp.zeros((probes, owned), F32)
    for d in range(slabs):
        for e in range(lines):
            at = d * lines + e
            place = jnp.where(iota((owned, LANES), 0) == places_ref[at : at + 1, :], 1.0, 0.0).astype(BF16)
            total = total + nt_dot(packed_ref[d, e * probes : (e + 1) * probes, :].astype(BF16), place)
    observed_ref[...] = total
    for k in range(1, groups):
        source = lax.rem(me + groups - k, groups)
        tile(k, source, source).wait()
    summed = jnp.sum(jnp.sum(traces[...], axis=0), axis=0, keepdims=True)
    mean_ref[...] = jnp.broadcast_to(jnp.sum(summed, axis=1, keepdims=True) * scale, mean_ref.shape)


def adjoint_kernel(cap_chunks, blocks, spread_ref, plan_ref, marks_ref, out_ref, sources, total):
    probes, rows, _ = out_ref.shape
    depth = probes * rows
    keys_group = 2 * blocks
    number = pl.program_id(0)

    @pl.when(number == 0)
    def _():
        raise_rows = jnp.where(iota((depth, probes), 0) // rows == iota((depth, probes), 1), 1.0, 0.0).astype(BF16)
        for g in range(3):
            count = group_chunks(marks_ref, g, keys_group, g * cap_chunks * LANES)

            @pl.loop(0, count)
            def _(k):
                chunk = g * cap_chunks + k
                raised = jnp.dot(raise_rows, spread_ref[chunk], preferred_element_type=F32)
                sources[chunk] = (raised * row_pattern(plan_ref, chunk, rows, depth)).astype(BF16)

    ranges = [chunk_range(marks_ref, g, number, keys_group, cap_chunks) for g in range(3)]
    table = jnp.concatenate([column_table(plan_ref, begin, number) for begin, _ in ranges], axis=1)
    source = jnp.concatenate([sources[begin] for begin, _ in ranges], axis=1)
    total[...] = nt_dot(source, table)
    for g in range(3):

        @pl.loop(ranges[g][0] + 1, ranges[g][1])
        def _(chunk):
            total[...] += nt_dot(sources[chunk], column_table(plan_ref, chunk, number))

    out_ref[...] = total[...].astype(BF16).reshape(probes, rows, BLOCK)


def general(slab_count, probe_groups, probe_fields, sensor_rows, sensor_cols, row_frac, col_frac, sensor_weights, owner_order):
    probes, rows, width = probe_fields.shape
    sensors = sensor_rows.shape[0]
    depth = probes * rows
    lines = sensors // LANES
    blocks = width // BLOCK
    keys = 6 * blocks
    most = min(sensors, 4 * sensors // slab_count)
    cap_chunks = -(-most // (8 * LANES)) * 8
    chunks = 3 * cap_chunks
    pair_lines = -(-most // (slab_count * LANES))
    outgoing = slab_count * pair_lines
    me = jnp.reshape(lax.axis_index("slab"), (1,)).astype(jnp.int32)
    boxed = [x.reshape(lines, LANES) for x in (sensor_rows, sensor_cols, row_frac, col_frac, sensor_weights, owner_order)]
    vmem = pl.BlockSpec(memory_space=VMEM)
    smem = pl.BlockSpec(memory_space=SMEM)
    plan, marks, places, peak = pl.pallas_call(
        functools.partial(plan_kernel, rows, cap_chunks, blocks, slab_count, pair_lines),
        out_shape=(
            jax.ShapeDtypeStruct((FIELDS, chunks, LANES), F32),
            jax.ShapeDtypeStruct((2, -(-keys // LANES) * LANES), jnp.int32),
            jax.ShapeDtypeStruct((outgoing, LANES), jnp.int32),
            jax.ShapeDtypeStruct((1,), jnp.int32),
        ),
        in_specs=[smem] + [vmem] * 6,
        out_specs=(vmem, vmem, vmem, smem),
        compiler_params=LIMIT,
        name="plan",
    )(me, *boxed)
    value = pl.pallas_call(
        functools.partial(forward_kernel, cap_chunks, blocks),
        out_shape=jax.ShapeDtypeStruct((chunks, probes, LANES), F32),
        grid=(blocks,),
        in_specs=[pl.BlockSpec((probes, rows, BLOCK), lambda n: (0, 0, n)), vmem, smem],
        out_specs=vmem,
        scratch_shapes=[VMEM((chunks, depth, LANES), F32), VMEM((depth, BLOCK), BF16)],
        compiler_params=LIMIT,
        name="forward",
    )(probe_fields, plan, marks)
    few = min(cap_chunks, -(-5 * most // (4 * rows * LANES)))

    def merged(above, below):
        return pl.pallas_call(
            functools.partial(merge_kernel, cap_chunks, blocks),
            out_shape=(
                jax.ShapeDtypeStruct((chunks, probes, LANES), BF16),
                jax.ShapeDtypeStruct((slab_count, pair_lines * probes + 8, LANES), F32),
            ),
            in_specs=[vmem, vmem, vmem, vmem, smem],
            out_specs=(vmem, vmem),
            scratch_shapes=[VMEM((probes, LANES), F32), VMEM((outgoing, probes, LANES), F32)],
            compiler_params=LIMIT,
            name="merge",
        )(value, above, below, plan, marks)

    spread, packed = lax.cond(
        peak[0] <= few * LANES,
        lambda: merged(*swap(slab_count, cap_chunks, few, 0, value)),
        lambda: merged(*swap(slab_count, cap_chunks, cap_chunks, 1, value)),
    )
    arrived = lax.all_to_all(packed, "slab", 0, 0, tiled=True)
    adjoint = pl.pallas_call(
        functools.partial(adjoint_kernel, cap_chunks, blocks),
        out_shape=jax.ShapeDtypeStruct((probes, rows, width), BF16),
        grid=(blocks,),
        in_specs=[vmem, vmem, smem],
        out_specs=pl.BlockSpec((probes, rows, BLOCK), lambda n: (0, 0, n)),
        scratch_shapes=[
            VMEM((chunks, depth, LANES), BF16),
            VMEM((depth, BLOCK), F32),
        ],
        compiler_params=LIMIT,
        cost_estimate=pl.CostEstimate(flops=4 * 10**9, bytes_accessed=8 * 10**6, transcendentals=0),
        name="adjoint",
    )(spread, plan, marks)
    observed, mean = pl.pallas_call(
        functools.partial(unpack_kernel, probe_groups, 1.0 / (probes * probe_groups * sensors)),
        out_shape=(
            jax.ShapeDtypeStruct((probes, sensors // slab_count), F32),
            jax.ShapeDtypeStruct((1, LANES), F32),
        ),
        in_specs=[vmem, vmem],
        out_specs=(vmem, vmem),
        scratch_shapes=[
            VMEM((probe_groups, 8, LANES), F32),
            pltpu.SemaphoreType.DMA((probe_groups,)),
            pltpu.SemaphoreType.DMA((probe_groups,)),
        ],
        compiler_params=pltpu.CompilerParams(collective_id=2, has_side_effects=True, vmem_limit_bytes=40 * 1024 * 1024),
        name="unpack",
    )(arrived, places)
    return adjoint, observed, mean[0, 0]


COLS = 256
FAST = 11
ROOM = 28 * 1024 * 1024
SMALL = pltpu.CompilerParams(vmem_limit_bytes=ROOM)


class Geo(typing.NamedTuple):
    rows: int
    probes: int
    slabs: int
    groups: int
    buckets: int
    tiles: int
    lines: int
    owned: int
    quarter: int
    edge_lines: int
    kinds: int


def bf(x):
    return x.astype(BF16)


def cells(rows, width):
    return bf(iota((rows, width), 0).astype(F32))


def match(rows, target):
    grid = cells(min(rows, COLS), target.shape[1])
    pieces = []
    for begin in range(0, rows, COLS):
        size = min(COLS, rows - begin)
        near = bf(jnp.clip(target - begin, -1.0, float(COLS)))
        pieces.append(jnp.where(grid[:size] == near, jnp.ones((), BF16), jnp.zeros((), BF16)))
    return pieces[0] if len(pieces) == 1 else jnp.concatenate(pieces, axis=0)


def observe_kernel(geo, me_ref, r_ref, c_ref, rf_ref, cf_ref, w_ref, order_ref, field_ref, plan_ref, slot_ref, flag_ref, value_ref, tiles, hots, ranks, fold, sem):
    lines, slabs, buckets, owned = geo.lines, geo.slabs, geo.buckets, geo.owned
    loads = 8
    rounds = geo.tiles // loads

    def load(g, j):
        t = g * loads + j
        return pltpu.make_async_copy(field_ref.at[:, t], tiles.at[t], sem.at[g])

    for g in reversed(range(rounds)):
        for j in range(loads):
            load(g, j).start()

    me = me_ref[0]
    step = min(4, lines)
    kinds = geo.kinds

    def wide(x, i):
        return jnp.concatenate([x[i + j : i + j + 1, :] for j in range(step)], axis=1)

    order = order_ref[...]
    slot = iota((lines, LANES), 0) * LANES + iota((lines, LANES), 1)
    order_hi, order_lo = bf((order >> 7).astype(F32)), bf((order & 127).astype(F32))
    order_hi, order_lo = order_hi.astype(F32), order_lo.astype(F32)
    mine_hi, mine_lo = (slot >> 7).astype(F32), (slot & 127).astype(F32)
    found = jnp.zeros((2 * lines, LANES), F32)
    line_cells, lane_cells = cells(lines, step * LANES), cells(LANES, step * LANES)
    zero, one = jnp.zeros((), BF16), jnp.ones((), BF16)
    for i in range(0, lines, step):
        here = line_cells == bf(wide(order_hi, i))
        stack = jnp.concatenate([jnp.where(here, bf(wide(mine_hi, i)), zero), jnp.where(here, bf(wide(mine_lo, i)), zero)], axis=0)
        place = jnp.where(lane_cells == bf(wide(order_lo, i)), one, zero)
        found = found + nt_dot(stack, place)
    slot_of = (found[:lines] * LANES + found[lines:]).astype(jnp.int32)

    r = r_ref[...]
    c = c_ref[...]
    rel = r - me * geo.rows + 1
    valid = (rel >= 0) & (rel <= geo.rows)
    bucket = c // COLS
    owner = slot_of // owned
    home = r // geo.rows
    edge = r - home * geo.rows == geo.rows - 1
    key = jnp.where(valid, bucket, -1)
    send_key = jnp.where(valid, owner, -1)
    first_key = jnp.where(owner == me, home, -1)
    second_key = jnp.where((owner == me) & edge, home + 1, -1)
    edge_key = jnp.where(valid & (rel == 0), 0, jnp.where(valid & (rel == geo.rows), 1, -1))

    def hot_of(i):
        line = slice(i, i + 1)
        recv = iota((slabs, LANES), 0)
        return (
            iota((buckets, LANES), 0) == key[line],
            recv == send_key[line],
            recv == first_key[line],
            recv == second_key[line],
            iota((16, LANES), 0) == edge_key[line],
        )

    for i in range(lines):
        a, b, c1, c2, d = hot_of(i)
        hot = jnp.concatenate([jnp.where(x, 1.0, 0.0) for x in (a, b, c1 | c2, d)], axis=0)
        hots[i * kinds : (i + 1) * kinds, :] = bf(hot)
    upper = iota((LANES, 2 * LANES), 0) < iota((LANES, 2 * LANES), 1)
    upper = bf(jnp.where(upper, 1.0, 0.0))
    before = jnp.dot(hots[...], upper, preferred_element_type=F32)
    carry = jnp.zeros((kinds, LANES), F32)
    for i in range(lines):
        part = before[i * kinds : (i + 1) * kinds]
        rank = part[:, :LANES] + carry
        a, b, c1, c2, d = hot_of(i)
        recv = rank[buckets + slabs : buckets + 2 * slabs]
        picks = (
            (a, rank[:buckets]),
            (b, rank[buckets : buckets + slabs]),
            (c1, recv),
            (c2, recv),
            (d, rank[buckets + 2 * slabs :]),
        )
        for k, (mask, value) in enumerate(picks):
            ranks[k, i : i + 1, :] = jnp.sum(jnp.where(mask, value, 0.0), axis=0, keepdims=True)
        carry = carry + part[:, LANES:]
    capacity = 4.0 * geo.quarter
    row = iota((kinds, LANES), 0)
    limit = jnp.where(row < buckets, float(LANES), jnp.where(row < buckets + 2 * slabs, capacity, float(geo.edge_lines * LANES)))
    over = jnp.sum(jnp.where(carry > limit, 1.0, 0.0), axis=0, keepdims=True)
    flag_ref[...] = jnp.broadcast_to(over, flag_ref.shape)

    spot, send, recv1, recv2, swap = (ranks[k] for k in range(5))
    rf, cf, w = rf_ref[...], cf_ref[...], w_ref[...]
    rf_top, w_top = bf(rf).astype(F32), bf(w).astype(F32)
    send_quarter = jnp.floor((send + 0.5) * (1.0 / geo.quarter))
    swap_line = jnp.floor((swap + 0.5) * (1.0 / LANES))
    values = (
        (c - bucket * COLS).astype(F32),
        bf(1.0 - cf).astype(F32),
        bf(cf).astype(F32),
        rf_top,
        rf - rf_top,
        w_top,
        w - w_top,
        (rel + 1 + 8 * owner).astype(F32),
        send - send_quarter * geo.quarter,
        jnp.minimum(send_quarter, 15.0) + 16.0 * jnp.minimum(jnp.where(edge_key >= 0, swap_line, 0.0), 15.0),
        swap - swap_line * LANES,
    )
    key_value = jnp.where(valid & (spot < LANES), bucket, -1).astype(F32)
    bucket_cells = cells(buckets, step * LANES)
    total = jnp.zeros((FAST * buckets, LANES), F32)
    for i in range(0, lines, step):
        here = bucket_cells == bf(wide(key_value, i))
        stack = jnp.concatenate([jnp.where(here, bf(wide(v, i)), zero) for v in values], axis=0)
        place = jnp.where(lane_cells == bf(jnp.minimum(wide(spot, i), 255.0)), one, zero)
        total = total + nt_dot(stack, place)
    for f in range(FAST):
        plan_ref[f] = total[f * buckets : (f + 1) * buckets, :]

    sent = slabs * geo.quarter

    def position(rank, source, use):
        quarter = jnp.floor((rank + 0.5) * (1.0 / geo.quarter))
        place = quarter * sent + source.astype(F32) * geo.quarter + (rank - quarter * geo.quarter)
        return jnp.where(use, place, 4.0 * sent + 8.0)

    here_slot = slot_of - me * owned
    owned_lines = owned // LANES
    slot_line = jnp.where(owner == me, here_slot >> 7, -1).astype(F32)
    slot_lane = (here_slot & 127).astype(F32)
    fields = []
    for place in (position(recv1, home, owner == me), position(recv2, home + 1, edge)):
        high = jnp.floor(place * (1.0 / 64.0))
        fields += [high, place - 64.0 * high]
    slot_cells = cells(owned_lines, step * LANES)
    pad = -(4 * owned_lines) % 16
    placed = jnp.zeros((4 * owned_lines + pad, LANES), F32)
    for i in range(0, lines, step):
        here = jnp.broadcast_to(wide(slot_line, i), (owned_lines, step * LANES)) == iota((owned_lines, step * LANES), 0).astype(F32)
        stack = [jnp.where(here, wide(v, i), 0.0) for v in fields]
        if pad:
            stack.append(jnp.zeros((pad, step * LANES), F32))
        place = jnp.where(lane_cells == bf(wide(slot_lane, i)), one, zero)
        placed = placed + nt_dot(bf(jnp.concatenate(stack, axis=0)), place)
    for f in range(2):
        at = 2 * f * owned_lines
        slot_ref[f] = placed[at : at + owned_lines] * 64.0 + placed[at + owned_lines : at + 2 * owned_lines]

    depth = geo.rows * geo.probes
    spill = None
    batch = loads // 2
    for g in reversed(range(rounds)):
        for j in range(loads):
            load(g, j).wait()
        group = list(reversed(range(g * batch, (g + 1) * batch)))
        parts = []
        for b in group:
            block = jnp.concatenate([tiles[2 * b].reshape(depth, LANES), tiles[2 * b + 1].reshape(depth, LANES)], axis=1)
            parts.append(jnp.dot(block, bucket_table(plan_ref, b), preferred_element_type=F32))
        for b, part in zip(group, parts):
            value = part[:, :LANES]
            if spill is not None:
                value = value + spill
            spill = part[:, LANES:]
            fold[b] = value
            terms = [fold[b, pl.ds(k, geo.probes, stride=geo.rows), :] * x for k, x in enumerate(row_weights(geo, plan_ref, b))]
            value_ref[b] = functools.reduce(jnp.add, terms)


def bucket_table(plan_ref, b):
    near, low, high = (plan_ref[f, pl.ds(b, 1), :] for f in range(3))
    grid = cells(COLS, LANES)
    zero = jnp.zeros((), BF16)
    main = jnp.where(grid == bf(near), bf(low), jnp.where(grid == bf(near + 1.0), bf(high), zero))
    if isinstance(b, int) and b == 0:
        return jnp.concatenate([main, jnp.zeros((COLS, LANES), BF16)], axis=1)
    before = b - 1 if isinstance(b, int) else jnp.maximum(b - 1, 0)
    last, spill = (plan_ref[f, pl.ds(before, 1), :] for f in (0, 2))
    spill = jnp.where(last == COLS - 1.0, spill, 0.0)
    over = bf(jnp.where(iota((16, LANES), 0) == 0, spill, 0.0))
    over = jnp.concatenate([over, jnp.zeros((COLS - 16, LANES), BF16)], axis=0)
    return jnp.concatenate([main, over], axis=1)


def place_code(plan_ref, b):
    code = plan_ref[7, pl.ds(b, 1), :]
    owner = jnp.floor(code * 0.125)
    return owner, code - 8.0 * owner


def row_weights(geo, plan_ref, b):
    rf = plan_ref[3, pl.ds(b, 1), :] + plan_ref[4, pl.ds(b, 1), :]
    _, rel = place_code(plan_ref, b)
    return [jnp.where(rel == k + 2.0, 1.0 - rf, jnp.where(rel == k + 1.0, rf, 0.0)) for k in range(geo.rows)]


def exchange_kernel(geo, value_ref, plan_ref, flag_ref, adjoint_ref, arrived_ref, total_ref, ok_ref, edges, places, shares, inbox, packed, sources, raised, tiles, sums, swap_send, swap_recv, owner_send, owner_recv, tile_send, tile_recv, sum_send, sum_recv):
    slabs, groups, probes, rows, quarter, buckets = geo.slabs, geo.groups, geo.probes, geo.rows, geo.quarter, geo.buckets
    me, mine = lax.axis_index("slab"), lax.axis_index("probe")
    lines = geo.edge_lines
    zero = jnp.zeros((), BF16)
    batch = 8

    def at(slab, probe):
        return dict(device_id=(slab, probe), device_id_type=pl.DeviceIdType.MESH)

    barrier = pltpu.get_barrier_semaphore()
    for k in range(1, slabs):
        pl.semaphore_signal(barrier, inc=1, **at(lax.rem(me + k, slabs), mine))
    for k in range(1, groups):
        pl.semaphore_signal(barrier, inc=1, **at(me, lax.rem(mine + k, groups)))

    def columns(j):
        return slice(j * LANES, (j + 1) * LANES)

    def edge_fields(b):
        _, rel = place_code(plan_ref, b)
        line = jnp.floor(plan_ref[9, pl.ds(b, 1), :] * (1.0 / 16.0))
        lane = plan_ref[10, pl.ds(b, 1), :]
        return rel, line, lane

    def weight_of(b):
        return plan_ref[5, pl.ds(b, 1), :] + plan_ref[6, pl.ds(b, 1), :]

    edges[...] = jnp.zeros_like(edges)
    shares[...] = jnp.zeros_like(shares)
    share_rows = shares.shape[0]

    @pl.loop(0, buckets // batch)
    def _(g):
        stacks, spots = [], []
        for j in range(batch):
            b = g * batch + j
            rel, line, lane = edge_fields(b)
            low, high = rel == 1.0, rel == rows + 1.0
            spot = match(2 * LANES, jnp.where(low, lane, jnp.where(high, lane + LANES, -1.0)))
            value = value_ref[b]
            share = jnp.where((iota((share_rows, LANES), 0).astype(F32) == line) & high, weight_of(b), 0.0)
            stacks.append(jnp.concatenate([bf(jnp.where(line == float(l), value, 0.0)) for l in range(lines)] + [bf(share)], axis=0))
            spots.append(spot)
            places[b] = spot
        part = nt_dot(jnp.concatenate(stacks, axis=1), jnp.concatenate(spots, axis=1))
        for side in range(2):
            edges[side] += part[: lines * probes, columns(side)]
        shares[...] += part[lines * probes :, columns(1)]

    pl.semaphore_wait(barrier, slabs + groups - 2)
    down, up = lax.rem(me + slabs - 1, slabs), lax.rem(me + 1, slabs)
    swaps = [
        pltpu.make_async_remote_copy(
            src_ref=edges.at[side], dst_ref=inbox.at[1 - side], send_sem=swap_send.at[side], recv_sem=swap_recv.at[side], **at(peer, mine)
        )
        for side, peer in ((0, down), (1, up))
    ]
    for copy in swaps:
        copy.start()

    packed[...] = jnp.zeros_like(packed)

    def pack(g, squares):
        hots, quads = [], []
        for j in range(batch):
            b = g * batch + j
            owner, rel = place_code(plan_ref, b)
            code = plan_ref[9, pl.ds(b, 1), :]
            fourth = code - 16.0 * jnp.floor(code * (1.0 / 16.0))
            row = jnp.where(rel > 0.0, owner * quarter + plan_ref[8, pl.ds(b, 1), :], -1.0)
            hots.append(match(slabs * quarter, row))
            value = value_ref[b]
            squares = squares + value * value * weight_of(b)
            quads.append(jnp.concatenate([bf(jnp.where(fourth == float(k), value, 0.0)) for k in range(4)], axis=0))
        part = nt_dot(jnp.concatenate(hots, axis=1), jnp.concatenate(quads, axis=1))
        packed[...] += part.reshape(packed.shape)
        return squares

    squares = lax.fori_loop(0, buckets // batch, pack, jnp.zeros((probes, LANES), F32))

    def owner_copy(k, source, peer):
        return pltpu.make_async_remote_copy(
            src_ref=packed.at[peer], dst_ref=arrived_ref.at[source], send_sem=owner_send.at[k], recv_sem=owner_recv.at[k], **at(peer, mine)
        )

    for k in range(1, slabs):
        owner_copy(k, me, lax.rem(me + k, slabs)).start()
    arrived_ref[me] = packed[me]

    for copy in swaps:
        copy.wait()
    for l in range(lines):
        part = slice(l * probes, (l + 1) * probes)
        squares = squares + edges[1, part] * inbox[1, part] * (2.0 * shares[l : l + 1])
    folded = squares[:8]
    for d in range(8, probes, 8):
        folded = folded + squares[d : d + 8]
    tiles[mine] = jnp.concatenate([folded, flag_ref[...]], axis=0)

    def tile_copy(k, source, peer):
        return pltpu.make_async_remote_copy(
            src_ref=tiles.at[mine], dst_ref=tiles.at[source], send_sem=tile_send.at[k], recv_sem=tile_recv.at[k], **at(me, peer)
        )

    for k in range(1, groups):
        tile_copy(k, mine, lax.rem(mine + k, groups)).start()

    both = bf(jnp.concatenate([inbox[0], inbox[1]], axis=1))
    sources[0] = jnp.zeros_like(sources[0])

    @pl.loop(0, buckets // batch)
    def _(g):
        spots = jnp.concatenate([places[g * batch + j] for j in range(batch)], axis=1)
        extra = jnp.dot(both, spots, preferred_element_type=F32)
        for j in range(batch):
            b = g * batch + j
            _, line, _ = edge_fields(b)
            full = value_ref[b]
            for l in range(lines):
                full = full + jnp.where(line == float(l), extra[l * probes : (l + 1) * probes, columns(j)], 0.0)
            spread = full * weight_of(b)
            for k, weight in enumerate(row_weights(geo, plan_ref, b)):
                raised[j, pl.ds(k, probes, stride=rows), :] = spread * weight
            sources[b + 1] = bf(raised[j])

    @pl.loop(0, buckets // batch)
    def _(g):
        parts = []
        for j in range(batch):
            b = g * batch + j
            source = jnp.concatenate([sources[b + 1], sources[b]], axis=1)
            parts.append(nt_dot(source, bucket_table(plan_ref, b)))
        for j in range(batch):
            for t in range(2):
                adjoint_ref[2 * (g * batch + j) + t] = bf(parts[j][:, columns(t)]).reshape(probes, rows, LANES)

    for k in range(1, groups):
        source = lax.rem(mine + groups - k, groups)
        tile_copy(k, source, source).wait()
    sums[me] = jnp.sum(tiles[...], axis=0)

    def sum_copy(k, source, peer):
        return pltpu.make_async_remote_copy(
            src_ref=sums.at[me], dst_ref=sums.at[source], send_sem=sum_send.at[k], recv_sem=sum_recv.at[k], **at(peer, mine)
        )

    for k in range(1, slabs):
        sum_copy(k, me, lax.rem(me + k, slabs)).start()
    for k in range(1, slabs):
        source = lax.rem(me + slabs - k, slabs)
        owner_copy(k, source, source).wait()
    for k in range(1, slabs):
        source = lax.rem(me + slabs - k, slabs)
        sum_copy(k, source, source).wait()
    total = jnp.sum(sums[...], axis=0)
    total_ref[...] = total
    ok_ref[0] = jnp.max(total[8:]).astype(jnp.int32)


def deliver_kernel(geo, scale, adjoint_ref, arrived_ref, slot_ref, total_ref, out_ref, observed_ref, mean_ref, observed, sem):
    slabs, probes, quarter, owned = geo.slabs, geo.probes, geo.quarter, geo.owned
    loads = 8

    def store(t):
        return pltpu.make_async_copy(adjoint_ref.at[t], out_ref.at[:, t], sem.at[0])

    for t in range(geo.tiles):
        store(t).start()
    sent = slabs * quarter
    arrived = jnp.transpose(arrived_ref[...].reshape(sent, 4 * probes))
    lines = owned // LANES
    spots = [jnp.concatenate([slot_ref[f, l : l + 1, :] for l in range(lines)], axis=1) for f in range(2)]
    total = jnp.zeros((probes, owned), F32)
    for k in range(4):
        hot = match(sent, spots[0] - float(k * sent)) + match(sent, spots[1] - float(k * sent))
        total = total + jnp.dot(bf(arrived[k * probes : (k + 1) * probes]), hot, preferred_element_type=F32)
    observed[...] = total
    pltpu.make_async_copy(observed, observed_ref, sem.at[1]).start()
    summed = jnp.sum(total_ref[:8], axis=0, keepdims=True)
    mean_ref[...] = jnp.broadcast_to(jnp.sum(summed, axis=1, keepdims=True) * scale, mean_ref.shape)
    pltpu.make_async_copy(observed, observed_ref, sem.at[1]).wait()
    for t in range(geo.tiles):
        store(t).wait()


def geometry(slabs, groups, probe_fields, sensors):
    probes, rows, width = probe_fields.shape
    most = min(sensors, 4 * sensors // slabs)
    quarter = -(-(most // slabs + 32) // 32) * 8
    edge_lines = -(-5 * most // (4 * rows * LANES))
    buckets = width // COLS
    return Geo(rows, probes, slabs, groups, buckets, width // LANES, sensors // LANES, sensors // slabs, quarter, edge_lines, buckets + 2 * slabs + 16)


def body(slab_count, probe_groups, probe_fields, *vectors):
    sensors = vectors[0].shape[0]
    geo = geometry(slab_count, probe_groups, probe_fields, sensors)
    probes, rows, width = probe_fields.shape
    depth = probes * rows
    lines, buckets, tiles = geo.lines, geo.buckets, geo.tiles
    me = jnp.reshape(lax.axis_index("slab"), (1,)).astype(jnp.int32)
    boxed = [x.reshape(lines, LANES) for x in vectors]
    field = probe_fields.reshape(probes, rows, tiles, LANES).transpose(0, 2, 1, 3)
    vmem = pl.BlockSpec(memory_space=VMEM)
    smem = pl.BlockSpec(memory_space=SMEM)
    hbm = pl.BlockSpec(memory_space=pltpu.HBM)
    dma = pltpu.SemaphoreType.DMA
    shape = jax.ShapeDtypeStruct
    plan, slots, flags, value = pl.pallas_call(
        functools.partial(observe_kernel, geo),
        out_shape=(
            shape((FAST, buckets, LANES), F32),
            shape((2, geo.owned // LANES, LANES), F32),
            shape((8, LANES), F32),
            shape((buckets, probes, LANES), F32),
        ),
        in_specs=[smem] + [vmem] * 6 + [hbm],
        out_specs=(vmem,) * 4,
        scratch_shapes=[
            VMEM((tiles, probes, rows, LANES), BF16),
            VMEM((lines * geo.kinds, LANES), BF16),
            VMEM((5, lines, LANES), F32),
            VMEM((buckets, depth, LANES), F32),
            dma((tiles // 8,)),
        ],
        compiler_params=SMALL,
        name="observe",
    )(me, *boxed, field)
    edge_rows = geo.edge_lines * probes
    adjoint, arrived, total, flag = pl.pallas_call(
        functools.partial(exchange_kernel, geo),
        out_shape=(
            shape((tiles, probes, rows, LANES), BF16),
            shape((slab_count, geo.quarter, 4 * probes), F32),
            shape((16, LANES), F32),
            shape((1,), jnp.int32),
        ),
        in_specs=[vmem] * 3,
        out_specs=(vmem, vmem, vmem, smem),
        scratch_shapes=[
            VMEM((2, edge_rows, LANES), F32),
            VMEM((buckets, 2 * LANES, LANES), BF16),
            VMEM((-(-geo.edge_lines // 16) * 16, LANES), F32),
            VMEM((2, edge_rows, LANES), F32),
            VMEM((slab_count, geo.quarter, 4 * probes), F32),
            VMEM((buckets + 1, depth, LANES), BF16),
            VMEM((8, depth, LANES), F32),
            VMEM((probe_groups, 16, LANES), F32),
            VMEM((slab_count, 16, LANES), F32),
            dma((2,)),
            dma((2,)),
            dma((slab_count,)),
            dma((slab_count,)),
            dma((probe_groups,)),
            dma((probe_groups,)),
            dma((slab_count,)),
            dma((slab_count,)),
        ],
        compiler_params=pltpu.CompilerParams(collective_id=3, has_side_effects=True, vmem_limit_bytes=ROOM),
        name="exchange",
    )(value, plan, flags)

    out, observed, mean = pl.pallas_call(
        functools.partial(deliver_kernel, geo, 1.0 / (probes * probe_groups * sensors)),
        out_shape=(
            shape((probes, tiles, rows, LANES), BF16),
            shape((probes, geo.owned), F32),
            shape((1, LANES), F32),
        ),
        in_specs=[vmem] * 4,
        out_specs=(hbm, hbm, vmem),
        scratch_shapes=[VMEM((probes, geo.owned), F32), dma((2,))],
        compiler_params=SMALL,
        name="deliver",
    )(adjoint, arrived, slots, total)
    out = out.transpose(0, 2, 1, 3).reshape(probes, rows, width)

    def again(state):
        out, observed, mean = general(slab_count, probe_groups, probe_fields, *vectors)
        return out, jnp.where(state[3] > 0, observed, state[1]), mean, state[3] * 0

    state = lax.while_loop(lambda state: state[3] != 0, again, (out, observed, mean[0, 0], flag[0]))
    return state[:3]


def solution(mesh):
    placed = (P("probe", "slab", None), P(), P(), P(), P(), P(), P())
    return jax.shard_map(
        functools.partial(body, mesh.shape["slab"], mesh.shape["probe"]),
        mesh=mesh,
        in_specs=placed,
        out_specs=(P("probe", "slab", None), P("probe", "slab"), P()),
        check_vma=False,
    )
```

```python
import functools
import typing

import jax
import jax.numpy as jnp
from jax import lax
from jax.experimental import pallas as pl
from jax.experimental.pallas import tpu as pltpu
from jax.sharding import PartitionSpec as P

LANES = 128
BLOCK = 1024
HALF = 256
FIELDS = 11
F32 = jnp.float32
BF16 = jnp.bfloat16
NT = (((1,), (1,)), ((), ()))
VMEM = pltpu.VMEM
SMEM = pltpu.SMEM
LIMIT = pltpu.CompilerParams(vmem_limit_bytes=60 * 1024 * 1024)


def iota(shape, dim):
    return lax.broadcasted_iota(jnp.int32, shape, dim)


def nt_dot(a, b):
    return lax.dot_general(a, b, NT, preferred_element_type=F32)


def plan_kernel(rows, cap_chunks, blocks, slabs, pair_lines, me_ref, r_ref, c_ref, rf_ref, cf_ref, w_ref, order_ref, plan_ref, marks_ref, places_ref, peak_ref):
    lines = r_ref.shape[0]
    sensors = lines * LANES
    step = min(4, lines)
    me = me_ref[0]
    first = me * rows
    owned = lines * LANES // slabs
    keys_group = 2 * blocks
    keys = 3 * keys_group
    chunks = 3 * cap_chunks

    def wide(x, i):
        return jnp.concatenate([x[i + j : i + j + 1, :] for j in range(step)], axis=1)

    order = order_ref[...]
    slot = iota((lines, LANES), 0) * LANES + iota((lines, LANES), 1)
    found = jnp.zeros((2 * lines, LANES), F32)
    for i in range(0, lines, step):
        target = wide(order, i)
        mine = wide(slot, i)
        here = iota((lines, step * LANES), 0) == (target >> 7)
        stack = jnp.concatenate(
            [jnp.where(here, (mine >> 7).astype(F32), 0.0), jnp.where(here, (mine & 127).astype(F32), 0.0)], axis=0
        ).astype(BF16)
        place = jnp.where(iota((LANES, step * LANES), 0) == (target & 127), 1.0, 0.0).astype(BF16)
        found = found + nt_dot(stack, place)
    slot_hi = found[:lines, :]
    slot_lo = found[lines:, :]

    r = r_ref[...]
    c = c_ref[...]
    rel = r - first + 1
    valid = (rel >= 0) & (rel <= rows)
    group = jnp.where(rel == 0, 0, jnp.where(rel == rows, 2, 1))
    block = c // BLOCK
    inner = c - block * BLOCK
    half = c // HALF
    slot_of = (slot_hi * LANES + slot_lo).astype(jnp.int32)
    owner = slot_of // owned
    home = r // rows
    send_key = jnp.where(home == me, owner, -1)
    recv_key = jnp.where(owner == me, home, -1)
    edge = jnp.where(r - home * rows == rows - 1, home, -1)
    edges = jnp.zeros((slabs, LANES), F32)
    for i in range(lines):
        edges = edges + jnp.where(iota((slabs, LANES), 0) == edge[i : i + 1, :], 1.0, 0.0)
    peak_ref[0] = jnp.max(jnp.sum(edges, axis=1, keepdims=True)).astype(jnp.int32)
    key = group * keys_group + 2 * block + jnp.where(inner == BLOCK - 1, 1, 0)
    key = jnp.where(valid, key, -1)

    count = jnp.zeros((keys, 1), F32)
    for i in range(lines):
        count = count + jnp.sum(jnp.where(iota((keys, LANES), 0) == key[i : i + 1, :], 1.0, 0.0), axis=1, keepdims=True)
    big = jnp.floor(count * (1.0 / 64.0))
    small = count - 64.0 * big
    ka, kb = iota((keys, keys), 0), iota((keys, keys), 1)
    below = jnp.where((kb < ka) & (kb // keys_group == ka // keys_group), 1.0, 0.0).astype(BF16)
    start = 64.0 * jnp.dot(below, jnp.broadcast_to(big, (keys, LANES)).astype(BF16), preferred_element_type=F32)
    start = start + jnp.dot(below, jnp.broadcast_to(small, (keys, LANES)).astype(BF16), preferred_element_type=F32)
    start = start + ((iota((keys, LANES), 0) // keys_group) * (cap_chunks * LANES)).astype(F32)
    wide_keys = marks_ref.shape[1]
    diagonal = iota((keys, wide_keys), 0) == iota((keys, wide_keys), 1)
    marks_ref[...] = jnp.concatenate(
        [jnp.sum(jnp.where(diagonal, x, 0.0), axis=0, keepdims=True) for x in (start[:, :1], start[:, :1] + count)], axis=0
    ).astype(jnp.int32)

    upper = jnp.where(iota((LANES, LANES), 0) < iota((LANES, LANES), 1), 1.0, 0.0).astype(BF16)
    carry = jnp.concatenate([start[:, :1], jnp.zeros((2 * slabs, 1), F32)], axis=0)
    spots, sends, recvs = [], [], []
    for i in range(lines):
        hot = jnp.concatenate(
            [
                jnp.where(iota((keys, LANES), 0) == key[i : i + 1, :], 1.0, 0.0),
                jnp.where(iota((slabs, LANES), 0) == send_key[i : i + 1, :], 1.0, 0.0),
                jnp.where(iota((slabs, LANES), 0) == recv_key[i : i + 1, :], 1.0, 0.0),
            ],
            axis=0,
        )
        before = jnp.dot(hot.astype(BF16), upper, preferred_element_type=F32)
        ranks = hot * (before + carry)
        spots.append(jnp.sum(ranks[:keys], axis=0, keepdims=True))
        sends.append(jnp.sum(ranks[keys : keys + slabs], axis=0, keepdims=True))
        recvs.append(jnp.sum(ranks[keys + slabs :], axis=0, keepdims=True))
        carry = carry + jnp.sum(hot, axis=1, keepdims=True)
    spot = jnp.concatenate(spots, axis=0).astype(jnp.int32)
    spot = jnp.where(valid, spot, -1)
    send = jnp.concatenate(sends, axis=0).astype(jnp.int32)
    recv = jnp.concatenate(recvs, axis=0).astype(jnp.int32)
    send_line = jnp.where(send_key >= 0, owner * pair_lines + (send >> 7), 200)
    recv_line = jnp.where(recv_key >= 0, home * pair_lines + (recv >> 7), -1)

    rf = rf_ref[...]
    cf = cf_ref[...]
    w = w_ref[...]
    rf_top = rf.astype(BF16).astype(F32)
    w_top = w.astype(BF16).astype(F32)
    values = [
        half.astype(F32),
        (c - half * HALF).astype(F32),
        (1.0 - cf).astype(BF16).astype(F32),
        cf.astype(BF16).astype(F32),
        rf_top,
        rf - rf_top,
        w_top,
        w - w_top,
        rel.astype(F32),
        send_line.astype(F32),
        (send & 127).astype(F32),
    ]
    total = jnp.zeros((FIELDS * chunks, LANES), F32)
    for i in range(0, lines, step):
        target = wide(spot, i)
        here = iota((chunks, step * LANES), 0) == (target >> 7)
        stack = jnp.concatenate([jnp.where(here, wide(v, i), 0.0) for v in values], axis=0).astype(BF16)
        place = jnp.where(iota((LANES, step * LANES), 0) == (target & 127), 1.0, 0.0).astype(BF16)
        total = total + nt_dot(stack, place)
    for f in range(FIELDS):
        plan_ref[f] = total[f * chunks : (f + 1) * chunks, :]

    slot_here = slot_of - me * owned
    received = slabs * pair_lines
    found = jnp.zeros((2 * received, LANES), F32)
    for i in range(0, lines, step):
        here = iota((received, step * LANES), 0) == wide(recv_line, i)
        target = wide(slot_here, i)
        stack = jnp.concatenate(
            [jnp.where(here, (target >> 7).astype(F32), 0.0), jnp.where(here, (target & 127).astype(F32), 0.0)], axis=0
        ).astype(BF16)
        place = jnp.where(iota((LANES, step * LANES), 0) == (wide(recv, i) & 127), 1.0, 0.0).astype(BF16)
        found = found + nt_dot(stack, place)
    places_ref[...] = (found[:received] * LANES + found[received:]).astype(jnp.int32)


def column_table(plan_ref, chunk, number):
    line = pl.ds(chunk, 1)
    column = plan_ref[0, line, :] * HALF + plan_ref[1, line, :] - (number * BLOCK).astype(F32)
    low = plan_ref[2, line, :].astype(BF16)
    high = plan_ref[3, line, :].astype(BF16)
    cells = iota((HALF, LANES), 0).astype(F32).astype(BF16)
    pieces = []
    for begin in range(0, BLOCK, HALF):
        near = jnp.clip(column - begin, -2.0, HALF).astype(BF16)
        after = jnp.clip(column - (begin - 1), -2.0, HALF).astype(BF16)
        pieces.append(jnp.where(cells == near, low, jnp.where(cells == after, high, jnp.zeros((), BF16))))
    return jnp.concatenate(pieces, axis=0)


def row_pattern(plan_ref, chunk, rows, depth):
    line = pl.ds(chunk, 1)
    rf = plan_ref[4, line, :] + plan_ref[5, line, :]
    rel = plan_ref[8, line, :].astype(jnp.int32)
    row = iota((depth, LANES), 0) % rows + 1
    return jnp.where(row == rel, 1.0 - rf, jnp.where(row == rel + 1, rf, 0.0))


def group_chunks(marks_ref, group, keys_group, base):
    count = (marks_ref[1, (group + 1) * keys_group - 1] - base + LANES - 1) // LANES
    return jnp.maximum(count, 1)


def chunk_range(marks_ref, group, number, keys_group, cap_chunks):
    at = group * keys_group + 2 * number
    begin = marks_ref[0, jnp.maximum(at - 1, group * keys_group)]
    end = marks_ref[1, at + 1]
    base = group * cap_chunks
    last = base + group_chunks(marks_ref, group, keys_group, base * LANES) - 1
    return jnp.minimum(begin // LANES, last), jnp.where(end > begin, (end + LANES - 1) // LANES, 0)


def forward_kernel(cap_chunks, blocks, field_ref, plan_ref, marks_ref, value_ref, sums, flat):
    probes, rows, _ = field_ref.shape
    depth = probes * rows
    keys_group = 2 * blocks
    number = pl.program_id(0)
    counts = [group_chunks(marks_ref, g, keys_group, g * cap_chunks * LANES) for g in range(3)]

    @pl.when(number == 0)
    def _():
        for g in range(3):

            @pl.loop(0, counts[g])
            def _(k):
                sums[g * cap_chunks + k] = jnp.zeros((depth, LANES), F32)

    block = field_ref[...].reshape(depth, BLOCK)
    flat[...] = block
    ranges = [chunk_range(marks_ref, g, number, keys_group, cap_chunks) for g in range(3)]
    table = jnp.concatenate([column_table(plan_ref, begin, number) for begin, _ in ranges], axis=1)
    part = jnp.dot(block, table, preferred_element_type=F32)
    for g in range(3):
        sums[ranges[g][0]] += part[:, g * LANES : (g + 1) * LANES]
    for g in range(3):

        @pl.loop(ranges[g][0] + 1, ranges[g][1])
        def _(chunk):
            sums[chunk] += jnp.dot(flat[...], column_table(plan_ref, chunk, number), preferred_element_type=F32)

    @pl.when(number == blocks - 1)
    def _():
        fold = jnp.where(iota((probes, depth), 1) // rows == iota((probes, depth), 0), 1.0, 0.0).astype(BF16)
        for g in range(3):

            @pl.loop(0, counts[g])
            def _(k):
                chunk = g * cap_chunks + k
                scaled = (sums[chunk] * row_pattern(plan_ref, chunk, rows, depth)).astype(BF16)
                value_ref[chunk] = jnp.dot(fold, scaled, preferred_element_type=F32)


def swap_kernel(slabs, top, value_ref, above_ref, below_ref, send_sem, recv_sem):
    probe, me = lax.axis_index("probe"), lax.axis_index("slab")
    width = above_ref.shape[0]
    down, up = lax.rem(me + slabs - 1, slabs), lax.rem(me + 1, slabs)
    barrier = pltpu.get_barrier_semaphore()
    for peer in (down, up):
        pl.semaphore_signal(barrier, inc=1, device_id=(peer, probe), device_id_type=pl.DeviceIdType.MESH)
    pl.semaphore_wait(barrier, 2)
    copies = []
    for k, (peer, begin, target) in enumerate(((down, 0, above_ref), (up, top, below_ref))):
        copies.append(
            pltpu.make_async_remote_copy(
                src_ref=value_ref.at[begin : begin + width],
                dst_ref=target,
                send_sem=send_sem.at[k],
                recv_sem=recv_sem.at[k],
                device_id=(peer, probe),
                device_id_type=pl.DeviceIdType.MESH,
            )
        )
    for copy in copies:
        copy.start()
    for copy in copies:
        copy.wait()


def swap(slabs, cap_chunks, width, number, value):
    part = (width, *value.shape[1:])
    any_space = pl.BlockSpec(memory_space=pl.ANY)
    above, below = pl.pallas_call(
        functools.partial(swap_kernel, slabs, 2 * cap_chunks),
        out_shape=(jax.ShapeDtypeStruct(part, F32), jax.ShapeDtypeStruct(part, F32)),
        in_specs=[any_space],
        out_specs=(any_space, any_space),
        scratch_shapes=[pltpu.SemaphoreType.DMA((2,)), pltpu.SemaphoreType.DMA((2,))],
        compiler_params=pltpu.CompilerParams(collective_id=number, has_side_effects=True),
        name="swap",
    )(value)
    return above, below


def merge_kernel(cap_chunks, blocks, value_ref, above_ref, below_ref, plan_ref, marks_ref, spread_ref, packed_ref, squares, parts):
    slabs = packed_ref.shape[0]
    outgoing, probes, _ = parts.shape
    lines = outgoing // slabs
    keys_group = 2 * blocks
    squares[...] = jnp.zeros_like(squares)
    parts[...] = jnp.zeros_like(parts)
    for g in range(3):
        count = group_chunks(marks_ref, g, keys_group, g * cap_chunks * LANES)

        @pl.loop(0, count)
        def _(k):
            chunk = g * cap_chunks + k
            value = value_ref[chunk]
            if g == 0:
                value = value + below_ref[k]
            if g == 2:
                value = value + above_ref[k]
            line = pl.ds(chunk, 1)
            spread = value * (plan_ref[6, line, :] + plan_ref[7, line, :])
            spread_ref[chunk] = spread.astype(BF16)
            if g > 0:
                squares[...] += spread * value
                high = plan_ref[9, line, :].astype(jnp.int32)
                low = plan_ref[10, line, :].astype(jnp.int32)
                place = jnp.where(iota((LANES, LANES), 0) == low, 1.0, 0.0).astype(BF16)
                stack = jnp.concatenate([jnp.where(high == d, value, 0.0) for d in range(outgoing)], axis=0).astype(BF16)
                parts[...] += nt_dot(stack, place).reshape(outgoing, probes, LANES)

    folded = squares[:8, :]
    for d in range(8, probes, 8):
        folded = folded + squares[d : d + 8, :]
    for d in range(slabs):
        for e in range(lines):
            packed_ref[d, e * probes : (e + 1) * probes, :] = parts[d * lines + e]
        packed_ref[d, lines * probes :, :] = folded


def unpack_kernel(groups, scale, packed_ref, places_ref, observed_ref, mean_ref, traces, send_sem, recv_sem):
    slab, me = lax.axis_index("slab"), lax.axis_index("probe")
    slabs = packed_ref.shape[0]
    probes, owned = observed_ref.shape
    lines = places_ref.shape[0] // slabs
    barrier = pltpu.get_barrier_semaphore()
    for k in range(1, groups):
        peer = lax.rem(me + k, groups)
        pl.semaphore_signal(barrier, inc=1, device_id=(slab, peer), device_id_type=pl.DeviceIdType.MESH)
    own = packed_ref[0, lines * probes :, :]
    for d in range(1, slabs):
        own = own + packed_ref[d, lines * probes :, :]
    traces[me] = own
    pl.semaphore_wait(barrier, groups - 1)

    def tile(k, source, peer):
        return pltpu.make_async_remote_copy(
            src_ref=traces.at[me],
            dst_ref=traces.at[source],
            send_sem=send_sem.at[k],
            recv_sem=recv_sem.at[k],
            device_id=(slab, peer),
            device_id_type=pl.DeviceIdType.MESH,
        )

    for k in range(1, groups):
        tile(k, me, lax.rem(me + k, groups)).start()
    total = jnp.zeros((probes, owned), F32)
    for d in range(slabs):
        for e in range(lines):
            at = d * lines + e
            place = jnp.where(iota((owned, LANES), 0) == places_ref[at : at + 1, :], 1.0, 0.0).astype(BF16)
            total = total + nt_dot(packed_ref[d, e * probes : (e + 1) * probes, :].astype(BF16), place)
    observed_ref[...] = total
    for k in range(1, groups):
        source = lax.rem(me + groups - k, groups)
        tile(k, source, source).wait()
    summed = jnp.sum(jnp.sum(traces[...], axis=0), axis=0, keepdims=True)
    mean_ref[...] = jnp.broadcast_to(jnp.sum(summed, axis=1, keepdims=True) * scale, mean_ref.shape)


def adjoint_kernel(cap_chunks, blocks, spread_ref, plan_ref, marks_ref, out_ref, sources, total):
    probes, rows, _ = out_ref.shape
    depth = probes * rows
    keys_group = 2 * blocks
    number = pl.program_id(0)

    @pl.when(number == 0)
    def _():
        raise_rows = jnp.where(iota((depth, probes), 0) // rows == iota((depth, probes), 1), 1.0, 0.0).astype(BF16)
        for g in range(3):
            count = group_chunks(marks_ref, g, keys_group, g * cap_chunks * LANES)

            @pl.loop(0, count)
            def _(k):
                chunk = g * cap_chunks + k
                raised = jnp.dot(raise_rows, spread_ref[chunk], preferred_element_type=F32)
                sources[chunk] = (raised * row_pattern(plan_ref, chunk, rows, depth)).astype(BF16)

    ranges = [chunk_range(marks_ref, g, number, keys_group, cap_chunks) for g in range(3)]
    table = jnp.concatenate([column_table(plan_ref, begin, number) for begin, _ in ranges], axis=1)
    source = jnp.concatenate([sources[begin] for begin, _ in ranges], axis=1)
    total[...] = nt_dot(source, table)
    for g in range(3):

        @pl.loop(ranges[g][0] + 1, ranges[g][1])
        def _(chunk):
            total[...] += nt_dot(sources[chunk], column_table(plan_ref, chunk, number))

    out_ref[...] = total[...].astype(BF16).reshape(probes, rows, BLOCK)


def general(slab_count, probe_groups, probe_fields, sensor_rows, sensor_cols, row_frac, col_frac, sensor_weights, owner_order):
    probes, rows, width = probe_fields.shape
    sensors = sensor_rows.shape[0]
    depth = probes * rows
    lines = sensors // LANES
    blocks = width // BLOCK
    keys = 6 * blocks
    most = min(sensors, 4 * sensors // slab_count)
    cap_chunks = -(-most // (8 * LANES)) * 8
    chunks = 3 * cap_chunks
    pair_lines = -(-most // (slab_count * LANES))
    outgoing = slab_count * pair_lines
    me = jnp.reshape(lax.axis_index("slab"), (1,)).astype(jnp.int32)
    boxed = [x.reshape(lines, LANES) for x in (sensor_rows, sensor_cols, row_frac, col_frac, sensor_weights, owner_order)]
    vmem = pl.BlockSpec(memory_space=VMEM)
    smem = pl.BlockSpec(memory_space=SMEM)
    plan, marks, places, peak = pl.pallas_call(
        functools.partial(plan_kernel, rows, cap_chunks, blocks, slab_count, pair_lines),
        out_shape=(
            jax.ShapeDtypeStruct((FIELDS, chunks, LANES), F32),
            jax.ShapeDtypeStruct((2, -(-keys // LANES) * LANES), jnp.int32),
            jax.ShapeDtypeStruct((outgoing, LANES), jnp.int32),
            jax.ShapeDtypeStruct((1,), jnp.int32),
        ),
        in_specs=[smem] + [vmem] * 6,
        out_specs=(vmem, vmem, vmem, smem),
        compiler_params=LIMIT,
        name="plan",
    )(me, *boxed)
    value = pl.pallas_call(
        functools.partial(forward_kernel, cap_chunks, blocks),
        out_shape=jax.ShapeDtypeStruct((chunks, probes, LANES), F32),
        grid=(blocks,),
        in_specs=[pl.BlockSpec((probes, rows, BLOCK), lambda n: (0, 0, n)), vmem, smem],
        out_specs=vmem,
        scratch_shapes=[VMEM((chunks, depth, LANES), F32), VMEM((depth, BLOCK), BF16)],
        compiler_params=LIMIT,
        name="forward",
    )(probe_fields, plan, marks)
    few = min(cap_chunks, -(-5 * most // (4 * rows * LANES)))

    def merged(above, below):
        return pl.pallas_call(
            functools.partial(merge_kernel, cap_chunks, blocks),
            out_shape=(
                jax.ShapeDtypeStruct((chunks, probes, LANES), BF16),
                jax.ShapeDtypeStruct((slab_count, pair_lines * probes + 8, LANES), F32),
            ),
            in_specs=[vmem, vmem, vmem, vmem, smem],
            out_specs=(vmem, vmem),
            scratch_shapes=[VMEM((probes, LANES), F32), VMEM((outgoing, probes, LANES), F32)],
            compiler_params=LIMIT,
            name="merge",
        )(value, above, below, plan, marks)

    spread, packed = lax.cond(
        peak[0] <= few * LANES,
        lambda: merged(*swap(slab_count, cap_chunks, few, 0, value)),
        lambda: merged(*swap(slab_count, cap_chunks, cap_chunks, 1, value)),
    )
    arrived = lax.all_to_all(packed, "slab", 0, 0, tiled=True)
    adjoint = pl.pallas_call(
        functools.partial(adjoint_kernel, cap_chunks, blocks),
        out_shape=jax.ShapeDtypeStruct((probes, rows, width), BF16),
        grid=(blocks,),
        in_specs=[vmem, vmem, smem],
        out_specs=pl.BlockSpec((probes, rows, BLOCK), lambda n: (0, 0, n)),
        scratch_shapes=[
            VMEM((chunks, depth, LANES), BF16),
            VMEM((depth, BLOCK), F32),
        ],
        compiler_params=LIMIT,
        cost_estimate=pl.CostEstimate(flops=4 * 10**9, bytes_accessed=8 * 10**6, transcendentals=0),
        name="adjoint",
    )(spread, plan, marks)
    observed, mean = pl.pallas_call(
        functools.partial(unpack_kernel, probe_groups, 1.0 / (probes * probe_groups * sensors)),
        out_shape=(
            jax.ShapeDtypeStruct((probes, sensors // slab_count), F32),
            jax.ShapeDtypeStruct((1, LANES), F32),
        ),
        in_specs=[vmem, vmem],
        out_specs=(vmem, vmem),
        scratch_shapes=[
            VMEM((probe_groups, 8, LANES), F32),
            pltpu.SemaphoreType.DMA((probe_groups,)),
            pltpu.SemaphoreType.DMA((probe_groups,)),
        ],
        compiler_params=pltpu.CompilerParams(collective_id=2, has_side_effects=True, vmem_limit_bytes=40 * 1024 * 1024),
        name="unpack",
    )(arrived, places)
    return adjoint, observed, mean[0, 0]


COLS = 256
FAST = 11
ROOM = 36 * 1024 * 1024
SMALL = pltpu.CompilerParams(vmem_limit_bytes=ROOM)


class Geo(typing.NamedTuple):
    rows: int
    probes: int
    slabs: int
    groups: int
    buckets: int
    tiles: int
    lines: int
    owned: int
    quarter: int
    edge_lines: int
    kinds: int


def bf(x):
    return x.astype(BF16)


def cells(rows, width):
    return bf(iota((rows, width), 0).astype(F32))


def match(rows, target):
    grid = cells(min(rows, COLS), target.shape[1])
    pieces = []
    for begin in range(0, rows, COLS):
        size = min(COLS, rows - begin)
        near = bf(jnp.clip(target - begin, -1.0, float(COLS)))
        pieces.append(jnp.where(grid[:size] == near, jnp.ones((), BF16), jnp.zeros((), BF16)))
    return pieces[0] if len(pieces) == 1 else jnp.concatenate(pieces, axis=0)


def observe(geo, me, r_ref, c_ref, rf_ref, cf_ref, w_ref, order_ref, field_ref, plan_ref, slot_ref, flag_ref, value_ref, tiles, hots, ranks, fold, sem):
    lines, slabs, buckets, owned = geo.lines, geo.slabs, geo.buckets, geo.owned
    loads = 8
    rounds = geo.tiles // loads

    def load(g, j):
        t = g * loads + j
        return pltpu.make_async_copy(field_ref.at[:, t], tiles.at[t], sem.at[g])

    for g in reversed(range(rounds)):
        for j in range(loads):
            load(g, j).start()

    step = min(4, lines)
    kinds = geo.kinds

    def wide(x, i):
        return jnp.concatenate([x[i + j : i + j + 1, :] for j in range(step)], axis=1)

    order = order_ref[...]
    slot = iota((lines, LANES), 0) * LANES + iota((lines, LANES), 1)
    order_hi, order_lo = bf((order >> 7).astype(F32)), bf((order & 127).astype(F32))
    order_hi, order_lo = order_hi.astype(F32), order_lo.astype(F32)
    mine_hi, mine_lo = (slot >> 7).astype(F32), (slot & 127).astype(F32)
    found = jnp.zeros((2 * lines, LANES), F32)
    line_cells, lane_cells = cells(lines, step * LANES), cells(LANES, step * LANES)
    zero, one = jnp.zeros((), BF16), jnp.ones((), BF16)
    for i in range(0, lines, step):
        here = line_cells == bf(wide(order_hi, i))
        stack = jnp.concatenate([jnp.where(here, bf(wide(mine_hi, i)), zero), jnp.where(here, bf(wide(mine_lo, i)), zero)], axis=0)
        place = jnp.where(lane_cells == bf(wide(order_lo, i)), one, zero)
        found = found + nt_dot(stack, place)
    slot_of = (found[:lines] * LANES + found[lines:]).astype(jnp.int32)

    r = r_ref[...]
    c = c_ref[...]
    rel = r - me * geo.rows + 1
    valid = (rel >= 0) & (rel <= geo.rows)
    bucket = c // COLS
    owner = slot_of // owned
    home = r // geo.rows
    edge = r - home * geo.rows == geo.rows - 1
    key = jnp.where(valid, bucket, -1)
    send_key = jnp.where(valid, owner, -1)
    first_key = jnp.where(owner == me, home, -1)
    second_key = jnp.where((owner == me) & edge, home + 1, -1)
    edge_key = jnp.where(valid & (rel == 0), 0, jnp.where(valid & (rel == geo.rows), 1, -1))

    def hot_of(i):
        line = slice(i, i + 1)
        recv = iota((slabs, LANES), 0)
        return (
            iota((buckets, LANES), 0) == key[line],
            recv == send_key[line],
            recv == first_key[line],
            recv == second_key[line],
            iota((16, LANES), 0) == edge_key[line],
        )

    for i in range(lines):
        a, b, c1, c2, d = hot_of(i)
        hot = jnp.concatenate([jnp.where(x, 1.0, 0.0) for x in (a, b, c1 | c2, d)], axis=0)
        hots[i * kinds : (i + 1) * kinds, :] = bf(hot)
    upper = iota((LANES, 2 * LANES), 0) < iota((LANES, 2 * LANES), 1)
    upper = bf(jnp.where(upper, 1.0, 0.0))
    before = jnp.dot(hots[...], upper, preferred_element_type=F32)
    carry = jnp.zeros((kinds, LANES), F32)
    for i in range(lines):
        part = before[i * kinds : (i + 1) * kinds]
        rank = part[:, :LANES] + carry
        a, b, c1, c2, d = hot_of(i)
        recv = rank[buckets + slabs : buckets + 2 * slabs]
        picks = (
            (a, rank[:buckets]),
            (b, rank[buckets : buckets + slabs]),
            (c1, recv),
            (c2, recv),
            (d, rank[buckets + 2 * slabs :]),
        )
        for k, (mask, value) in enumerate(picks):
            ranks[k, i : i + 1, :] = jnp.sum(jnp.where(mask, value, 0.0), axis=0, keepdims=True)
        carry = carry + part[:, LANES:]
    capacity = 4.0 * geo.quarter
    row = iota((kinds, LANES), 0)
    limit = jnp.where(row < buckets, float(LANES), jnp.where(row < buckets + 2 * slabs, capacity, float(geo.edge_lines * LANES)))
    over = jnp.sum(jnp.where(carry > limit, 1.0, 0.0), axis=0, keepdims=True)
    flag_ref[...] = jnp.broadcast_to(over, flag_ref.shape)

    spot, send, recv1, recv2, swap = (ranks[k] for k in range(5))
    rf, cf, w = rf_ref[...], cf_ref[...], w_ref[...]
    rf_top, w_top = bf(rf).astype(F32), bf(w).astype(F32)
    send_quarter = jnp.floor((send + 0.5) * (1.0 / geo.quarter))
    swap_line = jnp.floor((swap + 0.5) * (1.0 / LANES))
    values = (
        (c - bucket * COLS).astype(F32),
        bf(1.0 - cf).astype(F32),
        bf(cf).astype(F32),
        rf_top,
        rf - rf_top,
        w_top,
        w - w_top,
        (rel + 1 + 8 * owner).astype(F32),
        send - send_quarter * geo.quarter,
        jnp.minimum(send_quarter, 15.0) + 16.0 * jnp.minimum(jnp.where(edge_key >= 0, swap_line, 0.0), 15.0),
        swap - swap_line * LANES,
    )
    key_value = jnp.where(valid & (spot < LANES), bucket, -1).astype(F32)
    bucket_cells = cells(buckets, step * LANES)
    total = jnp.zeros((FAST * buckets, LANES), F32)
    for i in range(0, lines, step):
        here = bucket_cells == bf(wide(key_value, i))
        stack = jnp.concatenate([jnp.where(here, bf(wide(v, i)), zero) for v in values], axis=0)
        place = jnp.where(lane_cells == bf(jnp.minimum(wide(spot, i), 255.0)), one, zero)
        total = total + nt_dot(stack, place)
    for f in range(FAST):
        plan_ref[f] = total[f * buckets : (f + 1) * buckets, :]

    sent = slabs * geo.quarter

    def position(rank, source, use):
        quarter = jnp.floor((rank + 0.5) * (1.0 / geo.quarter))
        place = quarter * sent + source.astype(F32) * geo.quarter + (rank - quarter * geo.quarter)
        return jnp.where(use, place, 4.0 * sent + 8.0)

    here_slot = slot_of - me * owned
    owned_lines = owned // LANES
    slot_line = jnp.where(owner == me, here_slot >> 7, -1).astype(F32)
    slot_lane = (here_slot & 127).astype(F32)
    fields = []
    for place in (position(recv1, home, owner == me), position(recv2, home + 1, edge)):
        high = jnp.floor(place * (1.0 / 64.0))
        fields += [high, place - 64.0 * high]
    slot_cells = cells(owned_lines, step * LANES)
    pad = -(4 * owned_lines) % 16
    placed = jnp.zeros((4 * owned_lines + pad, LANES), F32)
    for i in range(0, lines, step):
        here = jnp.broadcast_to(wide(slot_line, i), (owned_lines, step * LANES)) == iota((owned_lines, step * LANES), 0).astype(F32)
        stack = [jnp.where(here, wide(v, i), 0.0) for v in fields]
        if pad:
            stack.append(jnp.zeros((pad, step * LANES), F32))
        place = jnp.where(lane_cells == bf(wide(slot_lane, i)), one, zero)
        placed = placed + nt_dot(bf(jnp.concatenate(stack, axis=0)), place)
    for f in range(2):
        at = 2 * f * owned_lines
        slot_ref[f] = placed[at : at + owned_lines] * 64.0 + placed[at + owned_lines : at + 2 * owned_lines]

    depth = geo.rows * geo.probes
    spill = None
    batch = loads // 2
    for g in reversed(range(rounds)):
        for j in range(loads):
            load(g, j).wait()
        group = list(reversed(range(g * batch, (g + 1) * batch)))
        parts = []
        for b in group:
            block = jnp.concatenate([tiles[2 * b].reshape(depth, LANES), tiles[2 * b + 1].reshape(depth, LANES)], axis=1)
            parts.append(jnp.dot(block, bucket_table(plan_ref, b), preferred_element_type=F32))
        for b, part in zip(group, parts):
            value = part[:, :LANES]
            if spill is not None:
                value = value + spill
            spill = part[:, LANES:]
            fold[b] = value
            terms = [fold[b, pl.ds(k, geo.probes, stride=geo.rows), :] * x for k, x in enumerate(row_weights(geo, plan_ref, b))]
            value_ref[b] = functools.reduce(jnp.add, terms)


def bucket_table(plan_ref, b):
    near, low, high = (plan_ref[f, pl.ds(b, 1), :] for f in range(3))
    grid = cells(COLS, LANES)
    zero = jnp.zeros((), BF16)
    main = jnp.where(grid == bf(near), bf(low), jnp.where(grid == bf(near + 1.0), bf(high), zero))
    if isinstance(b, int) and b == 0:
        return jnp.concatenate([main, jnp.zeros((COLS, LANES), BF16)], axis=1)
    before = b - 1 if isinstance(b, int) else jnp.maximum(b - 1, 0)
    last, spill = (plan_ref[f, pl.ds(before, 1), :] for f in (0, 2))
    spill = jnp.where(last == COLS - 1.0, spill, 0.0)
    over = bf(jnp.where(iota((16, LANES), 0) == 0, spill, 0.0))
    over = jnp.concatenate([over, jnp.zeros((COLS - 16, LANES), BF16)], axis=0)
    return jnp.concatenate([main, over], axis=1)


def place_code(plan_ref, b):
    code = plan_ref[7, pl.ds(b, 1), :]
    owner = jnp.floor(code * 0.125)
    return owner, code - 8.0 * owner


def row_weights(geo, plan_ref, b):
    rf = plan_ref[3, pl.ds(b, 1), :] + plan_ref[4, pl.ds(b, 1), :]
    _, rel = place_code(plan_ref, b)
    return [jnp.where(rel == k + 2.0, 1.0 - rf, jnp.where(rel == k + 1.0, rf, 0.0)) for k in range(geo.rows)]


def exchange_kernel(geo, r_ref, c_ref, rf_ref, cf_ref, w_ref, order_ref, field_ref, adjoint_ref, arrived_ref, slot_ref, total_ref, ok_ref, plan_ref, flag_ref, value_ref, tiles, hots, ranks, fold, edges, places, shares, inbox, packed, sources, raised, traces, load_sem, swap_send, swap_recv, owner_send, owner_recv, trace_send, trace_recv):
    slabs, groups, probes, rows, quarter, buckets = geo.slabs, geo.groups, geo.probes, geo.rows, geo.quarter, geo.buckets
    me, mine = lax.axis_index("slab"), lax.axis_index("probe")
    lines = geo.edge_lines
    zero = jnp.zeros((), BF16)
    batch = 8

    def at(slab, probe):
        return dict(device_id=(slab, probe), device_id_type=pl.DeviceIdType.MESH)

    everyone = slabs * groups
    linear = me * groups + mine

    def other(k):
        return lax.rem(linear + k, everyone)

    barrier = pltpu.get_barrier_semaphore()

    @pl.loop(1, everyone)
    def _(k):
        pl.semaphore_signal(barrier, inc=1, **at(other(k) // groups, other(k) % groups))

    observe(geo, me, r_ref, c_ref, rf_ref, cf_ref, w_ref, order_ref, field_ref, plan_ref, slot_ref, flag_ref, value_ref, tiles, hots, ranks, fold, load_sem)

    def columns(j):
        return slice(j * LANES, (j + 1) * LANES)

    def edge_fields(b):
        _, rel = place_code(plan_ref, b)
        line = jnp.floor(plan_ref[9, pl.ds(b, 1), :] * (1.0 / 16.0))
        lane = plan_ref[10, pl.ds(b, 1), :]
        return rel, line, lane

    def weight_of(b):
        return plan_ref[5, pl.ds(b, 1), :] + plan_ref[6, pl.ds(b, 1), :]

    edges[...] = jnp.zeros_like(edges)
    shares[...] = jnp.zeros_like(shares)
    share_rows = shares.shape[0]

    @pl.loop(0, buckets // batch)
    def _(g):
        stacks, spots = [], []
        for j in range(batch):
            b = g * batch + j
            rel, line, lane = edge_fields(b)
            low, high = rel == 1.0, rel == rows + 1.0
            spot = match(2 * LANES, jnp.where(low, lane, jnp.where(high, lane + LANES, -1.0)))
            value = value_ref[b]
            share = jnp.where((iota((share_rows, LANES), 0).astype(F32) == line) & high, weight_of(b), 0.0)
            stacks.append(jnp.concatenate([bf(jnp.where(line == float(l), value, 0.0)) for l in range(lines)] + [bf(share)], axis=0))
            spots.append(spot)
            places[b] = spot
        part = nt_dot(jnp.concatenate(stacks, axis=1), jnp.concatenate(spots, axis=1))
        for side in range(2):
            edges[side] += part[: lines * probes, columns(side)]
        shares[...] += part[lines * probes :, columns(1)]

    pl.semaphore_wait(barrier, everyone - 1)
    down, up = lax.rem(me + slabs - 1, slabs), lax.rem(me + 1, slabs)
    swaps = [
        pltpu.make_async_remote_copy(
            src_ref=edges.at[side], dst_ref=inbox.at[1 - side], send_sem=swap_send.at[side], recv_sem=swap_recv.at[side], **at(peer, mine)
        )
        for side, peer in ((0, down), (1, up))
    ]
    for copy in swaps:
        copy.start()

    packed[...] = jnp.zeros_like(packed)

    def pack(g, squares):
        hots, quads = [], []
        for j in range(batch):
            b = g * batch + j
            owner, rel = place_code(plan_ref, b)
            code = plan_ref[9, pl.ds(b, 1), :]
            fourth = code - 16.0 * jnp.floor(code * (1.0 / 16.0))
            row = jnp.where(rel > 0.0, owner * quarter + plan_ref[8, pl.ds(b, 1), :], -1.0)
            hots.append(match(slabs * quarter, row))
            value = value_ref[b]
            squares = squares + value * value * weight_of(b)
            quads.append(jnp.concatenate([bf(jnp.where(fourth == float(k), value, 0.0)) for k in range(4)], axis=0))
        part = nt_dot(jnp.concatenate(hots, axis=1), jnp.concatenate(quads, axis=1))
        packed[...] += part.reshape(packed.shape)
        return squares

    squares = lax.fori_loop(0, buckets // batch, pack, jnp.zeros((probes, LANES), F32))

    def owner_copy(k, source, peer):
        return pltpu.make_async_remote_copy(
            src_ref=packed.at[peer], dst_ref=arrived_ref.at[source], send_sem=owner_send.at[k], recv_sem=owner_recv.at[k], **at(peer, mine)
        )

    for k in range(1, slabs):
        owner_copy(k, me, lax.rem(me + k, slabs)).start()
    arrived_ref[me] = packed[me]

    for copy in swaps:
        copy.wait()
    for l in range(lines):
        part = slice(l * probes, (l + 1) * probes)
        squares = squares + edges[1, part] * inbox[1, part] * (2.0 * shares[l : l + 1])
    folded = squares[:8]
    for d in range(8, probes, 8):
        folded = folded + squares[d : d + 8]
    traces[linear] = jnp.concatenate([folded, flag_ref[...]], axis=0)

    def trace_copy(k, source, peer):
        return pltpu.make_async_remote_copy(
            src_ref=traces.at[linear],
            dst_ref=traces.at[source],
            send_sem=trace_send.at[k],
            recv_sem=trace_recv.at[k],
            **at(peer // groups, peer % groups),
        )

    @pl.loop(1, everyone)
    def _(k):
        trace_copy(k, linear, other(k)).start()

    both = bf(jnp.concatenate([inbox[0], inbox[1]], axis=1))
    sources[0] = jnp.zeros_like(sources[0])

    @pl.loop(0, buckets // batch)
    def _(g):
        spots = jnp.concatenate([places[g * batch + j] for j in range(batch)], axis=1)
        extra = jnp.dot(both, spots, preferred_element_type=F32)
        for j in range(batch):
            b = g * batch + j
            _, line, _ = edge_fields(b)
            full = value_ref[b]
            for l in range(lines):
                full = full + jnp.where(line == float(l), extra[l * probes : (l + 1) * probes, columns(j)], 0.0)
            spread = full * weight_of(b)
            for k, weight in enumerate(row_weights(geo, plan_ref, b)):
                raised[j, pl.ds(k, probes, stride=rows), :] = spread * weight
            sources[b + 1] = bf(raised[j])

    @pl.loop(0, buckets // batch)
    def _(g):
        parts = []
        for j in range(batch):
            b = g * batch + j
            source = jnp.concatenate([sources[b + 1], sources[b]], axis=1)
            parts.append(nt_dot(source, bucket_table(plan_ref, b)))
        for j in range(batch):
            for t in range(2):
                adjoint_ref[2 * (g * batch + j) + t] = bf(parts[j][:, columns(t)]).reshape(probes, rows, LANES)

    for k in range(1, slabs):
        source = lax.rem(me + slabs - k, slabs)
        owner_copy(k, source, source).wait()

    @pl.loop(1, everyone)
    def _(k):
        source = lax.rem(linear + everyone - k, everyone)
        trace_copy(k, source, source).wait()

    total = jnp.sum(traces[...], axis=0)
    total_ref[...] = total
    ok_ref[0] = jnp.max(total[8:]).astype(jnp.int32)


def deliver_kernel(geo, scale, adjoint_ref, arrived_ref, slot_ref, total_ref, out_ref, observed_ref, mean_ref, observed, sem):
    slabs, probes, quarter, owned = geo.slabs, geo.probes, geo.quarter, geo.owned
    loads = 8

    def store(t):
        return pltpu.make_async_copy(adjoint_ref.at[t], out_ref.at[:, t], sem.at[0])

    for t in range(geo.tiles):
        store(t).start()
    sent = slabs * quarter
    arrived = jnp.transpose(arrived_ref[...].reshape(sent, 4 * probes))
    lines = owned // LANES
    spots = [jnp.concatenate([slot_ref[f, l : l + 1, :] for l in range(lines)], axis=1) for f in range(2)]
    total = jnp.zeros((probes, owned), F32)
    for k in range(4):
        hot = match(sent, spots[0] - float(k * sent)) + match(sent, spots[1] - float(k * sent))
        total = total + jnp.dot(bf(arrived[k * probes : (k + 1) * probes]), hot, preferred_element_type=F32)
    observed[...] = total
    pltpu.make_async_copy(observed, observed_ref, sem.at[1]).start()
    summed = jnp.sum(total_ref[:8], axis=0, keepdims=True)
    mean_ref[...] = jnp.broadcast_to(jnp.sum(summed, axis=1, keepdims=True) * scale, mean_ref.shape)
    pltpu.make_async_copy(observed, observed_ref, sem.at[1]).wait()
    for t in range(geo.tiles):
        store(t).wait()


def geometry(slabs, groups, probe_fields, sensors):
    probes, rows, width = probe_fields.shape
    most = min(sensors, 4 * sensors // slabs)
    quarter = -(-(most // slabs + 32) // 32) * 8
    edge_lines = -(-5 * most // (4 * rows * LANES))
    buckets = width // COLS
    return Geo(rows, probes, slabs, groups, buckets, width // LANES, sensors // LANES, sensors // slabs, quarter, edge_lines, buckets + 2 * slabs + 16)


def body(slab_count, probe_groups, probe_fields, *vectors):
    sensors = vectors[0].shape[0]
    geo = geometry(slab_count, probe_groups, probe_fields, sensors)
    probes, rows, width = probe_fields.shape
    depth = probes * rows
    lines, buckets, tiles = geo.lines, geo.buckets, geo.tiles
    boxed = [x.reshape(lines, LANES) for x in vectors]
    field = probe_fields.reshape(probes, rows, tiles, LANES).transpose(0, 2, 1, 3)
    vmem = pl.BlockSpec(memory_space=VMEM)
    smem = pl.BlockSpec(memory_space=SMEM)
    hbm = pl.BlockSpec(memory_space=pltpu.HBM)
    dma = pltpu.SemaphoreType.DMA
    shape = jax.ShapeDtypeStruct
    edge_rows = geo.edge_lines * probes
    everyone = slab_count * probe_groups
    adjoint, arrived, slots, total, flag = pl.pallas_call(
        functools.partial(exchange_kernel, geo),
        out_shape=(
            shape((tiles, probes, rows, LANES), BF16),
            shape((slab_count, geo.quarter, 4 * probes), F32),
            shape((2, geo.owned // LANES, LANES), F32),
            shape((16, LANES), F32),
            shape((1,), jnp.int32),
        ),
        in_specs=[vmem] * 6 + [hbm],
        out_specs=(vmem, vmem, vmem, vmem, smem),
        scratch_shapes=[
            VMEM((FAST, buckets, LANES), F32),
            VMEM((8, LANES), F32),
            VMEM((buckets, probes, LANES), F32),
            VMEM((tiles, probes, rows, LANES), BF16),
            VMEM((lines * geo.kinds, LANES), BF16),
            VMEM((5, lines, LANES), F32),
            VMEM((buckets, depth, LANES), F32),
            VMEM((2, edge_rows, LANES), F32),
            VMEM((buckets, 2 * LANES, LANES), BF16),
            VMEM((-(-geo.edge_lines // 16) * 16, LANES), F32),
            VMEM((2, edge_rows, LANES), F32),
            VMEM((slab_count, geo.quarter, 4 * probes), F32),
            VMEM((buckets + 1, depth, LANES), BF16),
            VMEM((8, depth, LANES), F32),
            VMEM((everyone, 16, LANES), F32),
            dma((tiles // 8,)),
            dma((2,)),
            dma((2,)),
            dma((slab_count,)),
            dma((slab_count,)),
            dma((everyone,)),
            dma((everyone,)),
        ],
        compiler_params=pltpu.CompilerParams(collective_id=3, has_side_effects=True, vmem_limit_bytes=ROOM),
        name="exchange",
    )(*boxed, field)
    out, observed, mean = pl.pallas_call(
        functools.partial(deliver_kernel, geo, 1.0 / (probes * probe_groups * sensors)),
        out_shape=(
            shape((probes, tiles, rows, LANES), BF16),
            shape((probes, geo.owned), F32),
            shape((1, LANES), F32),
        ),
        in_specs=[vmem] * 4,
        out_specs=(hbm, hbm, vmem),
        scratch_shapes=[VMEM((probes, geo.owned), F32), dma((2,))],
        compiler_params=SMALL,
        name="deliver",
    )(adjoint, arrived, slots, total)
    out = out.transpose(0, 2, 1, 3).reshape(probes, rows, width)

    def again(state):
        out, observed, mean = general(slab_count, probe_groups, probe_fields, *vectors)
        return out, jnp.where(state[3] > 0, observed, state[1]), mean, state[3] * 0

    state = lax.while_loop(lambda state: state[3] != 0, again, (out, observed, mean[0, 0], flag[0]))
    return state[:3]


def solution(mesh):
    placed = (P("probe", "slab", None), P(), P(), P(), P(), P(), P())
    return jax.shard_map(
        functools.partial(body, mesh.shape["slab"], mesh.shape["probe"]),
        mesh=mesh,
        in_specs=placed,
        out_specs=(P("probe", "slab", None), P("probe", "slab"), P()),
        check_vma=False,
    )
```

```python
import functools
import typing

import jax
import jax.numpy as jnp
from jax import lax
from jax.experimental import pallas as pl
from jax.experimental.pallas import tpu as pltpu
from jax.sharding import PartitionSpec as P

LANES = 128
BLOCK = 1024
HALF = 256
FIELDS = 11
F32 = jnp.float32
BF16 = jnp.bfloat16
NT = (((1,), (1,)), ((), ()))
VMEM = pltpu.VMEM
SMEM = pltpu.SMEM
LIMIT = pltpu.CompilerParams(vmem_limit_bytes=60 * 1024 * 1024)


def iota(shape, dim):
    return lax.broadcasted_iota(jnp.int32, shape, dim)


def nt_dot(a, b):
    return lax.dot_general(a, b, NT, preferred_element_type=F32)


def plan_kernel(rows, cap_chunks, blocks, slabs, pair_lines, me_ref, r_ref, c_ref, rf_ref, cf_ref, w_ref, order_ref, plan_ref, marks_ref, places_ref, peak_ref):
    lines = r_ref.shape[0]
    sensors = lines * LANES
    step = min(4, lines)
    me = me_ref[0]
    first = me * rows
    owned = lines * LANES // slabs
    keys_group = 2 * blocks
    keys = 3 * keys_group
    chunks = 3 * cap_chunks

    def wide(x, i):
        return jnp.concatenate([x[i + j : i + j + 1, :] for j in range(step)], axis=1)

    order = order_ref[...]
    slot = iota((lines, LANES), 0) * LANES + iota((lines, LANES), 1)
    found = jnp.zeros((2 * lines, LANES), F32)
    for i in range(0, lines, step):
        target = wide(order, i)
        mine = wide(slot, i)
        here = iota((lines, step * LANES), 0) == (target >> 7)
        stack = jnp.concatenate(
            [jnp.where(here, (mine >> 7).astype(F32), 0.0), jnp.where(here, (mine & 127).astype(F32), 0.0)], axis=0
        ).astype(BF16)
        place = jnp.where(iota((LANES, step * LANES), 0) == (target & 127), 1.0, 0.0).astype(BF16)
        found = found + nt_dot(stack, place)
    slot_hi = found[:lines, :]
    slot_lo = found[lines:, :]

    r = r_ref[...]
    c = c_ref[...]
    rel = r - first + 1
    valid = (rel >= 0) & (rel <= rows)
    group = jnp.where(rel == 0, 0, jnp.where(rel == rows, 2, 1))
    block = c // BLOCK
    inner = c - block * BLOCK
    half = c // HALF
    slot_of = (slot_hi * LANES + slot_lo).astype(jnp.int32)
    owner = slot_of // owned
    home = r // rows
    send_key = jnp.where(home == me, owner, -1)
    recv_key = jnp.where(owner == me, home, -1)
    edge = jnp.where(r - home * rows == rows - 1, home, -1)
    edges = jnp.zeros((slabs, LANES), F32)
    for i in range(lines):
        edges = edges + jnp.where(iota((slabs, LANES), 0) == edge[i : i + 1, :], 1.0, 0.0)
    peak_ref[0] = jnp.max(jnp.sum(edges, axis=1, keepdims=True)).astype(jnp.int32)
    key = group * keys_group + 2 * block + jnp.where(inner == BLOCK - 1, 1, 0)
    key = jnp.where(valid, key, -1)

    count = jnp.zeros((keys, 1), F32)
    for i in range(lines):
        count = count + jnp.sum(jnp.where(iota((keys, LANES), 0) == key[i : i + 1, :], 1.0, 0.0), axis=1, keepdims=True)
    big = jnp.floor(count * (1.0 / 64.0))
    small = count - 64.0 * big
    ka, kb = iota((keys, keys), 0), iota((keys, keys), 1)
    below = jnp.where((kb < ka) & (kb // keys_group == ka // keys_group), 1.0, 0.0).astype(BF16)
    start = 64.0 * jnp.dot(below, jnp.broadcast_to(big, (keys, LANES)).astype(BF16), preferred_element_type=F32)
    start = start + jnp.dot(below, jnp.broadcast_to(small, (keys, LANES)).astype(BF16), preferred_element_type=F32)
    start = start + ((iota((keys, LANES), 0) // keys_group) * (cap_chunks * LANES)).astype(F32)
    wide_keys = marks_ref.shape[1]
    diagonal = iota((keys, wide_keys), 0) == iota((keys, wide_keys), 1)
    marks_ref[...] = jnp.concatenate(
        [jnp.sum(jnp.where(diagonal, x, 0.0), axis=0, keepdims=True) for x in (start[:, :1], start[:, :1] + count)], axis=0
    ).astype(jnp.int32)

    upper = jnp.where(iota((LANES, LANES), 0) < iota((LANES, LANES), 1), 1.0, 0.0).astype(BF16)
    carry = jnp.concatenate([start[:, :1], jnp.zeros((2 * slabs, 1), F32)], axis=0)
    spots, sends, recvs = [], [], []
    for i in range(lines):
        hot = jnp.concatenate(
            [
                jnp.where(iota((keys, LANES), 0) == key[i : i + 1, :], 1.0, 0.0),
                jnp.where(iota((slabs, LANES), 0) == send_key[i : i + 1, :], 1.0, 0.0),
                jnp.where(iota((slabs, LANES), 0) == recv_key[i : i + 1, :], 1.0, 0.0),
            ],
            axis=0,
        )
        before = jnp.dot(hot.astype(BF16), upper, preferred_element_type=F32)
        ranks = hot * (before + carry)
        spots.append(jnp.sum(ranks[:keys], axis=0, keepdims=True))
        sends.append(jnp.sum(ranks[keys : keys + slabs], axis=0, keepdims=True))
        recvs.append(jnp.sum(ranks[keys + slabs :], axis=0, keepdims=True))
        carry = carry + jnp.sum(hot, axis=1, keepdims=True)
    spot = jnp.concatenate(spots, axis=0).astype(jnp.int32)
    spot = jnp.where(valid, spot, -1)
    send = jnp.concatenate(sends, axis=0).astype(jnp.int32)
    recv = jnp.concatenate(recvs, axis=0).astype(jnp.int32)
    send_line = jnp.where(send_key >= 0, owner * pair_lines + (send >> 7), 200)
    recv_line = jnp.where(recv_key >= 0, home * pair_lines + (recv >> 7), -1)

    rf = rf_ref[...]
    cf = cf_ref[...]
    w = w_ref[...]
    rf_top = rf.astype(BF16).astype(F32)
    w_top = w.astype(BF16).astype(F32)
    values = [
        half.astype(F32),
        (c - half * HALF).astype(F32),
        (1.0 - cf).astype(BF16).astype(F32),
        cf.astype(BF16).astype(F32),
        rf_top,
        rf - rf_top,
        w_top,
        w - w_top,
        rel.astype(F32),
        send_line.astype(F32),
        (send & 127).astype(F32),
    ]
    total = jnp.zeros((FIELDS * chunks, LANES), F32)
    for i in range(0, lines, step):
        target = wide(spot, i)
        here = iota((chunks, step * LANES), 0) == (target >> 7)
        stack = jnp.concatenate([jnp.where(here, wide(v, i), 0.0) for v in values], axis=0).astype(BF16)
        place = jnp.where(iota((LANES, step * LANES), 0) == (target & 127), 1.0, 0.0).astype(BF16)
        total = total + nt_dot(stack, place)
    for f in range(FIELDS):
        plan_ref[f] = total[f * chunks : (f + 1) * chunks, :]

    slot_here = slot_of - me * owned
    received = slabs * pair_lines
    found = jnp.zeros((2 * received, LANES), F32)
    for i in range(0, lines, step):
        here = iota((received, step * LANES), 0) == wide(recv_line, i)
        target = wide(slot_here, i)
        stack = jnp.concatenate(
            [jnp.where(here, (target >> 7).astype(F32), 0.0), jnp.where(here, (target & 127).astype(F32), 0.0)], axis=0
        ).astype(BF16)
        place = jnp.where(iota((LANES, step * LANES), 0) == (wide(recv, i) & 127), 1.0, 0.0).astype(BF16)
        found = found + nt_dot(stack, place)
    places_ref[...] = (found[:received] * LANES + found[received:]).astype(jnp.int32)


def column_table(plan_ref, chunk, number):
    line = pl.ds(chunk, 1)
    column = plan_ref[0, line, :] * HALF + plan_ref[1, line, :] - (number * BLOCK).astype(F32)
    low = plan_ref[2, line, :].astype(BF16)
    high = plan_ref[3, line, :].astype(BF16)
    cells = iota((HALF, LANES), 0).astype(F32).astype(BF16)
    pieces = []
    for begin in range(0, BLOCK, HALF):
        near = jnp.clip(column - begin, -2.0, HALF).astype(BF16)
        after = jnp.clip(column - (begin - 1), -2.0, HALF).astype(BF16)
        pieces.append(jnp.where(cells == near, low, jnp.where(cells == after, high, jnp.zeros((), BF16))))
    return jnp.concatenate(pieces, axis=0)


def row_pattern(plan_ref, chunk, rows, depth):
    line = pl.ds(chunk, 1)
    rf = plan_ref[4, line, :] + plan_ref[5, line, :]
    rel = plan_ref[8, line, :].astype(jnp.int32)
    row = iota((depth, LANES), 0) % rows + 1
    return jnp.where(row == rel, 1.0 - rf, jnp.where(row == rel + 1, rf, 0.0))


def group_chunks(marks_ref, group, keys_group, base):
    count = (marks_ref[1, (group + 1) * keys_group - 1] - base + LANES - 1) // LANES
    return jnp.maximum(count, 1)


def chunk_range(marks_ref, group, number, keys_group, cap_chunks):
    at = group * keys_group + 2 * number
    begin = marks_ref[0, jnp.maximum(at - 1, group * keys_group)]
    end = marks_ref[1, at + 1]
    base = group * cap_chunks
    last = base + group_chunks(marks_ref, group, keys_group, base * LANES) - 1
    return jnp.minimum(begin // LANES, last), jnp.where(end > begin, (end + LANES - 1) // LANES, 0)


def forward_kernel(cap_chunks, blocks, field_ref, plan_ref, marks_ref, value_ref, sums, flat):
    probes, rows, _ = field_ref.shape
    depth = probes * rows
    keys_group = 2 * blocks
    number = pl.program_id(0)
    counts = [group_chunks(marks_ref, g, keys_group, g * cap_chunks * LANES) for g in range(3)]

    @pl.when(number == 0)
    def _():
        for g in range(3):

            @pl.loop(0, counts[g])
            def _(k):
                sums[g * cap_chunks + k] = jnp.zeros((depth, LANES), F32)

    block = field_ref[...].reshape(depth, BLOCK)
    flat[...] = block
    ranges = [chunk_range(marks_ref, g, number, keys_group, cap_chunks) for g in range(3)]
    table = jnp.concatenate([column_table(plan_ref, begin, number) for begin, _ in ranges], axis=1)
    part = jnp.dot(block, table, preferred_element_type=F32)
    for g in range(3):
        sums[ranges[g][0]] += part[:, g * LANES : (g + 1) * LANES]
    for g in range(3):

        @pl.loop(ranges[g][0] + 1, ranges[g][1])
        def _(chunk):
            sums[chunk] += jnp.dot(flat[...], column_table(plan_ref, chunk, number), preferred_element_type=F32)

    @pl.when(number == blocks - 1)
    def _():
        fold = jnp.where(iota((probes, depth), 1) // rows == iota((probes, depth), 0), 1.0, 0.0).astype(BF16)
        for g in range(3):

            @pl.loop(0, counts[g])
            def _(k):
                chunk = g * cap_chunks + k
                scaled = (sums[chunk] * row_pattern(plan_ref, chunk, rows, depth)).astype(BF16)
                value_ref[chunk] = jnp.dot(fold, scaled, preferred_element_type=F32)


def swap_kernel(slabs, top, value_ref, above_ref, below_ref, send_sem, recv_sem):
    probe, me = lax.axis_index("probe"), lax.axis_index("slab")
    width = above_ref.shape[0]
    down, up = lax.rem(me + slabs - 1, slabs), lax.rem(me + 1, slabs)
    barrier = pltpu.get_barrier_semaphore()
    for peer in (down, up):
        pl.semaphore_signal(barrier, inc=1, device_id=(peer, probe), device_id_type=pl.DeviceIdType.MESH)
    pl.semaphore_wait(barrier, 2)
    copies = []
    for k, (peer, begin, target) in enumerate(((down, 0, above_ref), (up, top, below_ref))):
        copies.append(
            pltpu.make_async_remote_copy(
                src_ref=value_ref.at[begin : begin + width],
                dst_ref=target,
                send_sem=send_sem.at[k],
                recv_sem=recv_sem.at[k],
                device_id=(peer, probe),
                device_id_type=pl.DeviceIdType.MESH,
            )
        )
    for copy in copies:
        copy.start()
    for copy in copies:
        copy.wait()


def swap(slabs, cap_chunks, width, number, value):
    part = (width, *value.shape[1:])
    any_space = pl.BlockSpec(memory_space=pl.ANY)
    above, below = pl.pallas_call(
        functools.partial(swap_kernel, slabs, 2 * cap_chunks),
        out_shape=(jax.ShapeDtypeStruct(part, F32), jax.ShapeDtypeStruct(part, F32)),
        in_specs=[any_space],
        out_specs=(any_space, any_space),
        scratch_shapes=[pltpu.SemaphoreType.DMA((2,)), pltpu.SemaphoreType.DMA((2,))],
        compiler_params=pltpu.CompilerParams(collective_id=number, has_side_effects=True),
        name="swap",
    )(value)
    return above, below


def merge_kernel(cap_chunks, blocks, value_ref, above_ref, below_ref, plan_ref, marks_ref, spread_ref, packed_ref, squares, parts):
    slabs = packed_ref.shape[0]
    outgoing, probes, _ = parts.shape
    lines = outgoing // slabs
    keys_group = 2 * blocks
    squares[...] = jnp.zeros_like(squares)
    parts[...] = jnp.zeros_like(parts)
    for g in range(3):
        count = group_chunks(marks_ref, g, keys_group, g * cap_chunks * LANES)

        @pl.loop(0, count)
        def _(k):
            chunk = g * cap_chunks + k
            value = value_ref[chunk]
            if g == 0:
                value = value + below_ref[k]
            if g == 2:
                value = value + above_ref[k]
            line = pl.ds(chunk, 1)
            spread = value * (plan_ref[6, line, :] + plan_ref[7, line, :])
            spread_ref[chunk] = spread.astype(BF16)
            if g > 0:
                squares[...] += spread * value
                high = plan_ref[9, line, :].astype(jnp.int32)
                low = plan_ref[10, line, :].astype(jnp.int32)
                place = jnp.where(iota((LANES, LANES), 0) == low, 1.0, 0.0).astype(BF16)
                stack = jnp.concatenate([jnp.where(high == d, value, 0.0) for d in range(outgoing)], axis=0).astype(BF16)
                parts[...] += nt_dot(stack, place).reshape(outgoing, probes, LANES)

    folded = squares[:8, :]
    for d in range(8, probes, 8):
        folded = folded + squares[d : d + 8, :]
    for d in range(slabs):
        for e in range(lines):
            packed_ref[d, e * probes : (e + 1) * probes, :] = parts[d * lines + e]
        packed_ref[d, lines * probes :, :] = folded


def unpack_kernel(groups, scale, packed_ref, places_ref, observed_ref, mean_ref, traces, send_sem, recv_sem):
    slab, me = lax.axis_index("slab"), lax.axis_index("probe")
    slabs = packed_ref.shape[0]
    probes, owned = observed_ref.shape
    lines = places_ref.shape[0] // slabs
    barrier = pltpu.get_barrier_semaphore()
    for k in range(1, groups):
        peer = lax.rem(me + k, groups)
        pl.semaphore_signal(barrier, inc=1, device_id=(slab, peer), device_id_type=pl.DeviceIdType.MESH)
    own = packed_ref[0, lines * probes :, :]
    for d in range(1, slabs):
        own = own + packed_ref[d, lines * probes :, :]
    traces[me] = own
    pl.semaphore_wait(barrier, groups - 1)

    def tile(k, source, peer):
        return pltpu.make_async_remote_copy(
            src_ref=traces.at[me],
            dst_ref=traces.at[source],
            send_sem=send_sem.at[k],
            recv_sem=recv_sem.at[k],
            device_id=(slab, peer),
            device_id_type=pl.DeviceIdType.MESH,
        )

    for k in range(1, groups):
        tile(k, me, lax.rem(me + k, groups)).start()
    total = jnp.zeros((probes, owned), F32)
    for d in range(slabs):
        for e in range(lines):
            at = d * lines + e
            place = jnp.where(iota((owned, LANES), 0) == places_ref[at : at + 1, :], 1.0, 0.0).astype(BF16)
            total = total + nt_dot(packed_ref[d, e * probes : (e + 1) * probes, :].astype(BF16), place)
    observed_ref[...] = total
    for k in range(1, groups):
        source = lax.rem(me + groups - k, groups)
        tile(k, source, source).wait()
    summed = jnp.sum(jnp.sum(traces[...], axis=0), axis=0, keepdims=True)
    mean_ref[...] = jnp.broadcast_to(jnp.sum(summed, axis=1, keepdims=True) * scale, mean_ref.shape)


def adjoint_kernel(cap_chunks, blocks, spread_ref, plan_ref, marks_ref, out_ref, sources, total):
    probes, rows, _ = out_ref.shape
    depth = probes * rows
    keys_group = 2 * blocks
    number = pl.program_id(0)

    @pl.when(number == 0)
    def _():
        raise_rows = jnp.where(iota((depth, probes), 0) // rows == iota((depth, probes), 1), 1.0, 0.0).astype(BF16)
        for g in range(3):
            count = group_chunks(marks_ref, g, keys_group, g * cap_chunks * LANES)

            @pl.loop(0, count)
            def _(k):
                chunk = g * cap_chunks + k
                raised = jnp.dot(raise_rows, spread_ref[chunk], preferred_element_type=F32)
                sources[chunk] = (raised * row_pattern(plan_ref, chunk, rows, depth)).astype(BF16)

    ranges = [chunk_range(marks_ref, g, number, keys_group, cap_chunks) for g in range(3)]
    table = jnp.concatenate([column_table(plan_ref, begin, number) for begin, _ in ranges], axis=1)
    source = jnp.concatenate([sources[begin] for begin, _ in ranges], axis=1)
    total[...] = nt_dot(source, table)
    for g in range(3):

        @pl.loop(ranges[g][0] + 1, ranges[g][1])
        def _(chunk):
            total[...] += nt_dot(sources[chunk], column_table(plan_ref, chunk, number))

    out_ref[...] = total[...].astype(BF16).reshape(probes, rows, BLOCK)


def general(slab_count, probe_groups, probe_fields, sensor_rows, sensor_cols, row_frac, col_frac, sensor_weights, owner_order):
    probes, rows, width = probe_fields.shape
    sensors = sensor_rows.shape[0]
    depth = probes * rows
    lines = sensors // LANES
    blocks = width // BLOCK
    keys = 6 * blocks
    most = min(sensors, 4 * sensors // slab_count)
    cap_chunks = -(-most // (8 * LANES)) * 8
    chunks = 3 * cap_chunks
    pair_lines = -(-most // (slab_count * LANES))
    outgoing = slab_count * pair_lines
    me = jnp.reshape(lax.axis_index("slab"), (1,)).astype(jnp.int32)
    boxed = [x.reshape(lines, LANES) for x in (sensor_rows, sensor_cols, row_frac, col_frac, sensor_weights, owner_order)]
    vmem = pl.BlockSpec(memory_space=VMEM)
    smem = pl.BlockSpec(memory_space=SMEM)
    plan, marks, places, peak = pl.pallas_call(
        functools.partial(plan_kernel, rows, cap_chunks, blocks, slab_count, pair_lines),
        out_shape=(
            jax.ShapeDtypeStruct((FIELDS, chunks, LANES), F32),
            jax.ShapeDtypeStruct((2, -(-keys // LANES) * LANES), jnp.int32),
            jax.ShapeDtypeStruct((outgoing, LANES), jnp.int32),
            jax.ShapeDtypeStruct((1,), jnp.int32),
        ),
        in_specs=[smem] + [vmem] * 6,
        out_specs=(vmem, vmem, vmem, smem),
        compiler_params=LIMIT,
        name="plan",
    )(me, *boxed)
    value = pl.pallas_call(
        functools.partial(forward_kernel, cap_chunks, blocks),
        out_shape=jax.ShapeDtypeStruct((chunks, probes, LANES), F32),
        grid=(blocks,),
        in_specs=[pl.BlockSpec((probes, rows, BLOCK), lambda n: (0, 0, n)), vmem, smem],
        out_specs=vmem,
        scratch_shapes=[VMEM((chunks, depth, LANES), F32), VMEM((depth, BLOCK), BF16)],
        compiler_params=LIMIT,
        name="forward",
    )(probe_fields, plan, marks)
    few = min(cap_chunks, -(-5 * most // (4 * rows * LANES)))

    def merged(above, below):
        return pl.pallas_call(
            functools.partial(merge_kernel, cap_chunks, blocks),
            out_shape=(
                jax.ShapeDtypeStruct((chunks, probes, LANES), BF16),
                jax.ShapeDtypeStruct((slab_count, pair_lines * probes + 8, LANES), F32),
            ),
            in_specs=[vmem, vmem, vmem, vmem, smem],
            out_specs=(vmem, vmem),
            scratch_shapes=[VMEM((probes, LANES), F32), VMEM((outgoing, probes, LANES), F32)],
            compiler_params=LIMIT,
            name="merge",
        )(value, above, below, plan, marks)

    spread, packed = lax.cond(
        peak[0] <= few * LANES,
        lambda: merged(*swap(slab_count, cap_chunks, few, 0, value)),
        lambda: merged(*swap(slab_count, cap_chunks, cap_chunks, 1, value)),
    )
    arrived = lax.all_to_all(packed, "slab", 0, 0, tiled=True)
    adjoint = pl.pallas_call(
        functools.partial(adjoint_kernel, cap_chunks, blocks),
        out_shape=jax.ShapeDtypeStruct((probes, rows, width), BF16),
        grid=(blocks,),
        in_specs=[vmem, vmem, smem],
        out_specs=pl.BlockSpec((probes, rows, BLOCK), lambda n: (0, 0, n)),
        scratch_shapes=[
            VMEM((chunks, depth, LANES), BF16),
            VMEM((depth, BLOCK), F32),
        ],
        compiler_params=LIMIT,
        cost_estimate=pl.CostEstimate(flops=4 * 10**9, bytes_accessed=8 * 10**6, transcendentals=0),
        name="adjoint",
    )(spread, plan, marks)
    observed, mean = pl.pallas_call(
        functools.partial(unpack_kernel, probe_groups, 1.0 / (probes * probe_groups * sensors)),
        out_shape=(
            jax.ShapeDtypeStruct((probes, sensors // slab_count), F32),
            jax.ShapeDtypeStruct((1, LANES), F32),
        ),
        in_specs=[vmem, vmem],
        out_specs=(vmem, vmem),
        scratch_shapes=[
            VMEM((probe_groups, 8, LANES), F32),
            pltpu.SemaphoreType.DMA((probe_groups,)),
            pltpu.SemaphoreType.DMA((probe_groups,)),
        ],
        compiler_params=pltpu.CompilerParams(collective_id=2, has_side_effects=True, vmem_limit_bytes=40 * 1024 * 1024),
        name="unpack",
    )(arrived, places)
    return adjoint, observed, mean[0, 0]


COLS = 256
FAST = 11
EARLY = 3
ROOM = 36 * 1024 * 1024
SMALL = pltpu.CompilerParams(vmem_limit_bytes=ROOM)


class Geo(typing.NamedTuple):
    rows: int
    probes: int
    slabs: int
    groups: int
    buckets: int
    tiles: int
    lines: int
    owned: int
    quarter: int
    edge_lines: int
    kinds: int


def bf(x):
    return x.astype(BF16)


def cells(rows, width):
    return bf(iota((rows, width), 0).astype(F32))


def match(rows, target):
    grid = cells(min(rows, COLS), target.shape[1])
    pieces = []
    for begin in range(0, rows, COLS):
        size = min(COLS, rows - begin)
        near = bf(jnp.clip(target - begin, -1.0, float(COLS)))
        pieces.append(jnp.where(grid[:size] == near, jnp.ones((), BF16), jnp.zeros((), BF16)))
    return pieces[0] if len(pieces) == 1 else jnp.concatenate(pieces, axis=0)


def observe(geo, me, r_ref, c_ref, rf_ref, cf_ref, w_ref, order_ref, field_ref, plan_ref, slot_ref, flag_ref, value_ref, tiles, hots, ranks, fold, sem):
    lines, slabs, buckets, owned = geo.lines, geo.slabs, geo.buckets, geo.owned
    loads = 8
    rounds = geo.tiles // loads

    def load(g, j):
        t = g * loads + j
        return pltpu.make_async_copy(field_ref.at[:, t], tiles.at[t], sem.at[g])

    for g in reversed(range(rounds)):
        for j in range(loads):
            load(g, j).start()

    step = min(4, lines)
    kinds = geo.kinds

    def wide(x, i):
        return jnp.concatenate([x[i + j : i + j + 1, :] for j in range(step)], axis=1)

    order = order_ref[...]
    slot = iota((lines, LANES), 0) * LANES + iota((lines, LANES), 1)
    order_hi, order_lo = bf((order >> 7).astype(F32)), bf((order & 127).astype(F32))
    order_hi, order_lo = order_hi.astype(F32), order_lo.astype(F32)
    mine_hi, mine_lo = (slot >> 7).astype(F32), (slot & 127).astype(F32)
    found = jnp.zeros((2 * lines, LANES), F32)
    line_cells, lane_cells = cells(lines, step * LANES), cells(LANES, step * LANES)
    zero, one = jnp.zeros((), BF16), jnp.ones((), BF16)
    for i in range(0, lines, step):
        here = line_cells == bf(wide(order_hi, i))
        stack = jnp.concatenate([jnp.where(here, bf(wide(mine_hi, i)), zero), jnp.where(here, bf(wide(mine_lo, i)), zero)], axis=0)
        place = jnp.where(lane_cells == bf(wide(order_lo, i)), one, zero)
        found = found + nt_dot(stack, place)
    slot_of = (found[:lines] * LANES + found[lines:]).astype(jnp.int32)

    r = r_ref[...]
    c = c_ref[...]
    rel = r - me * geo.rows + 1
    valid = (rel >= 0) & (rel <= geo.rows)
    bucket = c // COLS
    owner = slot_of // owned
    home = r // geo.rows
    edge = r - home * geo.rows == geo.rows - 1
    key = jnp.where(valid, bucket, -1)
    send_key = jnp.where(valid, owner, -1)
    first_key = jnp.where(owner == me, home, -1)
    second_key = jnp.where((owner == me) & edge, home + 1, -1)
    edge_key = jnp.where(valid & (rel == 0), 0, jnp.where(valid & (rel == geo.rows), 1, -1))

    def hot_of(i):
        line = slice(i, i + 1)
        recv = iota((slabs, LANES), 0)
        return (
            iota((buckets, LANES), 0) == key[line],
            recv == send_key[line],
            recv == first_key[line],
            recv == second_key[line],
            iota((16, LANES), 0) == edge_key[line],
        )

    for i in range(lines):
        a, b, c1, c2, d = hot_of(i)
        hot = jnp.concatenate([jnp.where(x, 1.0, 0.0) for x in (a, b, c1 | c2, d)], axis=0)
        hots[i * kinds : (i + 1) * kinds, :] = bf(hot)
    upper = iota((LANES, 2 * LANES), 0) < iota((LANES, 2 * LANES), 1)
    upper = bf(jnp.where(upper, 1.0, 0.0))
    before = jnp.dot(hots[...], upper, preferred_element_type=F32)
    carry = jnp.zeros((kinds, LANES), F32)
    for i in range(lines):
        part = before[i * kinds : (i + 1) * kinds]
        rank = part[:, :LANES] + carry
        a, b, c1, c2, d = hot_of(i)
        recv = rank[buckets + slabs : buckets + 2 * slabs]
        picks = (
            (a, rank[:buckets]),
            (b, rank[buckets : buckets + slabs]),
            (c1, recv),
            (c2, recv),
            (d, rank[buckets + 2 * slabs :]),
        )
        for k, (mask, value) in enumerate(picks):
            ranks[k, i : i + 1, :] = jnp.sum(jnp.where(mask, value, 0.0), axis=0, keepdims=True)
        carry = carry + part[:, LANES:]
    capacity = 4.0 * geo.quarter
    row = iota((kinds, LANES), 0)
    limit = jnp.where(row < buckets, float(LANES), jnp.where(row < buckets + 2 * slabs, capacity, float(geo.edge_lines * LANES)))
    over = jnp.sum(jnp.where(carry > limit, 1.0, 0.0), axis=0, keepdims=True)
    flag_ref[...] = jnp.broadcast_to(over, flag_ref.shape)

    spot, send, recv1, recv2, swap = (ranks[k] for k in range(5))
    rf, cf, w = rf_ref[...], cf_ref[...], w_ref[...]
    rf_top, w_top = bf(rf).astype(F32), bf(w).astype(F32)
    send_quarter = jnp.floor((send + 0.5) * (1.0 / geo.quarter))
    swap_line = jnp.floor((swap + 0.5) * (1.0 / LANES))
    values = (
        (c - bucket * COLS).astype(F32),
        bf(1.0 - cf).astype(F32),
        bf(cf).astype(F32),
        rf_top,
        rf - rf_top,
        w_top,
        w - w_top,
        (rel + 1 + 8 * owner).astype(F32),
        send - send_quarter * geo.quarter,
        jnp.minimum(send_quarter, 15.0) + 16.0 * jnp.minimum(jnp.where(edge_key >= 0, swap_line, 0.0), 15.0),
        swap - swap_line * LANES,
    )
    key_value = jnp.where(valid & (spot < LANES), bucket, -1).astype(F32)
    bucket_cells = cells(buckets, step * LANES)
    total = jnp.zeros((FAST * buckets, LANES), F32)
    for i in range(0, lines, step):
        here = bucket_cells == bf(wide(key_value, i))
        stack = jnp.concatenate([jnp.where(here, bf(wide(v, i)), zero) for v in values], axis=0)
        place = jnp.where(lane_cells == bf(jnp.minimum(wide(spot, i), 255.0)), one, zero)
        total = total + nt_dot(stack, place)
    for f in range(FAST):
        plan_ref[f] = total[f * buckets : (f + 1) * buckets, :]

    sent = slabs * geo.quarter

    def position(rank, source, use):
        quarter = jnp.floor((rank + 0.5) * (1.0 / geo.quarter))
        place = quarter * sent + source.astype(F32) * geo.quarter + (rank - quarter * geo.quarter)
        return jnp.where(use, place, 4.0 * sent + 8.0)

    here_slot = slot_of - me * owned
    owned_lines = owned // LANES
    slot_line = jnp.where(owner == me, here_slot >> 7, -1).astype(F32)
    slot_lane = (here_slot & 127).astype(F32)
    fields = []
    for place in (position(recv1, home, owner == me), position(recv2, home + 1, edge)):
        high = jnp.floor(place * (1.0 / 64.0))
        fields += [high, place - 64.0 * high]
    slot_cells = cells(owned_lines, step * LANES)
    pad = -(4 * owned_lines) % 16
    placed = jnp.zeros((4 * owned_lines + pad, LANES), F32)
    for i in range(0, lines, step):
        here = jnp.broadcast_to(wide(slot_line, i), (owned_lines, step * LANES)) == iota((owned_lines, step * LANES), 0).astype(F32)
        stack = [jnp.where(here, wide(v, i), 0.0) for v in fields]
        if pad:
            stack.append(jnp.zeros((pad, step * LANES), F32))
        place = jnp.where(lane_cells == bf(wide(slot_lane, i)), one, zero)
        placed = placed + nt_dot(bf(jnp.concatenate(stack, axis=0)), place)
    for f in range(2):
        at = 2 * f * owned_lines
        slot_ref[f] = placed[at : at + owned_lines] * 64.0 + placed[at + owned_lines : at + 2 * owned_lines]

    depth = geo.rows * geo.probes
    spill = None
    batch = loads // 2
    for g in reversed(range(rounds)):
        for j in range(loads):
            load(g, j).wait()
        group = list(reversed(range(g * batch, (g + 1) * batch)))
        parts = []
        for b in group:
            block = jnp.concatenate([tiles[2 * b].reshape(depth, LANES), tiles[2 * b + 1].reshape(depth, LANES)], axis=1)
            parts.append(jnp.dot(block, bucket_table(plan_ref, b), preferred_element_type=F32))
        for b, part in zip(group, parts):
            value = part[:, :LANES]
            if spill is not None:
                value = value + spill
            spill = part[:, LANES:]
            fold[b] = value
            terms = [fold[b, pl.ds(k, geo.probes, stride=geo.rows), :] * x for k, x in enumerate(row_weights(geo, plan_ref, b))]
            value_ref[b] = functools.reduce(jnp.add, terms)


def bucket_table(plan_ref, b):
    near, low, high = (plan_ref[f, pl.ds(b, 1), :] for f in range(3))
    grid = cells(COLS, LANES)
    zero = jnp.zeros((), BF16)
    main = jnp.where(grid == bf(near), bf(low), jnp.where(grid == bf(near + 1.0), bf(high), zero))
    if isinstance(b, int) and b == 0:
        return jnp.concatenate([main, jnp.zeros((COLS, LANES), BF16)], axis=1)
    before = b - 1 if isinstance(b, int) else jnp.maximum(b - 1, 0)
    last, spill = (plan_ref[f, pl.ds(before, 1), :] for f in (0, 2))
    spill = jnp.where(last == COLS - 1.0, spill, 0.0)
    over = bf(jnp.where(iota((16, LANES), 0) == 0, spill, 0.0))
    over = jnp.concatenate([over, jnp.zeros((COLS - 16, LANES), BF16)], axis=0)
    return jnp.concatenate([main, over], axis=1)


def place_code(plan_ref, b):
    code = plan_ref[7, pl.ds(b, 1), :]
    owner = jnp.floor(code * 0.125)
    return owner, code - 8.0 * owner


def row_weights(geo, plan_ref, b):
    rf = plan_ref[3, pl.ds(b, 1), :] + plan_ref[4, pl.ds(b, 1), :]
    _, rel = place_code(plan_ref, b)
    return [jnp.where(rel == k + 2.0, 1.0 - rf, jnp.where(rel == k + 1.0, rf, 0.0)) for k in range(geo.rows)]


def exchange_kernel(geo, r_ref, c_ref, rf_ref, cf_ref, w_ref, order_ref, field_ref, adjoint_ref, arrived_ref, slot_ref, total_ref, ok_ref, plan_ref, flag_ref, value_ref, tiles, hots, ranks, fold, edges, places, shares, inbox, packed, sources, raised, traces, sums, load_sem, swap_send, swap_recv, owner_send, owner_recv, trace_send, trace_recv, sum_send, sum_recv):
    slabs, groups, probes, rows, quarter, buckets = geo.slabs, geo.groups, geo.probes, geo.rows, geo.quarter, geo.buckets
    me, mine = lax.axis_index("slab"), lax.axis_index("probe")
    lines = geo.edge_lines
    zero = jnp.zeros((), BF16)
    batch = 8

    def at(slab, probe):
        return dict(device_id=(slab, probe), device_id_type=pl.DeviceIdType.MESH)

    barrier = pltpu.get_barrier_semaphore()
    for k in range(1, slabs):
        pl.semaphore_signal(barrier, inc=1, **at(lax.rem(me + k, slabs), mine))
    for k in range(1, groups):
        pl.semaphore_signal(barrier, inc=1, **at(me, lax.rem(mine + k, groups)))

    observe(geo, me, r_ref, c_ref, rf_ref, cf_ref, w_ref, order_ref, field_ref, plan_ref, slot_ref, flag_ref, value_ref, tiles, hots, ranks, fold, load_sem)

    def columns(j):
        return slice(j * LANES, (j + 1) * LANES)

    def edge_fields(b):
        _, rel = place_code(plan_ref, b)
        line = jnp.floor(plan_ref[9, pl.ds(b, 1), :] * (1.0 / 16.0))
        lane = plan_ref[10, pl.ds(b, 1), :]
        return rel, line, lane

    def weight_of(b):
        return plan_ref[5, pl.ds(b, 1), :] + plan_ref[6, pl.ds(b, 1), :]

    share_rows = shares.shape[0]

    found = None
    for g in range(buckets // batch):
        stacks, spots = [], []
        for j in range(batch):
            b = g * batch + j
            rel, line, lane = edge_fields(b)
            low, high = rel == 1.0, rel == rows + 1.0
            spot = match(2 * LANES, jnp.where(low, lane, jnp.where(high, lane + LANES, -1.0)))
            value = value_ref[b]
            share = jnp.where((iota((share_rows, LANES), 0).astype(F32) == line) & high, weight_of(b), 0.0)
            stacks.append(jnp.concatenate([bf(jnp.where(line == float(l), value, 0.0)) for l in range(lines)] + [bf(share)], axis=0))
            spots.append(spot)
            places[b] = spot
        part = nt_dot(jnp.concatenate(stacks, axis=1), jnp.concatenate(spots, axis=1))
        found = part if found is None else found + part
    for side in range(2):
        edges[side] = found[: lines * probes, columns(side)]
    shares[...] = found[lines * probes :, columns(1)]

    pl.semaphore_wait(barrier, slabs + groups - 2)
    down, up = lax.rem(me + slabs - 1, slabs), lax.rem(me + 1, slabs)
    swaps = [
        pltpu.make_async_remote_copy(
            src_ref=edges.at[side], dst_ref=inbox.at[1 - side], send_sem=swap_send.at[side], recv_sem=swap_recv.at[side], **at(peer, mine)
        )
        for side, peer in ((0, down), (1, up))
    ]
    for copy in swaps:
        copy.start()

    packed[...] = jnp.zeros_like(packed)

    def pack(g, squares):
        hots, quads = [], []
        for j in range(batch):
            b = g * batch + j
            owner, rel = place_code(plan_ref, b)
            code = plan_ref[9, pl.ds(b, 1), :]
            fourth = code - 16.0 * jnp.floor(code * (1.0 / 16.0))
            row = jnp.where(rel > 0.0, owner * quarter + plan_ref[8, pl.ds(b, 1), :], -1.0)
            hots.append(match(slabs * quarter, row))
            value = value_ref[b]
            squares = squares + value * value * weight_of(b)
            quads.append(jnp.concatenate([bf(jnp.where(fourth == float(k), value, 0.0)) for k in range(4)], axis=0))
        part = nt_dot(jnp.concatenate(hots, axis=1), jnp.concatenate(quads, axis=1))
        packed[...] += part.reshape(packed.shape)
        return squares

    squares = lax.fori_loop(0, buckets // batch, pack, jnp.zeros((probes, LANES), F32))

    def owner_copy(k, source, peer):
        return pltpu.make_async_remote_copy(
            src_ref=packed.at[peer], dst_ref=arrived_ref.at[source], send_sem=owner_send.at[k], recv_sem=owner_recv.at[k], **at(peer, mine)
        )

    for k in range(1, slabs):
        owner_copy(k, me, lax.rem(me + k, slabs)).start()
    arrived_ref[me] = packed[me]

    for copy in swaps:
        copy.wait()
    for l in range(lines):
        part = slice(l * probes, (l + 1) * probes)
        squares = squares + edges[1, part] * inbox[1, part] * (2.0 * shares[l : l + 1])
    folded = squares[:8]
    for d in range(8, probes, 8):
        folded = folded + squares[d : d + 8]
    traces[mine] = jnp.concatenate([folded, flag_ref[...]], axis=0)

    def trace_copy(k, source, peer):
        return pltpu.make_async_remote_copy(
            src_ref=traces.at[mine], dst_ref=traces.at[source], send_sem=trace_send.at[k], recv_sem=trace_recv.at[k], **at(me, peer)
        )

    for k in range(1, groups):
        trace_copy(k, mine, lax.rem(mine + k, groups)).start()

    both = bf(jnp.concatenate([inbox[0], inbox[1]], axis=1))
    sources[0] = jnp.zeros_like(sources[0])

    @pl.loop(0, buckets // batch)
    def _(g):
        spots = jnp.concatenate([places[g * batch + j] for j in range(batch)], axis=1)
        extra = jnp.dot(both, spots, preferred_element_type=F32)
        for j in range(batch):
            b = g * batch + j
            _, line, _ = edge_fields(b)
            full = value_ref[b]
            for l in range(lines):
                full = full + jnp.where(line == float(l), extra[l * probes : (l + 1) * probes, columns(j)], 0.0)
            spread = full * weight_of(b)
            for k, weight in enumerate(row_weights(geo, plan_ref, b)):
                raised[j, pl.ds(k, probes, stride=rows), :] = spread * weight
            sources[b + 1] = bf(raised[j])

    def spread_back(g):
        parts = []
        for j in range(batch):
            b = g * batch + j
            source = jnp.concatenate([sources[b + 1], sources[b]], axis=1)
            parts.append(nt_dot(source, bucket_table(plan_ref, b)))
        for j in range(batch):
            for t in range(2):
                adjoint_ref[2 * (g * batch + j) + t] = bf(parts[j][:, columns(t)]).reshape(probes, rows, LANES)

    rounds = buckets // batch
    early = max(1, rounds * EARLY // 4)
    pl.loop(0, early)(spread_back)
    for k in range(1, groups):
        source = lax.rem(mine + groups - k, groups)
        trace_copy(k, source, source).wait()
    sums[me] = jnp.sum(traces[...], axis=0)

    def sum_copy(k, source, peer):
        return pltpu.make_async_remote_copy(
            src_ref=sums.at[me], dst_ref=sums.at[source], send_sem=sum_send.at[k], recv_sem=sum_recv.at[k], **at(peer, mine)
        )

    for k in range(1, slabs):
        sum_copy(k, me, lax.rem(me + k, slabs)).start()

    if early < rounds:
        pl.loop(early, rounds)(spread_back)
    for k in range(1, slabs):
        source = lax.rem(me + slabs - k, slabs)
        owner_copy(k, source, source).wait()
    for k in range(1, slabs):
        source = lax.rem(me + slabs - k, slabs)
        sum_copy(k, source, source).wait()
    total = jnp.sum(sums[...], axis=0)
    total_ref[...] = total
    ok_ref[0] = jnp.max(total[8:]).astype(jnp.int32)


def deliver_kernel(geo, scale, adjoint_ref, arrived_ref, slot_ref, total_ref, out_ref, observed_ref, mean_ref, observed, sem):
    slabs, probes, quarter, owned = geo.slabs, geo.probes, geo.quarter, geo.owned
    loads = 8

    def store(t):
        return pltpu.make_async_copy(adjoint_ref.at[t], out_ref.at[:, t], sem.at[0])

    for t in range(geo.tiles):
        store(t).start()
    sent = slabs * quarter
    arrived = jnp.transpose(arrived_ref[...].reshape(sent, 4 * probes))
    lines = owned // LANES
    spots = [jnp.concatenate([slot_ref[f, l : l + 1, :] for l in range(lines)], axis=1) for f in range(2)]
    total = jnp.zeros((probes, owned), F32)
    for k in range(4):
        hot = match(sent, spots[0] - float(k * sent)) + match(sent, spots[1] - float(k * sent))
        total = total + jnp.dot(bf(arrived[k * probes : (k + 1) * probes]), hot, preferred_element_type=F32)
    observed[...] = total
    pltpu.make_async_copy(observed, observed_ref, sem.at[1]).start()
    summed = jnp.sum(total_ref[:8], axis=0, keepdims=True)
    mean_ref[...] = jnp.broadcast_to(jnp.sum(summed, axis=1, keepdims=True) * scale, mean_ref.shape)
    pltpu.make_async_copy(observed, observed_ref, sem.at[1]).wait()
    for t in range(geo.tiles):
        store(t).wait()


def geometry(slabs, groups, probe_fields, sensors):
    probes, rows, width = probe_fields.shape
    most = min(sensors, 4 * sensors // slabs)
    quarter = -(-(most // slabs + 32) // 32) * 8
    edge_lines = -(-5 * most // (4 * rows * LANES))
    buckets = width // COLS
    return Geo(rows, probes, slabs, groups, buckets, width // LANES, sensors // LANES, sensors // slabs, quarter, edge_lines, buckets + 2 * slabs + 16)


def body(slab_count, probe_groups, probe_fields, *vectors):
    sensors = vectors[0].shape[0]
    geo = geometry(slab_count, probe_groups, probe_fields, sensors)
    probes, rows, width = probe_fields.shape
    depth = probes * rows
    lines, buckets, tiles = geo.lines, geo.buckets, geo.tiles
    boxed = [x.reshape(lines, LANES) for x in vectors]
    field = probe_fields.reshape(probes, rows, tiles, LANES).transpose(0, 2, 1, 3)
    vmem = pl.BlockSpec(memory_space=VMEM)
    smem = pl.BlockSpec(memory_space=SMEM)
    hbm = pl.BlockSpec(memory_space=pltpu.HBM)
    dma = pltpu.SemaphoreType.DMA
    shape = jax.ShapeDtypeStruct
    edge_rows = geo.edge_lines * probes
    adjoint, arrived, slots, total, flag = pl.pallas_call(
        functools.partial(exchange_kernel, geo),
        out_shape=(
            shape((tiles, probes, rows, LANES), BF16),
            shape((slab_count, geo.quarter, 4 * probes), F32),
            shape((2, geo.owned // LANES, LANES), F32),
            shape((16, LANES), F32),
            shape((1,), jnp.int32),
        ),
        in_specs=[vmem] * 6 + [hbm],
        out_specs=(vmem, vmem, vmem, vmem, smem),
        scratch_shapes=[
            VMEM((FAST, buckets, LANES), F32),
            VMEM((8, LANES), F32),
            VMEM((buckets, probes, LANES), F32),
            VMEM((tiles, probes, rows, LANES), BF16),
            VMEM((lines * geo.kinds, LANES), BF16),
            VMEM((5, lines, LANES), F32),
            VMEM((buckets, depth, LANES), F32),
            VMEM((2, edge_rows, LANES), F32),
            VMEM((buckets, 2 * LANES, LANES), BF16),
            VMEM((-(-geo.edge_lines // 16) * 16, LANES), F32),
            VMEM((2, edge_rows, LANES), F32),
            VMEM((slab_count, geo.quarter, 4 * probes), F32),
            VMEM((buckets + 1, depth, LANES), BF16),
            VMEM((8, depth, LANES), F32),
            VMEM((probe_groups, 16, LANES), F32),
            VMEM((slab_count, 16, LANES), F32),
            dma((tiles // 8,)),
            dma((2,)),
            dma((2,)),
            dma((slab_count,)),
            dma((slab_count,)),
            dma((probe_groups,)),
            dma((probe_groups,)),
            dma((slab_count,)),
            dma((slab_count,)),
        ],
        compiler_params=pltpu.CompilerParams(collective_id=3, has_side_effects=True, vmem_limit_bytes=ROOM),
        name="exchange",
    )(*boxed, field)
    out, observed, mean = pl.pallas_call(
        functools.partial(deliver_kernel, geo, 1.0 / (probes * probe_groups * sensors)),
        out_shape=(
            shape((probes, tiles, rows, LANES), BF16),
            shape((probes, geo.owned), F32),
            shape((1, LANES), F32),
        ),
        in_specs=[vmem] * 4,
        out_specs=(hbm, hbm, vmem),
        scratch_shapes=[VMEM((probes, geo.owned), F32), dma((2,))],
        compiler_params=SMALL,
        name="deliver",
    )(adjoint, arrived, slots, total)
    out = out.transpose(0, 2, 1, 3).reshape(probes, rows, width)

    def again(state):
        out, observed, mean = general(slab_count, probe_groups, probe_fields, *vectors)
        return out, jnp.where(state[3] > 0, observed, state[1]), mean, state[3] * 0

    state = lax.while_loop(lambda state: state[3] != 0, again, (out, observed, mean[0, 0], flag[0]))
    return state[:3]


def solution(mesh):
    placed = (P("probe", "slab", None), P(), P(), P(), P(), P(), P())
    return jax.shard_map(
        functools.partial(body, mesh.shape["slab"], mesh.shape["probe"]),
        mesh=mesh,
        in_specs=placed,
        out_specs=(P("probe", "slab", None), P("probe", "slab"), P()),
        check_vma=False,
    )
```

```python
import functools
import typing

import jax
import jax.numpy as jnp
from jax import lax
from jax.experimental import pallas as pl
from jax.experimental.pallas import tpu as pltpu
from jax.sharding import PartitionSpec as P

LANES = 128
BLOCK = 1024
HALF = 256
FIELDS = 11
F32 = jnp.float32
BF16 = jnp.bfloat16
NT = (((1,), (1,)), ((), ()))
VMEM = pltpu.VMEM
SMEM = pltpu.SMEM
LIMIT = pltpu.CompilerParams(vmem_limit_bytes=60 * 1024 * 1024)


def iota(shape, dim):
    return lax.broadcasted_iota(jnp.int32, shape, dim)


def nt_dot(a, b):
    return lax.dot_general(a, b, NT, preferred_element_type=F32)


def plan_kernel(rows, cap_chunks, blocks, slabs, pair_lines, me_ref, r_ref, c_ref, rf_ref, cf_ref, w_ref, order_ref, plan_ref, marks_ref, places_ref, peak_ref):
    lines = r_ref.shape[0]
    sensors = lines * LANES
    step = min(4, lines)
    me = me_ref[0]
    first = me * rows
    owned = lines * LANES // slabs
    keys_group = 2 * blocks
    keys = 3 * keys_group
    chunks = 3 * cap_chunks

    def wide(x, i):
        return jnp.concatenate([x[i + j : i + j + 1, :] for j in range(step)], axis=1)

    order = order_ref[...]
    slot = iota((lines, LANES), 0) * LANES + iota((lines, LANES), 1)
    found = jnp.zeros((2 * lines, LANES), F32)
    for i in range(0, lines, step):
        target = wide(order, i)
        mine = wide(slot, i)
        here = iota((lines, step * LANES), 0) == (target >> 7)
        stack = jnp.concatenate(
            [jnp.where(here, (mine >> 7).astype(F32), 0.0), jnp.where(here, (mine & 127).astype(F32), 0.0)], axis=0
        ).astype(BF16)
        place = jnp.where(iota((LANES, step * LANES), 0) == (target & 127), 1.0, 0.0).astype(BF16)
        found = found + nt_dot(stack, place)
    slot_hi = found[:lines, :]
    slot_lo = found[lines:, :]

    r = r_ref[...]
    c = c_ref[...]
    rel = r - first + 1
    valid = (rel >= 0) & (rel <= rows)
    group = jnp.where(rel == 0, 0, jnp.where(rel == rows, 2, 1))
    block = c // BLOCK
    inner = c - block * BLOCK
    half = c // HALF
    slot_of = (slot_hi * LANES + slot_lo).astype(jnp.int32)
    owner = slot_of // owned
    home = r // rows
    send_key = jnp.where(home == me, owner, -1)
    recv_key = jnp.where(owner == me, home, -1)
    edge = jnp.where(r - home * rows == rows - 1, home, -1)
    edges = jnp.zeros((slabs, LANES), F32)
    for i in range(lines):
        edges = edges + jnp.where(iota((slabs, LANES), 0) == edge[i : i + 1, :], 1.0, 0.0)
    peak_ref[0] = jnp.max(jnp.sum(edges, axis=1, keepdims=True)).astype(jnp.int32)
    key = group * keys_group + 2 * block + jnp.where(inner == BLOCK - 1, 1, 0)
    key = jnp.where(valid, key, -1)

    count = jnp.zeros((keys, 1), F32)
    for i in range(lines):
        count = count + jnp.sum(jnp.where(iota((keys, LANES), 0) == key[i : i + 1, :], 1.0, 0.0), axis=1, keepdims=True)
    big = jnp.floor(count * (1.0 / 64.0))
    small = count - 64.0 * big
    ka, kb = iota((keys, keys), 0), iota((keys, keys), 1)
    below = jnp.where((kb < ka) & (kb // keys_group == ka // keys_group), 1.0, 0.0).astype(BF16)
    start = 64.0 * jnp.dot(below, jnp.broadcast_to(big, (keys, LANES)).astype(BF16), preferred_element_type=F32)
    start = start + jnp.dot(below, jnp.broadcast_to(small, (keys, LANES)).astype(BF16), preferred_element_type=F32)
    start = start + ((iota((keys, LANES), 0) // keys_group) * (cap_chunks * LANES)).astype(F32)
    wide_keys = marks_ref.shape[1]
    diagonal = iota((keys, wide_keys), 0) == iota((keys, wide_keys), 1)
    marks_ref[...] = jnp.concatenate(
        [jnp.sum(jnp.where(diagonal, x, 0.0), axis=0, keepdims=True) for x in (start[:, :1], start[:, :1] + count)], axis=0
    ).astype(jnp.int32)

    upper = jnp.where(iota((LANES, LANES), 0) < iota((LANES, LANES), 1), 1.0, 0.0).astype(BF16)
    carry = jnp.concatenate([start[:, :1], jnp.zeros((2 * slabs, 1), F32)], axis=0)
    spots, sends, recvs = [], [], []
    for i in range(lines):
        hot = jnp.concatenate(
            [
                jnp.where(iota((keys, LANES), 0) == key[i : i + 1, :], 1.0, 0.0),
                jnp.where(iota((slabs, LANES), 0) == send_key[i : i + 1, :], 1.0, 0.0),
                jnp.where(iota((slabs, LANES), 0) == recv_key[i : i + 1, :], 1.0, 0.0),
            ],
            axis=0,
        )
        before = jnp.dot(hot.astype(BF16), upper, preferred_element_type=F32)
        ranks = hot * (before + carry)
        spots.append(jnp.sum(ranks[:keys], axis=0, keepdims=True))
        sends.append(jnp.sum(ranks[keys : keys + slabs], axis=0, keepdims=True))
        recvs.append(jnp.sum(ranks[keys + slabs :], axis=0, keepdims=True))
        carry = carry + jnp.sum(hot, axis=1, keepdims=True)
    spot = jnp.concatenate(spots, axis=0).astype(jnp.int32)
    spot = jnp.where(valid, spot, -1)
    send = jnp.concatenate(sends, axis=0).astype(jnp.int32)
    recv = jnp.concatenate(recvs, axis=0).astype(jnp.int32)
    send_line = jnp.where(send_key >= 0, owner * pair_lines + (send >> 7), 200)
    recv_line = jnp.where(recv_key >= 0, home * pair_lines + (recv >> 7), -1)

    rf = rf_ref[...]
    cf = cf_ref[...]
    w = w_ref[...]
    rf_top = rf.astype(BF16).astype(F32)
    w_top = w.astype(BF16).astype(F32)
    values = [
        half.astype(F32),
        (c - half * HALF).astype(F32),
        (1.0 - cf).astype(BF16).astype(F32),
        cf.astype(BF16).astype(F32),
        rf_top,
        rf - rf_top,
        w_top,
        w - w_top,
        rel.astype(F32),
        send_line.astype(F32),
        (send & 127).astype(F32),
    ]
    total = jnp.zeros((FIELDS * chunks, LANES), F32)
    for i in range(0, lines, step):
        target = wide(spot, i)
        here = iota((chunks, step * LANES), 0) == (target >> 7)
        stack = jnp.concatenate([jnp.where(here, wide(v, i), 0.0) for v in values], axis=0).astype(BF16)
        place = jnp.where(iota((LANES, step * LANES), 0) == (target & 127), 1.0, 0.0).astype(BF16)
        total = total + nt_dot(stack, place)
    for f in range(FIELDS):
        plan_ref[f] = total[f * chunks : (f + 1) * chunks, :]

    slot_here = slot_of - me * owned
    received = slabs * pair_lines
    found = jnp.zeros((2 * received, LANES), F32)
    for i in range(0, lines, step):
        here = iota((received, step * LANES), 0) == wide(recv_line, i)
        target = wide(slot_here, i)
        stack = jnp.concatenate(
            [jnp.where(here, (target >> 7).astype(F32), 0.0), jnp.where(here, (target & 127).astype(F32), 0.0)], axis=0
        ).astype(BF16)
        place = jnp.where(iota((LANES, step * LANES), 0) == (wide(recv, i) & 127), 1.0, 0.0).astype(BF16)
        found = found + nt_dot(stack, place)
    places_ref[...] = (found[:received] * LANES + found[received:]).astype(jnp.int32)


def column_table(plan_ref, chunk, number):
    line = pl.ds(chunk, 1)
    column = plan_ref[0, line, :] * HALF + plan_ref[1, line, :] - (number * BLOCK).astype(F32)
    low = plan_ref[2, line, :].astype(BF16)
    high = plan_ref[3, line, :].astype(BF16)
    cells = iota((HALF, LANES), 0).astype(F32).astype(BF16)
    pieces = []
    for begin in range(0, BLOCK, HALF):
        near = jnp.clip(column - begin, -2.0, HALF).astype(BF16)
        after = jnp.clip(column - (begin - 1), -2.0, HALF).astype(BF16)
        pieces.append(jnp.where(cells == near, low, jnp.where(cells == after, high, jnp.zeros((), BF16))))
    return jnp.concatenate(pieces, axis=0)


def row_pattern(plan_ref, chunk, rows, depth):
    line = pl.ds(chunk, 1)
    rf = plan_ref[4, line, :] + plan_ref[5, line, :]
    rel = plan_ref[8, line, :].astype(jnp.int32)
    row = iota((depth, LANES), 0) % rows + 1
    return jnp.where(row == rel, 1.0 - rf, jnp.where(row == rel + 1, rf, 0.0))


def group_chunks(marks_ref, group, keys_group, base):
    count = (marks_ref[1, (group + 1) * keys_group - 1] - base + LANES - 1) // LANES
    return jnp.maximum(count, 1)


def chunk_range(marks_ref, group, number, keys_group, cap_chunks):
    at = group * keys_group + 2 * number
    begin = marks_ref[0, jnp.maximum(at - 1, group * keys_group)]
    end = marks_ref[1, at + 1]
    base = group * cap_chunks
    last = base + group_chunks(marks_ref, group, keys_group, base * LANES) - 1
    return jnp.minimum(begin // LANES, last), jnp.where(end > begin, (end + LANES - 1) // LANES, 0)


def forward_kernel(cap_chunks, blocks, field_ref, plan_ref, marks_ref, value_ref, sums, flat):
    probes, rows, _ = field_ref.shape
    depth = probes * rows
    keys_group = 2 * blocks
    number = pl.program_id(0)
    counts = [group_chunks(marks_ref, g, keys_group, g * cap_chunks * LANES) for g in range(3)]

    @pl.when(number == 0)
    def _():
        for g in range(3):

            @pl.loop(0, counts[g])
            def _(k):
                sums[g * cap_chunks + k] = jnp.zeros((depth, LANES), F32)

    block = field_ref[...].reshape(depth, BLOCK)
    flat[...] = block
    ranges = [chunk_range(marks_ref, g, number, keys_group, cap_chunks) for g in range(3)]
    table = jnp.concatenate([column_table(plan_ref, begin, number) for begin, _ in ranges], axis=1)
    part = jnp.dot(block, table, preferred_element_type=F32)
    for g in range(3):
        sums[ranges[g][0]] += part[:, g * LANES : (g + 1) * LANES]
    for g in range(3):

        @pl.loop(ranges[g][0] + 1, ranges[g][1])
        def _(chunk):
            sums[chunk] += jnp.dot(flat[...], column_table(plan_ref, chunk, number), preferred_element_type=F32)

    @pl.when(number == blocks - 1)
    def _():
        fold = jnp.where(iota((probes, depth), 1) // rows == iota((probes, depth), 0), 1.0, 0.0).astype(BF16)
        for g in range(3):

            @pl.loop(0, counts[g])
            def _(k):
                chunk = g * cap_chunks + k
                scaled = (sums[chunk] * row_pattern(plan_ref, chunk, rows, depth)).astype(BF16)
                value_ref[chunk] = jnp.dot(fold, scaled, preferred_element_type=F32)


def swap_kernel(slabs, top, value_ref, above_ref, below_ref, send_sem, recv_sem):
    probe, me = lax.axis_index("probe"), lax.axis_index("slab")
    width = above_ref.shape[0]
    down, up = lax.rem(me + slabs - 1, slabs), lax.rem(me + 1, slabs)
    barrier = pltpu.get_barrier_semaphore()
    for peer in (down, up):
        pl.semaphore_signal(barrier, inc=1, device_id=(peer, probe), device_id_type=pl.DeviceIdType.MESH)
    pl.semaphore_wait(barrier, 2)
    copies = []
    for k, (peer, begin, target) in enumerate(((down, 0, above_ref), (up, top, below_ref))):
        copies.append(
            pltpu.make_async_remote_copy(
                src_ref=value_ref.at[begin : begin + width],
                dst_ref=target,
                send_sem=send_sem.at[k],
                recv_sem=recv_sem.at[k],
                device_id=(peer, probe),
                device_id_type=pl.DeviceIdType.MESH,
            )
        )
    for copy in copies:
        copy.start()
    for copy in copies:
        copy.wait()


def swap(slabs, cap_chunks, width, number, value):
    part = (width, *value.shape[1:])
    any_space = pl.BlockSpec(memory_space=pl.ANY)
    above, below = pl.pallas_call(
        functools.partial(swap_kernel, slabs, 2 * cap_chunks),
        out_shape=(jax.ShapeDtypeStruct(part, F32), jax.ShapeDtypeStruct(part, F32)),
        in_specs=[any_space],
        out_specs=(any_space, any_space),
        scratch_shapes=[pltpu.SemaphoreType.DMA((2,)), pltpu.SemaphoreType.DMA((2,))],
        compiler_params=pltpu.CompilerParams(collective_id=number, has_side_effects=True),
        name="swap",
    )(value)
    return above, below


def merge_kernel(cap_chunks, blocks, value_ref, above_ref, below_ref, plan_ref, marks_ref, spread_ref, packed_ref, squares, parts):
    slabs = packed_ref.shape[0]
    outgoing, probes, _ = parts.shape
    lines = outgoing // slabs
    keys_group = 2 * blocks
    squares[...] = jnp.zeros_like(squares)
    parts[...] = jnp.zeros_like(parts)
    for g in range(3):
        count = group_chunks(marks_ref, g, keys_group, g * cap_chunks * LANES)

        @pl.loop(0, count)
        def _(k):
            chunk = g * cap_chunks + k
            value = value_ref[chunk]
            if g == 0:
                value = value + below_ref[k]
            if g == 2:
                value = value + above_ref[k]
            line = pl.ds(chunk, 1)
            spread = value * (plan_ref[6, line, :] + plan_ref[7, line, :])
            spread_ref[chunk] = spread.astype(BF16)
            if g > 0:
                squares[...] += spread * value
                high = plan_ref[9, line, :].astype(jnp.int32)
                low = plan_ref[10, line, :].astype(jnp.int32)
                place = jnp.where(iota((LANES, LANES), 0) == low, 1.0, 0.0).astype(BF16)
                stack = jnp.concatenate([jnp.where(high == d, value, 0.0) for d in range(outgoing)], axis=0).astype(BF16)
                parts[...] += nt_dot(stack, place).reshape(outgoing, probes, LANES)

    folded = squares[:8, :]
    for d in range(8, probes, 8):
        folded = folded + squares[d : d + 8, :]
    for d in range(slabs):
        for e in range(lines):
            packed_ref[d, e * probes : (e + 1) * probes, :] = parts[d * lines + e]
        packed_ref[d, lines * probes :, :] = folded


def unpack_kernel(groups, scale, packed_ref, places_ref, observed_ref, mean_ref, traces, send_sem, recv_sem):
    slab, me = lax.axis_index("slab"), lax.axis_index("probe")
    slabs = packed_ref.shape[0]
    probes, owned = observed_ref.shape
    lines = places_ref.shape[0] // slabs
    barrier = pltpu.get_barrier_semaphore()
    for k in range(1, groups):
        peer = lax.rem(me + k, groups)
        pl.semaphore_signal(barrier, inc=1, device_id=(slab, peer), device_id_type=pl.DeviceIdType.MESH)
    own = packed_ref[0, lines * probes :, :]
    for d in range(1, slabs):
        own = own + packed_ref[d, lines * probes :, :]
    traces[me] = own
    pl.semaphore_wait(barrier, groups - 1)

    def tile(k, source, peer):
        return pltpu.make_async_remote_copy(
            src_ref=traces.at[me],
            dst_ref=traces.at[source],
            send_sem=send_sem.at[k],
            recv_sem=recv_sem.at[k],
            device_id=(slab, peer),
            device_id_type=pl.DeviceIdType.MESH,
        )

    for k in range(1, groups):
        tile(k, me, lax.rem(me + k, groups)).start()
    total = jnp.zeros((probes, owned), F32)
    for d in range(slabs):
        for e in range(lines):
            at = d * lines + e
            place = jnp.where(iota((owned, LANES), 0) == places_ref[at : at + 1, :], 1.0, 0.0).astype(BF16)
            total = total + nt_dot(packed_ref[d, e * probes : (e + 1) * probes, :].astype(BF16), place)
    observed_ref[...] = total
    for k in range(1, groups):
        source = lax.rem(me + groups - k, groups)
        tile(k, source, source).wait()
    summed = jnp.sum(jnp.sum(traces[...], axis=0), axis=0, keepdims=True)
    mean_ref[...] = jnp.broadcast_to(jnp.sum(summed, axis=1, keepdims=True) * scale, mean_ref.shape)


def adjoint_kernel(cap_chunks, blocks, spread_ref, plan_ref, marks_ref, out_ref, sources, total):
    probes, rows, _ = out_ref.shape
    depth = probes * rows
    keys_group = 2 * blocks
    number = pl.program_id(0)

    @pl.when(number == 0)
    def _():
        raise_rows = jnp.where(iota((depth, probes), 0) // rows == iota((depth, probes), 1), 1.0, 0.0).astype(BF16)
        for g in range(3):
            count = group_chunks(marks_ref, g, keys_group, g * cap_chunks * LANES)

            @pl.loop(0, count)
            def _(k):
                chunk = g * cap_chunks + k
                raised = jnp.dot(raise_rows, spread_ref[chunk], preferred_element_type=F32)
                sources[chunk] = (raised * row_pattern(plan_ref, chunk, rows, depth)).astype(BF16)

    ranges = [chunk_range(marks_ref, g, number, keys_group, cap_chunks) for g in range(3)]
    table = jnp.concatenate([column_table(plan_ref, begin, number) for begin, _ in ranges], axis=1)
    source = jnp.concatenate([sources[begin] for begin, _ in ranges], axis=1)
    total[...] = nt_dot(source, table)
    for g in range(3):

        @pl.loop(ranges[g][0] + 1, ranges[g][1])
        def _(chunk):
            total[...] += nt_dot(sources[chunk], column_table(plan_ref, chunk, number))

    out_ref[...] = total[...].astype(BF16).reshape(probes, rows, BLOCK)


def general(slab_count, probe_groups, probe_fields, sensor_rows, sensor_cols, row_frac, col_frac, sensor_weights, owner_order):
    probes, rows, width = probe_fields.shape
    sensors = sensor_rows.shape[0]
    depth = probes * rows
    lines = sensors // LANES
    blocks = width // BLOCK
    keys = 6 * blocks
    most = min(sensors, 4 * sensors // slab_count)
    cap_chunks = -(-most // (8 * LANES)) * 8
    chunks = 3 * cap_chunks
    pair_lines = -(-most // (slab_count * LANES))
    outgoing = slab_count * pair_lines
    me = jnp.reshape(lax.axis_index("slab"), (1,)).astype(jnp.int32)
    boxed = [x.reshape(lines, LANES) for x in (sensor_rows, sensor_cols, row_frac, col_frac, sensor_weights, owner_order)]
    vmem = pl.BlockSpec(memory_space=VMEM)
    smem = pl.BlockSpec(memory_space=SMEM)
    plan, marks, places, peak = pl.pallas_call(
        functools.partial(plan_kernel, rows, cap_chunks, blocks, slab_count, pair_lines),
        out_shape=(
            jax.ShapeDtypeStruct((FIELDS, chunks, LANES), F32),
            jax.ShapeDtypeStruct((2, -(-keys // LANES) * LANES), jnp.int32),
            jax.ShapeDtypeStruct((outgoing, LANES), jnp.int32),
            jax.ShapeDtypeStruct((1,), jnp.int32),
        ),
        in_specs=[smem] + [vmem] * 6,
        out_specs=(vmem, vmem, vmem, smem),
        compiler_params=LIMIT,
        name="plan",
    )(me, *boxed)
    value = pl.pallas_call(
        functools.partial(forward_kernel, cap_chunks, blocks),
        out_shape=jax.ShapeDtypeStruct((chunks, probes, LANES), F32),
        grid=(blocks,),
        in_specs=[pl.BlockSpec((probes, rows, BLOCK), lambda n: (0, 0, n)), vmem, smem],
        out_specs=vmem,
        scratch_shapes=[VMEM((chunks, depth, LANES), F32), VMEM((depth, BLOCK), BF16)],
        compiler_params=LIMIT,
        name="forward",
    )(probe_fields, plan, marks)
    few = min(cap_chunks, -(-5 * most // (4 * rows * LANES)))

    def merged(above, below):
        return pl.pallas_call(
            functools.partial(merge_kernel, cap_chunks, blocks),
            out_shape=(
                jax.ShapeDtypeStruct((chunks, probes, LANES), BF16),
                jax.ShapeDtypeStruct((slab_count, pair_lines * probes + 8, LANES), F32),
            ),
            in_specs=[vmem, vmem, vmem, vmem, smem],
            out_specs=(vmem, vmem),
            scratch_shapes=[VMEM((probes, LANES), F32), VMEM((outgoing, probes, LANES), F32)],
            compiler_params=LIMIT,
            name="merge",
        )(value, above, below, plan, marks)

    spread, packed = lax.cond(
        peak[0] <= few * LANES,
        lambda: merged(*swap(slab_count, cap_chunks, few, 0, value)),
        lambda: merged(*swap(slab_count, cap_chunks, cap_chunks, 1, value)),
    )
    arrived = lax.all_to_all(packed, "slab", 0, 0, tiled=True)
    adjoint = pl.pallas_call(
        functools.partial(adjoint_kernel, cap_chunks, blocks),
        out_shape=jax.ShapeDtypeStruct((probes, rows, width), BF16),
        grid=(blocks,),
        in_specs=[vmem, vmem, smem],
        out_specs=pl.BlockSpec((probes, rows, BLOCK), lambda n: (0, 0, n)),
        scratch_shapes=[
            VMEM((chunks, depth, LANES), BF16),
            VMEM((depth, BLOCK), F32),
        ],
        compiler_params=LIMIT,
        cost_estimate=pl.CostEstimate(flops=4 * 10**9, bytes_accessed=8 * 10**6, transcendentals=0),
        name="adjoint",
    )(spread, plan, marks)
    observed, mean = pl.pallas_call(
        functools.partial(unpack_kernel, probe_groups, 1.0 / (probes * probe_groups * sensors)),
        out_shape=(
            jax.ShapeDtypeStruct((probes, sensors // slab_count), F32),
            jax.ShapeDtypeStruct((1, LANES), F32),
        ),
        in_specs=[vmem, vmem],
        out_specs=(vmem, vmem),
        scratch_shapes=[
            VMEM((probe_groups, 8, LANES), F32),
            pltpu.SemaphoreType.DMA((probe_groups,)),
            pltpu.SemaphoreType.DMA((probe_groups,)),
        ],
        compiler_params=pltpu.CompilerParams(collective_id=2, has_side_effects=True, vmem_limit_bytes=40 * 1024 * 1024),
        name="unpack",
    )(arrived, places)
    return adjoint, observed, mean[0, 0]


COLS = 256
FAST = 11
EARLY = 3
ROOM = 36 * 1024 * 1024
SMALL = pltpu.CompilerParams(vmem_limit_bytes=ROOM)


class Geo(typing.NamedTuple):
    rows: int
    probes: int
    slabs: int
    groups: int
    buckets: int
    tiles: int
    lines: int
    owned: int
    quarter: int
    edge_lines: int
    kinds: int


def bf(x):
    return x.astype(BF16)


def cells(rows, width):
    return bf(iota((rows, width), 0).astype(F32))


def match(rows, target):
    grid = cells(min(rows, COLS), target.shape[1])
    pieces = []
    for begin in range(0, rows, COLS):
        size = min(COLS, rows - begin)
        near = bf(jnp.clip(target - begin, -1.0, float(COLS)))
        pieces.append(jnp.where(grid[:size] == near, jnp.ones((), BF16), jnp.zeros((), BF16)))
    return pieces[0] if len(pieces) == 1 else jnp.concatenate(pieces, axis=0)


def observe(geo, me, r_ref, c_ref, rf_ref, cf_ref, w_ref, order_ref, field_ref, plan_ref, slot_ref, flag_ref, value_ref, tiles, hots, ranks, fold, sem):
    lines, slabs, buckets, owned = geo.lines, geo.slabs, geo.buckets, geo.owned
    loads = 8
    rounds = geo.tiles // loads

    def load(g, j):
        t = g * loads + j
        return pltpu.make_async_copy(field_ref.at[:, t], tiles.at[t], sem.at[g])

    for g in reversed(range(rounds)):
        for j in range(loads):
            load(g, j).start()

    step = min(4, lines)
    kinds = geo.kinds

    def wide(x, i):
        return jnp.concatenate([x[i + j : i + j + 1, :] for j in range(step)], axis=1)

    order = order_ref[...]
    slot = iota((lines, LANES), 0) * LANES + iota((lines, LANES), 1)
    order_hi, order_lo = bf((order >> 7).astype(F32)), bf((order & 127).astype(F32))
    order_hi, order_lo = order_hi.astype(F32), order_lo.astype(F32)
    mine_hi, mine_lo = (slot >> 7).astype(F32), (slot & 127).astype(F32)
    found = jnp.zeros((2 * lines, LANES), F32)
    line_cells, lane_cells = cells(lines, step * LANES), cells(LANES, step * LANES)
    zero, one = jnp.zeros((), BF16), jnp.ones((), BF16)
    for i in range(0, lines, step):
        here = line_cells == bf(wide(order_hi, i))
        stack = jnp.concatenate([jnp.where(here, bf(wide(mine_hi, i)), zero), jnp.where(here, bf(wide(mine_lo, i)), zero)], axis=0)
        place = jnp.where(lane_cells == bf(wide(order_lo, i)), one, zero)
        found = found + nt_dot(stack, place)
    slot_of = (found[:lines] * LANES + found[lines:]).astype(jnp.int32)

    r = r_ref[...]
    c = c_ref[...]
    rel = r - me * geo.rows + 1
    valid = (rel >= 0) & (rel <= geo.rows)
    bucket = c // COLS
    owner = slot_of // owned
    home = r // geo.rows
    edge = r - home * geo.rows == geo.rows - 1
    key = jnp.where(valid, bucket, -1)
    send_key = jnp.where(valid, owner, -1)
    first_key = jnp.where(owner == me, home, -1)
    second_key = jnp.where((owner == me) & edge, home + 1, -1)
    edge_key = jnp.where(valid & (rel == 0), 0, jnp.where(valid & (rel == geo.rows), 1, -1))

    def hot_of(i):
        line = slice(i, i + 1)
        recv = iota((slabs, LANES), 0)
        return (
            iota((buckets, LANES), 0) == key[line],
            recv == send_key[line],
            recv == first_key[line],
            recv == second_key[line],
            iota((16, LANES), 0) == edge_key[line],
        )

    for i in range(lines):
        a, b, c1, c2, d = hot_of(i)
        hot = jnp.concatenate([jnp.where(x, 1.0, 0.0) for x in (a, b, c1 | c2, d)], axis=0)
        hots[i * kinds : (i + 1) * kinds, :] = bf(hot)
    upper = iota((LANES, 2 * LANES), 0) < iota((LANES, 2 * LANES), 1)
    upper = bf(jnp.where(upper, 1.0, 0.0))
    before = jnp.dot(hots[...], upper, preferred_element_type=F32)
    carry = jnp.zeros((kinds, LANES), F32)
    for i in range(lines):
        part = before[i * kinds : (i + 1) * kinds]
        rank = part[:, :LANES] + carry
        a, b, c1, c2, d = hot_of(i)
        recv = rank[buckets + slabs : buckets + 2 * slabs]
        picks = (
            (a, rank[:buckets]),
            (b, rank[buckets : buckets + slabs]),
            (c1, recv),
            (c2, recv),
            (d, rank[buckets + 2 * slabs :]),
        )
        for k, (mask, value) in enumerate(picks):
            ranks[k, i : i + 1, :] = jnp.sum(jnp.where(mask, value, 0.0), axis=0, keepdims=True)
        carry = carry + part[:, LANES:]
    capacity = 4.0 * geo.quarter
    row = iota((kinds, LANES), 0)
    limit = jnp.where(row < buckets, float(LANES), jnp.where(row < buckets + 2 * slabs, capacity, float(geo.edge_lines * LANES)))
    over = jnp.sum(jnp.where(carry > limit, 1.0, 0.0), axis=0, keepdims=True)
    flag_ref[...] = jnp.broadcast_to(over, flag_ref.shape)

    spot, send, recv1, recv2, swap = (ranks[k] for k in range(5))
    rf, cf, w = rf_ref[...], cf_ref[...], w_ref[...]
    rf_top, w_top = bf(rf).astype(F32), bf(w).astype(F32)
    send_quarter = jnp.floor((send + 0.5) * (1.0 / geo.quarter))
    swap_line = jnp.floor((swap + 0.5) * (1.0 / LANES))
    values = (
        (c - bucket * COLS).astype(F32),
        bf(1.0 - cf).astype(F32),
        bf(cf).astype(F32),
        rf_top,
        rf - rf_top,
        w_top,
        w - w_top,
        (rel + 1 + 8 * owner).astype(F32),
        send - send_quarter * geo.quarter,
        jnp.minimum(send_quarter, 15.0) + 16.0 * jnp.minimum(jnp.where(edge_key >= 0, swap_line, 0.0), 15.0),
        swap - swap_line * LANES,
    )
    key_value = jnp.where(valid & (spot < LANES), bucket, -1).astype(F32)
    bucket_cells = cells(buckets, step * LANES)
    total = jnp.zeros((FAST * buckets, LANES), F32)
    for i in range(0, lines, step):
        here = bucket_cells == bf(wide(key_value, i))
        stack = jnp.concatenate([jnp.where(here, bf(wide(v, i)), zero) for v in values], axis=0)
        place = jnp.where(lane_cells == bf(jnp.minimum(wide(spot, i), 255.0)), one, zero)
        total = total + nt_dot(stack, place)
    for f in range(FAST):
        plan_ref[f] = total[f * buckets : (f + 1) * buckets, :]

    sent = slabs * geo.quarter

    def position(rank, source, use):
        quarter = jnp.floor((rank + 0.5) * (1.0 / geo.quarter))
        place = quarter * sent + source.astype(F32) * geo.quarter + (rank - quarter * geo.quarter)
        return jnp.where(use, place, 4.0 * sent + 8.0)

    here_slot = slot_of - me * owned
    owned_lines = owned // LANES
    slot_line = jnp.where(owner == me, here_slot >> 7, -1).astype(F32)
    slot_lane = (here_slot & 127).astype(F32)
    fields = []
    for place in (position(recv1, home, owner == me), position(recv2, home + 1, edge)):
        high = jnp.floor(place * (1.0 / 64.0))
        fields += [high, place - 64.0 * high]
    slot_cells = cells(owned_lines, step * LANES)
    pad = -(4 * owned_lines) % 16
    placed = jnp.zeros((4 * owned_lines + pad, LANES), F32)
    for i in range(0, lines, step):
        here = jnp.broadcast_to(wide(slot_line, i), (owned_lines, step * LANES)) == iota((owned_lines, step * LANES), 0).astype(F32)
        stack = [jnp.where(here, wide(v, i), 0.0) for v in fields]
        if pad:
            stack.append(jnp.zeros((pad, step * LANES), F32))
        place = jnp.where(lane_cells == bf(wide(slot_lane, i)), one, zero)
        placed = placed + nt_dot(bf(jnp.concatenate(stack, axis=0)), place)
    for f in range(2):
        at = 2 * f * owned_lines
        slot_ref[f] = placed[at : at + owned_lines] * 64.0 + placed[at + owned_lines : at + 2 * owned_lines]

    depth = geo.rows * geo.probes
    spill = None
    batch = loads // 2
    for g in reversed(range(rounds)):
        for j in range(loads):
            load(g, j).wait()
        group = list(reversed(range(g * batch, (g + 1) * batch)))
        parts = []
        for b in group:
            block = jnp.concatenate([tiles[2 * b].reshape(depth, LANES), tiles[2 * b + 1].reshape(depth, LANES)], axis=1)
            parts.append(jnp.dot(block, bucket_table(plan_ref, b), preferred_element_type=F32))
        for b, part in zip(group, parts):
            value = part[:, :LANES]
            if spill is not None:
                value = value + spill
            spill = part[:, LANES:]
            fold[b] = value
            terms = [fold[b, pl.ds(k, geo.probes, stride=geo.rows), :] * x for k, x in enumerate(row_weights(geo, plan_ref, b))]
            value_ref[b] = functools.reduce(jnp.add, terms)


def bucket_table(plan_ref, b):
    near, low, high = (plan_ref[f, pl.ds(b, 1), :] for f in range(3))
    grid = cells(COLS, LANES)
    zero = jnp.zeros((), BF16)
    main = jnp.where(grid == bf(near), bf(low), jnp.where(grid == bf(near + 1.0), bf(high), zero))
    if isinstance(b, int) and b == 0:
        return jnp.concatenate([main, jnp.zeros((COLS, LANES), BF16)], axis=1)
    before = b - 1 if isinstance(b, int) else jnp.maximum(b - 1, 0)
    last, spill = (plan_ref[f, pl.ds(before, 1), :] for f in (0, 2))
    spill = jnp.where(last == COLS - 1.0, spill, 0.0)
    over = bf(jnp.where(iota((16, LANES), 0) == 0, spill, 0.0))
    over = jnp.concatenate([over, jnp.zeros((COLS - 16, LANES), BF16)], axis=0)
    return jnp.concatenate([main, over], axis=1)


def place_code(plan_ref, b):
    code = plan_ref[7, pl.ds(b, 1), :]
    owner = jnp.floor(code * 0.125)
    return owner, code - 8.0 * owner


def row_weights(geo, plan_ref, b):
    rf = plan_ref[3, pl.ds(b, 1), :] + plan_ref[4, pl.ds(b, 1), :]
    _, rel = place_code(plan_ref, b)
    return [jnp.where(rel == k + 2.0, 1.0 - rf, jnp.where(rel == k + 1.0, rf, 0.0)) for k in range(geo.rows)]


def exchange_kernel(geo, r_ref, c_ref, rf_ref, cf_ref, w_ref, order_ref, field_ref, adjoint_ref, arrived_ref, slot_ref, total_ref, ok_ref, plan_ref, flag_ref, value_ref, tiles, hots, ranks, fold, edges, places, shares, inbox, packed, sources, raised, traces, sums, load_sem, swap_send, swap_recv, owner_send, owner_recv, trace_send, trace_recv, sum_send, sum_recv):
    slabs, groups, probes, rows, quarter, buckets = geo.slabs, geo.groups, geo.probes, geo.rows, geo.quarter, geo.buckets
    me, mine = lax.axis_index("slab"), lax.axis_index("probe")
    lines = geo.edge_lines
    zero = jnp.zeros((), BF16)
    batch = 8

    def at(slab, probe):
        return dict(device_id=(slab, probe), device_id_type=pl.DeviceIdType.MESH)

    barrier = pltpu.get_barrier_semaphore()
    for k in range(1, slabs):
        pl.semaphore_signal(barrier, inc=1, **at(lax.rem(me + k, slabs), mine))
    for k in range(1, groups):
        pl.semaphore_signal(barrier, inc=1, **at(me, lax.rem(mine + k, groups)))

    observe(geo, me, r_ref, c_ref, rf_ref, cf_ref, w_ref, order_ref, field_ref, plan_ref, slot_ref, flag_ref, value_ref, tiles, hots, ranks, fold, load_sem)

    def columns(j):
        return slice(j * LANES, (j + 1) * LANES)

    def edge_fields(b):
        _, rel = place_code(plan_ref, b)
        line = jnp.floor(plan_ref[9, pl.ds(b, 1), :] * (1.0 / 16.0))
        lane = plan_ref[10, pl.ds(b, 1), :]
        return rel, line, lane

    def weight_of(b):
        return plan_ref[5, pl.ds(b, 1), :] + plan_ref[6, pl.ds(b, 1), :]

    share_rows = shares.shape[0]

    @pl.when(me == 0)
    def _():
        inbox[0] = jnp.zeros_like(inbox[0])

    @pl.when(me == slabs - 1)
    def _():
        inbox[1] = jnp.zeros_like(inbox[1])

    found = None
    for g in range(buckets // batch):
        stacks, spots = [], []
        for j in range(batch):
            b = g * batch + j
            rel, line, lane = edge_fields(b)
            low, high = rel == 1.0, rel == rows + 1.0
            spot = match(2 * LANES, jnp.where(low, lane, jnp.where(high, lane + LANES, -1.0)))
            value = value_ref[b]
            share = jnp.where((iota((share_rows, LANES), 0).astype(F32) == line) & high, weight_of(b), 0.0)
            stacks.append(jnp.concatenate([bf(jnp.where(line == float(l), value, 0.0)) for l in range(lines)] + [bf(share)], axis=0))
            spots.append(spot)
            places[b] = spot
        part = nt_dot(jnp.concatenate(stacks, axis=1), jnp.concatenate(spots, axis=1))
        found = part if found is None else found + part
    for side in range(2):
        edges[side] = found[: lines * probes, columns(side)]
    shares[...] = found[lines * probes :, columns(1)]

    pl.semaphore_wait(barrier, slabs + groups - 2)
    down, up = lax.rem(me + slabs - 1, slabs), lax.rem(me + 1, slabs)
    swaps = [
        pltpu.make_async_remote_copy(
            src_ref=edges.at[side], dst_ref=inbox.at[1 - side], send_sem=swap_send.at[side], recv_sem=swap_recv.at[side], **at(peer, mine)
        )
        for side, peer in ((0, down), (1, up))
    ]
    ends = (me > 0, me < slabs - 1)
    for side, copy in enumerate(swaps):
        pl.when(ends[side])(copy.start)

    packed[...] = jnp.zeros_like(packed)

    def pack(g, squares):
        hots, quads = [], []
        for j in range(batch):
            b = g * batch + j
            owner, rel = place_code(plan_ref, b)
            code = plan_ref[9, pl.ds(b, 1), :]
            fourth = code - 16.0 * jnp.floor(code * (1.0 / 16.0))
            row = jnp.where(rel > 0.0, owner * quarter + plan_ref[8, pl.ds(b, 1), :], -1.0)
            hots.append(match(slabs * quarter, row))
            value = value_ref[b]
            squares = squares + value * value * weight_of(b)
            quads.append(jnp.concatenate([bf(jnp.where(fourth == float(k), value, 0.0)) for k in range(4)], axis=0))
        part = nt_dot(jnp.concatenate(hots, axis=1), jnp.concatenate(quads, axis=1))
        packed[...] += part.reshape(packed.shape)
        return squares

    squares = lax.fori_loop(0, buckets // batch, pack, jnp.zeros((probes, LANES), F32))

    def owner_copy(k, source, peer):
        return pltpu.make_async_remote_copy(
            src_ref=packed.at[peer], dst_ref=arrived_ref.at[source], send_sem=owner_send.at[k], recv_sem=owner_recv.at[k], **at(peer, mine)
        )

    for k in range(1, slabs):
        owner_copy(k, me, lax.rem(me + k, slabs)).start()
    arrived_ref[me] = packed[me]

    for side, copy in enumerate(swaps):
        pl.when(ends[side])(copy.wait_send)
        pl.when(ends[1 - side])(copy.wait_recv)
    for l in range(lines):
        part = slice(l * probes, (l + 1) * probes)
        squares = squares + edges[1, part] * inbox[1, part] * (2.0 * shares[l : l + 1])
    folded = squares[:8]
    for d in range(8, probes, 8):
        folded = folded + squares[d : d + 8]
    traces[mine] = jnp.where(flag_ref[:1] > 0.0, jnp.inf, jnp.sum(folded, axis=0, keepdims=True))

    def trace_copy(k, source, peer):
        return pltpu.make_async_remote_copy(
            src_ref=traces.at[mine], dst_ref=traces.at[source], send_sem=trace_send.at[k], recv_sem=trace_recv.at[k], **at(me, peer)
        )

    for k in range(1, groups):
        trace_copy(k, mine, lax.rem(mine + k, groups)).start()

    both = bf(jnp.concatenate([inbox[0], inbox[1]], axis=1))
    sources[0] = jnp.zeros_like(sources[0])

    @pl.loop(0, buckets // batch)
    def _(g):
        spots = jnp.concatenate([places[g * batch + j] for j in range(batch)], axis=1)
        extra = jnp.dot(both, spots, preferred_element_type=F32)
        for j in range(batch):
            b = g * batch + j
            _, line, _ = edge_fields(b)
            full = value_ref[b]
            for l in range(lines):
                full = full + jnp.where(line == float(l), extra[l * probes : (l + 1) * probes, columns(j)], 0.0)
            spread = full * weight_of(b)
            for k, weight in enumerate(row_weights(geo, plan_ref, b)):
                raised[j, pl.ds(k, probes, stride=rows), :] = spread * weight
            sources[b + 1] = bf(raised[j])

    def spread_back(g):
        parts = []
        for j in range(batch):
            b = g * batch + j
            source = jnp.concatenate([sources[b + 1], sources[b]], axis=1)
            parts.append(nt_dot(source, bucket_table(plan_ref, b)))
        for j in range(batch):
            for t in range(2):
                adjoint_ref[2 * (g * batch + j) + t] = bf(parts[j][:, columns(t)]).reshape(probes, rows, LANES)

    rounds = buckets // batch
    early = max(1, rounds * EARLY // 4)
    pl.loop(0, early)(spread_back)
    for k in range(1, groups):
        source = lax.rem(mine + groups - k, groups)
        trace_copy(k, source, source).wait()
    sums[me] = jnp.sum(traces[...], axis=0)

    def sum_copy(k, source, peer):
        return pltpu.make_async_remote_copy(
            src_ref=sums.at[me], dst_ref=sums.at[source], send_sem=sum_send.at[k], recv_sem=sum_recv.at[k], **at(peer, mine)
        )

    for k in range(1, slabs):
        sum_copy(k, me, lax.rem(me + k, slabs)).start()

    if early < rounds:
        pl.loop(early, rounds)(spread_back)
    for k in range(1, slabs):
        source = lax.rem(me + slabs - k, slabs)
        owner_copy(k, source, source).wait()
    for k in range(1, slabs):
        source = lax.rem(me + slabs - k, slabs)
        sum_copy(k, source, source).wait()
    total = jnp.sum(sums[...], axis=0)
    total_ref[...] = total
    ok_ref[0] = jnp.max(jnp.where(total < jnp.inf, 0.0, 1.0)).astype(jnp.int32)


def deliver_kernel(geo, scale, adjoint_ref, arrived_ref, slot_ref, total_ref, out_ref, observed_ref, mean_ref, observed, sem):
    slabs, probes, quarter, owned = geo.slabs, geo.probes, geo.quarter, geo.owned
    loads = 8

    def store(t):
        return pltpu.make_async_copy(adjoint_ref.at[t], out_ref.at[:, t], sem.at[0])

    for t in range(geo.tiles):
        store(t).start()
    sent = slabs * quarter
    arrived = jnp.transpose(arrived_ref[...].reshape(sent, 4 * probes))
    lines = owned // LANES
    spots = [jnp.concatenate([slot_ref[f, l : l + 1, :] for l in range(lines)], axis=1) for f in range(2)]
    total = jnp.zeros((probes, owned), F32)
    for k in range(4):
        hot = match(sent, spots[0] - float(k * sent)) + match(sent, spots[1] - float(k * sent))
        total = total + jnp.dot(bf(arrived[k * probes : (k + 1) * probes]), hot, preferred_element_type=F32)
    observed[...] = total
    pltpu.make_async_copy(observed, observed_ref, sem.at[1]).start()
    mean_ref[...] = jnp.broadcast_to(jnp.sum(total_ref[...], axis=1, keepdims=True) * scale, mean_ref.shape)
    pltpu.make_async_copy(observed, observed_ref, sem.at[1]).wait()
    for t in range(geo.tiles):
        store(t).wait()


def geometry(slabs, groups, probe_fields, sensors):
    probes, rows, width = probe_fields.shape
    most = min(sensors, 4 * sensors // slabs)
    quarter = -(-(most // slabs + 32) // 32) * 8
    edge_lines = -(-5 * most // (4 * rows * LANES))
    buckets = width // COLS
    return Geo(rows, probes, slabs, groups, buckets, width // LANES, sensors // LANES, sensors // slabs, quarter, edge_lines, buckets + 2 * slabs + 16)


def body(slab_count, probe_groups, probe_fields, *vectors):
    sensors = vectors[0].shape[0]
    geo = geometry(slab_count, probe_groups, probe_fields, sensors)
    probes, rows, width = probe_fields.shape
    depth = probes * rows
    lines, buckets, tiles = geo.lines, geo.buckets, geo.tiles
    boxed = [x.reshape(lines, LANES) for x in vectors]
    field = probe_fields.reshape(probes, rows, tiles, LANES).transpose(0, 2, 1, 3)
    vmem = pl.BlockSpec(memory_space=VMEM)
    smem = pl.BlockSpec(memory_space=SMEM)
    hbm = pl.BlockSpec(memory_space=pltpu.HBM)
    dma = pltpu.SemaphoreType.DMA
    shape = jax.ShapeDtypeStruct
    edge_rows = geo.edge_lines * probes
    adjoint, arrived, slots, total, flag = pl.pallas_call(
        functools.partial(exchange_kernel, geo),
        out_shape=(
            shape((tiles, probes, rows, LANES), BF16),
            shape((slab_count, geo.quarter, 4 * probes), F32),
            shape((2, geo.owned // LANES, LANES), F32),
            shape((1, LANES), F32),
            shape((1,), jnp.int32),
        ),
        in_specs=[vmem] * 6 + [hbm],
        out_specs=(vmem, vmem, vmem, vmem, smem),
        scratch_shapes=[
            VMEM((FAST, buckets, LANES), F32),
            VMEM((8, LANES), F32),
            VMEM((buckets, probes, LANES), F32),
            VMEM((tiles, probes, rows, LANES), BF16),
            VMEM((lines * geo.kinds, LANES), BF16),
            VMEM((5, lines, LANES), F32),
            VMEM((buckets, depth, LANES), F32),
            VMEM((2, edge_rows, LANES), F32),
            VMEM((buckets, 2 * LANES, LANES), BF16),
            VMEM((-(-geo.edge_lines // 16) * 16, LANES), F32),
            VMEM((2, edge_rows, LANES), F32),
            VMEM((slab_count, geo.quarter, 4 * probes), F32),
            VMEM((buckets + 1, depth, LANES), BF16),
            VMEM((8, depth, LANES), F32),
            VMEM((probe_groups, 1, LANES), F32),
            VMEM((slab_count, 1, LANES), F32),
            dma((tiles // 8,)),
            dma((2,)),
            dma((2,)),
            dma((slab_count,)),
            dma((slab_count,)),
            dma((probe_groups,)),
            dma((probe_groups,)),
            dma((slab_count,)),
            dma((slab_count,)),
        ],
        compiler_params=pltpu.CompilerParams(collective_id=3, has_side_effects=True, vmem_limit_bytes=ROOM),
        name="exchange",
    )(*boxed, field)
    out, observed, mean = pl.pallas_call(
        functools.partial(deliver_kernel, geo, 1.0 / (probes * probe_groups * sensors)),
        out_shape=(
            shape((probes, tiles, rows, LANES), BF16),
            shape((probes, geo.owned), F32),
            shape((1, LANES), F32),
        ),
        in_specs=[vmem] * 4,
        out_specs=(hbm, hbm, vmem),
        scratch_shapes=[VMEM((probes, geo.owned), F32), dma((2,))],
        compiler_params=SMALL,
        name="deliver",
    )(adjoint, arrived, slots, total)
    out = out.transpose(0, 2, 1, 3).reshape(probes, rows, width)

    def again(state):
        out, observed, mean = general(slab_count, probe_groups, probe_fields, *vectors)
        return out, jnp.where(state[3] > 0, observed, state[1]), mean, state[3] * 0

    state = lax.while_loop(lambda state: state[3] != 0, again, (out, observed, mean[0, 0], flag[0]))
    return state[:3]


def solution(mesh):
    placed = (P("probe", "slab", None), P(), P(), P(), P(), P(), P())
    return jax.shard_map(
        functools.partial(body, mesh.shape["slab"], mesh.shape["probe"]),
        mesh=mesh,
        in_specs=placed,
        out_specs=(P("probe", "slab", None), P("probe", "slab"), P()),
        check_vma=False,
    )
```

```python
import functools
import typing

import jax
import jax.numpy as jnp
from jax import lax
from jax.experimental import pallas as pl
from jax.experimental.pallas import tpu as pltpu
from jax.sharding import PartitionSpec as P

LANES = 128
BLOCK = 1024
HALF = 256
FIELDS = 11
F32 = jnp.float32
BF16 = jnp.bfloat16
NT = (((1,), (1,)), ((), ()))
VMEM = pltpu.VMEM
SMEM = pltpu.SMEM
LIMIT = pltpu.CompilerParams(vmem_limit_bytes=60 * 1024 * 1024)


def iota(shape, dim):
    return lax.broadcasted_iota(jnp.int32, shape, dim)


def nt_dot(a, b):
    return lax.dot_general(a, b, NT, preferred_element_type=F32)


def plan_kernel(rows, cap_chunks, blocks, slabs, pair_lines, me_ref, r_ref, c_ref, rf_ref, cf_ref, w_ref, order_ref, plan_ref, marks_ref, places_ref, peak_ref):
    lines = r_ref.shape[0]
    sensors = lines * LANES
    step = min(4, lines)
    me = me_ref[0]
    first = me * rows
    owned = lines * LANES // slabs
    keys_group = 2 * blocks
    keys = 3 * keys_group
    chunks = 3 * cap_chunks

    def wide(x, i):
        return jnp.concatenate([x[i + j : i + j + 1, :] for j in range(step)], axis=1)

    order = order_ref[...]
    slot = iota((lines, LANES), 0) * LANES + iota((lines, LANES), 1)
    found = jnp.zeros((2 * lines, LANES), F32)
    for i in range(0, lines, step):
        target = wide(order, i)
        mine = wide(slot, i)
        here = iota((lines, step * LANES), 0) == (target >> 7)
        stack = jnp.concatenate(
            [jnp.where(here, (mine >> 7).astype(F32), 0.0), jnp.where(here, (mine & 127).astype(F32), 0.0)], axis=0
        ).astype(BF16)
        place = jnp.where(iota((LANES, step * LANES), 0) == (target & 127), 1.0, 0.0).astype(BF16)
        found = found + nt_dot(stack, place)
    slot_hi = found[:lines, :]
    slot_lo = found[lines:, :]

    r = r_ref[...]
    c = c_ref[...]
    rel = r - first + 1
    valid = (rel >= 0) & (rel <= rows)
    group = jnp.where(rel == 0, 0, jnp.where(rel == rows, 2, 1))
    block = c // BLOCK
    inner = c - block * BLOCK
    half = c // HALF
    slot_of = (slot_hi * LANES + slot_lo).astype(jnp.int32)
    owner = slot_of // owned
    home = r // rows
    send_key = jnp.where(home == me, owner, -1)
    recv_key = jnp.where(owner == me, home, -1)
    edge = jnp.where(r - home * rows == rows - 1, home, -1)
    edges = jnp.zeros((slabs, LANES), F32)
    for i in range(lines):
        edges = edges + jnp.where(iota((slabs, LANES), 0) == edge[i : i + 1, :], 1.0, 0.0)
    peak_ref[0] = jnp.max(jnp.sum(edges, axis=1, keepdims=True)).astype(jnp.int32)
    key = group * keys_group + 2 * block + jnp.where(inner == BLOCK - 1, 1, 0)
    key = jnp.where(valid, key, -1)

    count = jnp.zeros((keys, 1), F32)
    for i in range(lines):
        count = count + jnp.sum(jnp.where(iota((keys, LANES), 0) == key[i : i + 1, :], 1.0, 0.0), axis=1, keepdims=True)
    big = jnp.floor(count * (1.0 / 64.0))
    small = count - 64.0 * big
    ka, kb = iota((keys, keys), 0), iota((keys, keys), 1)
    below = jnp.where((kb < ka) & (kb // keys_group == ka // keys_group), 1.0, 0.0).astype(BF16)
    start = 64.0 * jnp.dot(below, jnp.broadcast_to(big, (keys, LANES)).astype(BF16), preferred_element_type=F32)
    start = start + jnp.dot(below, jnp.broadcast_to(small, (keys, LANES)).astype(BF16), preferred_element_type=F32)
    start = start + ((iota((keys, LANES), 0) // keys_group) * (cap_chunks * LANES)).astype(F32)
    wide_keys = marks_ref.shape[1]
    diagonal = iota((keys, wide_keys), 0) == iota((keys, wide_keys), 1)
    marks_ref[...] = jnp.concatenate(
        [jnp.sum(jnp.where(diagonal, x, 0.0), axis=0, keepdims=True) for x in (start[:, :1], start[:, :1] + count)], axis=0
    ).astype(jnp.int32)

    upper = jnp.where(iota((LANES, LANES), 0) < iota((LANES, LANES), 1), 1.0, 0.0).astype(BF16)
    carry = jnp.concatenate([start[:, :1], jnp.zeros((2 * slabs, 1), F32)], axis=0)
    spots, sends, recvs = [], [], []
    for i in range(lines):
        hot = jnp.concatenate(
            [
                jnp.where(iota((keys, LANES), 0) == key[i : i + 1, :], 1.0, 0.0),
                jnp.where(iota((slabs, LANES), 0) == send_key[i : i + 1, :], 1.0, 0.0),
                jnp.where(iota((slabs, LANES), 0) == recv_key[i : i + 1, :], 1.0, 0.0),
            ],
            axis=0,
        )
        before = jnp.dot(hot.astype(BF16), upper, preferred_element_type=F32)
        ranks = hot * (before + carry)
        spots.append(jnp.sum(ranks[:keys], axis=0, keepdims=True))
        sends.append(jnp.sum(ranks[keys : keys + slabs], axis=0, keepdims=True))
        recvs.append(jnp.sum(ranks[keys + slabs :], axis=0, keepdims=True))
        carry = carry + jnp.sum(hot, axis=1, keepdims=True)
    spot = jnp.concatenate(spots, axis=0).astype(jnp.int32)
    spot = jnp.where(valid, spot, -1)
    send = jnp.concatenate(sends, axis=0).astype(jnp.int32)
    recv = jnp.concatenate(recvs, axis=0).astype(jnp.int32)
    send_line = jnp.where(send_key >= 0, owner * pair_lines + (send >> 7), 200)
    recv_line = jnp.where(recv_key >= 0, home * pair_lines + (recv >> 7), -1)

    rf = rf_ref[...]
    cf = cf_ref[...]
    w = w_ref[...]
    rf_top = rf.astype(BF16).astype(F32)
    w_top = w.astype(BF16).astype(F32)
    values = [
        half.astype(F32),
        (c - half * HALF).astype(F32),
        (1.0 - cf).astype(BF16).astype(F32),
        cf.astype(BF16).astype(F32),
        rf_top,
        rf - rf_top,
        w_top,
        w - w_top,
        rel.astype(F32),
        send_line.astype(F32),
        (send & 127).astype(F32),
    ]
    total = jnp.zeros((FIELDS * chunks, LANES), F32)
    for i in range(0, lines, step):
        target = wide(spot, i)
        here = iota((chunks, step * LANES), 0) == (target >> 7)
        stack = jnp.concatenate([jnp.where(here, wide(v, i), 0.0) for v in values], axis=0).astype(BF16)
        place = jnp.where(iota((LANES, step * LANES), 0) == (target & 127), 1.0, 0.0).astype(BF16)
        total = total + nt_dot(stack, place)
    for f in range(FIELDS):
        plan_ref[f] = total[f * chunks : (f + 1) * chunks, :]

    slot_here = slot_of - me * owned
    received = slabs * pair_lines
    found = jnp.zeros((2 * received, LANES), F32)
    for i in range(0, lines, step):
        here = iota((received, step * LANES), 0) == wide(recv_line, i)
        target = wide(slot_here, i)
        stack = jnp.concatenate(
            [jnp.where(here, (target >> 7).astype(F32), 0.0), jnp.where(here, (target & 127).astype(F32), 0.0)], axis=0
        ).astype(BF16)
        place = jnp.where(iota((LANES, step * LANES), 0) == (wide(recv, i) & 127), 1.0, 0.0).astype(BF16)
        found = found + nt_dot(stack, place)
    places_ref[...] = (found[:received] * LANES + found[received:]).astype(jnp.int32)


def column_table(plan_ref, chunk, number):
    line = pl.ds(chunk, 1)
    column = plan_ref[0, line, :] * HALF + plan_ref[1, line, :] - (number * BLOCK).astype(F32)
    low = plan_ref[2, line, :].astype(BF16)
    high = plan_ref[3, line, :].astype(BF16)
    cells = iota((HALF, LANES), 0).astype(F32).astype(BF16)
    pieces = []
    for begin in range(0, BLOCK, HALF):
        near = jnp.clip(column - begin, -2.0, HALF).astype(BF16)
        after = jnp.clip(column - (begin - 1), -2.0, HALF).astype(BF16)
        pieces.append(jnp.where(cells == near, low, jnp.where(cells == after, high, jnp.zeros((), BF16))))
    return jnp.concatenate(pieces, axis=0)


def row_pattern(plan_ref, chunk, rows, depth):
    line = pl.ds(chunk, 1)
    rf = plan_ref[4, line, :] + plan_ref[5, line, :]
    rel = plan_ref[8, line, :].astype(jnp.int32)
    row = iota((depth, LANES), 0) % rows + 1
    return jnp.where(row == rel, 1.0 - rf, jnp.where(row == rel + 1, rf, 0.0))


def group_chunks(marks_ref, group, keys_group, base):
    count = (marks_ref[1, (group + 1) * keys_group - 1] - base + LANES - 1) // LANES
    return jnp.maximum(count, 1)


def chunk_range(marks_ref, group, number, keys_group, cap_chunks):
    at = group * keys_group + 2 * number
    begin = marks_ref[0, jnp.maximum(at - 1, group * keys_group)]
    end = marks_ref[1, at + 1]
    base = group * cap_chunks
    last = base + group_chunks(marks_ref, group, keys_group, base * LANES) - 1
    return jnp.minimum(begin // LANES, last), jnp.where(end > begin, (end + LANES - 1) // LANES, 0)


def forward_kernel(cap_chunks, blocks, field_ref, plan_ref, marks_ref, value_ref, sums, flat):
    probes, rows, _ = field_ref.shape
    depth = probes * rows
    keys_group = 2 * blocks
    number = pl.program_id(0)
    counts = [group_chunks(marks_ref, g, keys_group, g * cap_chunks * LANES) for g in range(3)]

    @pl.when(number == 0)
    def _():
        for g in range(3):

            @pl.loop(0, counts[g])
            def _(k):
                sums[g * cap_chunks + k] = jnp.zeros((depth, LANES), F32)

    block = field_ref[...].reshape(depth, BLOCK)
    flat[...] = block
    ranges = [chunk_range(marks_ref, g, number, keys_group, cap_chunks) for g in range(3)]
    table = jnp.concatenate([column_table(plan_ref, begin, number) for begin, _ in ranges], axis=1)
    part = jnp.dot(block, table, preferred_element_type=F32)
    for g in range(3):
        sums[ranges[g][0]] += part[:, g * LANES : (g + 1) * LANES]
    for g in range(3):

        @pl.loop(ranges[g][0] + 1, ranges[g][1])
        def _(chunk):
            sums[chunk] += jnp.dot(flat[...], column_table(plan_ref, chunk, number), preferred_element_type=F32)

    @pl.when(number == blocks - 1)
    def _():
        fold = jnp.where(iota((probes, depth), 1) // rows == iota((probes, depth), 0), 1.0, 0.0).astype(BF16)
        for g in range(3):

            @pl.loop(0, counts[g])
            def _(k):
                chunk = g * cap_chunks + k
                scaled = (sums[chunk] * row_pattern(plan_ref, chunk, rows, depth)).astype(BF16)
                value_ref[chunk] = jnp.dot(fold, scaled, preferred_element_type=F32)


def swap_kernel(slabs, top, value_ref, above_ref, below_ref, send_sem, recv_sem):
    probe, me = lax.axis_index("probe"), lax.axis_index("slab")
    width = above_ref.shape[0]
    down, up = lax.rem(me + slabs - 1, slabs), lax.rem(me + 1, slabs)
    barrier = pltpu.get_barrier_semaphore()
    for peer in (down, up):
        pl.semaphore_signal(barrier, inc=1, device_id=(peer, probe), device_id_type=pl.DeviceIdType.MESH)
    pl.semaphore_wait(barrier, 2)
    copies = []
    for k, (peer, begin, target) in enumerate(((down, 0, above_ref), (up, top, below_ref))):
        copies.append(
            pltpu.make_async_remote_copy(
                src_ref=value_ref.at[begin : begin + width],
                dst_ref=target,
                send_sem=send_sem.at[k],
                recv_sem=recv_sem.at[k],
                device_id=(peer, probe),
                device_id_type=pl.DeviceIdType.MESH,
            )
        )
    for copy in copies:
        copy.start()
    for copy in copies:
        copy.wait()


def swap(slabs, cap_chunks, width, number, value):
    part = (width, *value.shape[1:])
    any_space = pl.BlockSpec(memory_space=pl.ANY)
    above, below = pl.pallas_call(
        functools.partial(swap_kernel, slabs, 2 * cap_chunks),
        out_shape=(jax.ShapeDtypeStruct(part, F32), jax.ShapeDtypeStruct(part, F32)),
        in_specs=[any_space],
        out_specs=(any_space, any_space),
        scratch_shapes=[pltpu.SemaphoreType.DMA((2,)), pltpu.SemaphoreType.DMA((2,))],
        compiler_params=pltpu.CompilerParams(collective_id=number, has_side_effects=True),
        name="swap",
    )(value)
    return above, below


def merge_kernel(cap_chunks, blocks, value_ref, above_ref, below_ref, plan_ref, marks_ref, spread_ref, packed_ref, squares, parts):
    slabs = packed_ref.shape[0]
    outgoing, probes, _ = parts.shape
    lines = outgoing // slabs
    keys_group = 2 * blocks
    squares[...] = jnp.zeros_like(squares)
    parts[...] = jnp.zeros_like(parts)
    for g in range(3):
        count = group_chunks(marks_ref, g, keys_group, g * cap_chunks * LANES)

        @pl.loop(0, count)
        def _(k):
            chunk = g * cap_chunks + k
            value = value_ref[chunk]
            if g == 0:
                value = value + below_ref[k]
            if g == 2:
                value = value + above_ref[k]
            line = pl.ds(chunk, 1)
            spread = value * (plan_ref[6, line, :] + plan_ref[7, line, :])
            spread_ref[chunk] = spread.astype(BF16)
            if g > 0:
                squares[...] += spread * value
                high = plan_ref[9, line, :].astype(jnp.int32)
                low = plan_ref[10, line, :].astype(jnp.int32)
                place = jnp.where(iota((LANES, LANES), 0) == low, 1.0, 0.0).astype(BF16)
                stack = jnp.concatenate([jnp.where(high == d, value, 0.0) for d in range(outgoing)], axis=0).astype(BF16)
                parts[...] += nt_dot(stack, place).reshape(outgoing, probes, LANES)

    folded = squares[:8, :]
    for d in range(8, probes, 8):
        folded = folded + squares[d : d + 8, :]
    for d in range(slabs):
        for e in range(lines):
            packed_ref[d, e * probes : (e + 1) * probes, :] = parts[d * lines + e]
        packed_ref[d, lines * probes :, :] = folded


def unpack_kernel(groups, scale, packed_ref, places_ref, observed_ref, mean_ref, traces, send_sem, recv_sem):
    slab, me = lax.axis_index("slab"), lax.axis_index("probe")
    slabs = packed_ref.shape[0]
    probes, owned = observed_ref.shape
    lines = places_ref.shape[0] // slabs
    barrier = pltpu.get_barrier_semaphore()
    for k in range(1, groups):
        peer = lax.rem(me + k, groups)
        pl.semaphore_signal(barrier, inc=1, device_id=(slab, peer), device_id_type=pl.DeviceIdType.MESH)
    own = packed_ref[0, lines * probes :, :]
    for d in range(1, slabs):
        own = own + packed_ref[d, lines * probes :, :]
    traces[me] = own
    pl.semaphore_wait(barrier, groups - 1)

    def tile(k, source, peer):
        return pltpu.make_async_remote_copy(
            src_ref=traces.at[me],
            dst_ref=traces.at[source],
            send_sem=send_sem.at[k],
            recv_sem=recv_sem.at[k],
            device_id=(slab, peer),
            device_id_type=pl.DeviceIdType.MESH,
        )

    for k in range(1, groups):
        tile(k, me, lax.rem(me + k, groups)).start()
    total = jnp.zeros((probes, owned), F32)
    for d in range(slabs):
        for e in range(lines):
            at = d * lines + e
            place = jnp.where(iota((owned, LANES), 0) == places_ref[at : at + 1, :], 1.0, 0.0).astype(BF16)
            total = total + nt_dot(packed_ref[d, e * probes : (e + 1) * probes, :].astype(BF16), place)
    observed_ref[...] = total
    for k in range(1, groups):
        source = lax.rem(me + groups - k, groups)
        tile(k, source, source).wait()
    summed = jnp.sum(jnp.sum(traces[...], axis=0), axis=0, keepdims=True)
    mean_ref[...] = jnp.broadcast_to(jnp.sum(summed, axis=1, keepdims=True) * scale, mean_ref.shape)


def adjoint_kernel(cap_chunks, blocks, spread_ref, plan_ref, marks_ref, out_ref, sources, total):
    probes, rows, _ = out_ref.shape
    depth = probes * rows
    keys_group = 2 * blocks
    number = pl.program_id(0)

    @pl.when(number == 0)
    def _():
        raise_rows = jnp.where(iota((depth, probes), 0) // rows == iota((depth, probes), 1), 1.0, 0.0).astype(BF16)
        for g in range(3):
            count = group_chunks(marks_ref, g, keys_group, g * cap_chunks * LANES)

            @pl.loop(0, count)
            def _(k):
                chunk = g * cap_chunks + k
                raised = jnp.dot(raise_rows, spread_ref[chunk], preferred_element_type=F32)
                sources[chunk] = (raised * row_pattern(plan_ref, chunk, rows, depth)).astype(BF16)

    ranges = [chunk_range(marks_ref, g, number, keys_group, cap_chunks) for g in range(3)]
    table = jnp.concatenate([column_table(plan_ref, begin, number) for begin, _ in ranges], axis=1)
    source = jnp.concatenate([sources[begin] for begin, _ in ranges], axis=1)
    total[...] = nt_dot(source, table)
    for g in range(3):

        @pl.loop(ranges[g][0] + 1, ranges[g][1])
        def _(chunk):
            total[...] += nt_dot(sources[chunk], column_table(plan_ref, chunk, number))

    out_ref[...] = total[...].astype(BF16).reshape(probes, rows, BLOCK)


def general(slab_count, probe_groups, probe_fields, sensor_rows, sensor_cols, row_frac, col_frac, sensor_weights, owner_order):
    probes, rows, width = probe_fields.shape
    sensors = sensor_rows.shape[0]
    depth = probes * rows
    lines = sensors // LANES
    blocks = width // BLOCK
    keys = 6 * blocks
    most = min(sensors, 4 * sensors // slab_count)
    cap_chunks = -(-most // (8 * LANES)) * 8
    chunks = 3 * cap_chunks
    pair_lines = -(-most // (slab_count * LANES))
    outgoing = slab_count * pair_lines
    me = jnp.reshape(lax.axis_index("slab"), (1,)).astype(jnp.int32)
    boxed = [x.reshape(lines, LANES) for x in (sensor_rows, sensor_cols, row_frac, col_frac, sensor_weights, owner_order)]
    vmem = pl.BlockSpec(memory_space=VMEM)
    smem = pl.BlockSpec(memory_space=SMEM)
    plan, marks, places, peak = pl.pallas_call(
        functools.partial(plan_kernel, rows, cap_chunks, blocks, slab_count, pair_lines),
        out_shape=(
            jax.ShapeDtypeStruct((FIELDS, chunks, LANES), F32),
            jax.ShapeDtypeStruct((2, -(-keys // LANES) * LANES), jnp.int32),
            jax.ShapeDtypeStruct((outgoing, LANES), jnp.int32),
            jax.ShapeDtypeStruct((1,), jnp.int32),
        ),
        in_specs=[smem] + [vmem] * 6,
        out_specs=(vmem, vmem, vmem, smem),
        compiler_params=LIMIT,
        name="plan",
    )(me, *boxed)
    value = pl.pallas_call(
        functools.partial(forward_kernel, cap_chunks, blocks),
        out_shape=jax.ShapeDtypeStruct((chunks, probes, LANES), F32),
        grid=(blocks,),
        in_specs=[pl.BlockSpec((probes, rows, BLOCK), lambda n: (0, 0, n)), vmem, smem],
        out_specs=vmem,
        scratch_shapes=[VMEM((chunks, depth, LANES), F32), VMEM((depth, BLOCK), BF16)],
        compiler_params=LIMIT,
        name="forward",
    )(probe_fields, plan, marks)
    few = min(cap_chunks, -(-5 * most // (4 * rows * LANES)))

    def merged(above, below):
        return pl.pallas_call(
            functools.partial(merge_kernel, cap_chunks, blocks),
            out_shape=(
                jax.ShapeDtypeStruct((chunks, probes, LANES), BF16),
                jax.ShapeDtypeStruct((slab_count, pair_lines * probes + 8, LANES), F32),
            ),
            in_specs=[vmem, vmem, vmem, vmem, smem],
            out_specs=(vmem, vmem),
            scratch_shapes=[VMEM((probes, LANES), F32), VMEM((outgoing, probes, LANES), F32)],
            compiler_params=LIMIT,
            name="merge",
        )(value, above, below, plan, marks)

    spread, packed = lax.cond(
        peak[0] <= few * LANES,
        lambda: merged(*swap(slab_count, cap_chunks, few, 0, value)),
        lambda: merged(*swap(slab_count, cap_chunks, cap_chunks, 1, value)),
    )
    arrived = lax.all_to_all(packed, "slab", 0, 0, tiled=True)
    adjoint = pl.pallas_call(
        functools.partial(adjoint_kernel, cap_chunks, blocks),
        out_shape=jax.ShapeDtypeStruct((probes, rows, width), BF16),
        grid=(blocks,),
        in_specs=[vmem, vmem, smem],
        out_specs=pl.BlockSpec((probes, rows, BLOCK), lambda n: (0, 0, n)),
        scratch_shapes=[
            VMEM((chunks, depth, LANES), BF16),
            VMEM((depth, BLOCK), F32),
        ],
        compiler_params=LIMIT,
        cost_estimate=pl.CostEstimate(flops=4 * 10**9, bytes_accessed=8 * 10**6, transcendentals=0),
        name="adjoint",
    )(spread, plan, marks)
    observed, mean = pl.pallas_call(
        functools.partial(unpack_kernel, probe_groups, 1.0 / (probes * probe_groups * sensors)),
        out_shape=(
            jax.ShapeDtypeStruct((probes, sensors // slab_count), F32),
            jax.ShapeDtypeStruct((1, LANES), F32),
        ),
        in_specs=[vmem, vmem],
        out_specs=(vmem, vmem),
        scratch_shapes=[
            VMEM((probe_groups, 8, LANES), F32),
            pltpu.SemaphoreType.DMA((probe_groups,)),
            pltpu.SemaphoreType.DMA((probe_groups,)),
        ],
        compiler_params=pltpu.CompilerParams(collective_id=2, has_side_effects=True, vmem_limit_bytes=40 * 1024 * 1024),
        name="unpack",
    )(arrived, places)
    return adjoint, observed, mean[0, 0]


COLS = 256
FAST = 11
EARLY = 3
ROOM = 36 * 1024 * 1024
SMALL = pltpu.CompilerParams(vmem_limit_bytes=ROOM)


class Geo(typing.NamedTuple):
    rows: int
    probes: int
    slabs: int
    groups: int
    buckets: int
    tiles: int
    lines: int
    owned: int
    quarter: int
    edge_lines: int
    kinds: int


def bf(x):
    return x.astype(BF16)


def cells(rows, width):
    return bf(iota((rows, width), 0).astype(F32))


def match(rows, target):
    grid = cells(min(rows, COLS), target.shape[1])
    pieces = []
    for begin in range(0, rows, COLS):
        size = min(COLS, rows - begin)
        near = bf(jnp.clip(target - begin, -1.0, float(COLS)))
        pieces.append(jnp.where(grid[:size] == near, jnp.ones((), BF16), jnp.zeros((), BF16)))
    return pieces[0] if len(pieces) == 1 else jnp.concatenate(pieces, axis=0)


def observe(geo, me, r_ref, c_ref, rf_ref, cf_ref, w_ref, order_ref, field_ref, plan_ref, slot_ref, flag_ref, value_ref, tiles, hots, ranks, fold, sem):
    lines, slabs, buckets, owned = geo.lines, geo.slabs, geo.buckets, geo.owned
    loads = 8
    rounds = geo.tiles // loads

    def load(g, j):
        t = g * loads + j
        return pltpu.make_async_copy(field_ref.at[:, t], tiles.at[t], sem.at[g])

    for g in reversed(range(rounds)):
        for j in range(loads):
            load(g, j).start()

    step = min(4, lines)
    kinds = geo.kinds

    def wide(x, i):
        return jnp.concatenate([x[i + j : i + j + 1, :] for j in range(step)], axis=1)

    order = order_ref[...]
    slot = iota((lines, LANES), 0) * LANES + iota((lines, LANES), 1)
    order_hi, order_lo = bf((order >> 7).astype(F32)), bf((order & 127).astype(F32))
    order_hi, order_lo = order_hi.astype(F32), order_lo.astype(F32)
    mine_hi, mine_lo = (slot >> 7).astype(F32), (slot & 127).astype(F32)
    found = jnp.zeros((2 * lines, LANES), F32)
    line_cells, lane_cells = cells(lines, step * LANES), cells(LANES, step * LANES)
    zero, one = jnp.zeros((), BF16), jnp.ones((), BF16)
    for i in range(0, lines, step):
        here = line_cells == bf(wide(order_hi, i))
        stack = jnp.concatenate([jnp.where(here, bf(wide(mine_hi, i)), zero), jnp.where(here, bf(wide(mine_lo, i)), zero)], axis=0)
        place = jnp.where(lane_cells == bf(wide(order_lo, i)), one, zero)
        found = found + nt_dot(stack, place)
    slot_of = (found[:lines] * LANES + found[lines:]).astype(jnp.int32)

    r = r_ref[...]
    c = c_ref[...]
    rel = r - me * geo.rows + 1
    valid = (rel >= 0) & (rel <= geo.rows)
    bucket = c // COLS
    owner = slot_of // owned
    home = r // geo.rows
    edge = r - home * geo.rows == geo.rows - 1
    key = jnp.where(valid, bucket, -1)
    send_key = jnp.where(valid, owner, -1)
    first_key = jnp.where(owner == me, home, -1)
    second_key = jnp.where((owner == me) & edge, home + 1, -1)
    edge_key = jnp.where(valid & (rel == 0), 0, jnp.where(valid & (rel == geo.rows), 1, -1))

    def hot_of(i):
        line = slice(i, i + 1)
        recv = iota((slabs, LANES), 0)
        return (
            iota((buckets, LANES), 0) == key[line],
            recv == send_key[line],
            recv == first_key[line],
            recv == second_key[line],
            iota((16, LANES), 0) == edge_key[line],
        )

    for i in range(lines):
        a, b, c1, c2, d = hot_of(i)
        hot = jnp.concatenate([jnp.where(x, 1.0, 0.0) for x in (a, b, c1 | c2, d)], axis=0)
        hots[i * kinds : (i + 1) * kinds, :] = bf(hot)
    upper = iota((LANES, 2 * LANES), 0) < iota((LANES, 2 * LANES), 1)
    upper = bf(jnp.where(upper, 1.0, 0.0))
    before = jnp.dot(hots[...], upper, preferred_element_type=F32)
    carry = jnp.zeros((kinds, LANES), F32)
    for i in range(lines):
        part = before[i * kinds : (i + 1) * kinds]
        rank = part[:, :LANES] + carry
        a, b, c1, c2, d = hot_of(i)
        recv = rank[buckets + slabs : buckets + 2 * slabs]
        picks = (
            (a, rank[:buckets]),
            (b, rank[buckets : buckets + slabs]),
            (c1, recv),
            (c2, recv),
            (d, rank[buckets + 2 * slabs :]),
        )
        for k, (mask, value) in enumerate(picks):
            ranks[k, i : i + 1, :] = jnp.sum(jnp.where(mask, value, 0.0), axis=0, keepdims=True)
        carry = carry + part[:, LANES:]
    capacity = 4.0 * geo.quarter
    row = iota((kinds, LANES), 0)
    limit = jnp.where(row < buckets, float(LANES), jnp.where(row < buckets + 2 * slabs, capacity, float(geo.edge_lines * LANES)))
    over = jnp.sum(jnp.where(carry > limit, 1.0, 0.0), axis=0, keepdims=True)
    flag_ref[...] = jnp.broadcast_to(over, flag_ref.shape)

    spot, send, recv1, recv2, swap = (ranks[k] for k in range(5))
    rf, cf, w = rf_ref[...], cf_ref[...], w_ref[...]
    rf_top, w_top = bf(rf).astype(F32), bf(w).astype(F32)
    send_quarter = jnp.floor((send + 0.5) * (1.0 / geo.quarter))
    swap_line = jnp.floor((swap + 0.5) * (1.0 / LANES))
    values = (
        (c - bucket * COLS).astype(F32),
        bf(1.0 - cf).astype(F32),
        bf(cf).astype(F32),
        rf_top,
        rf - rf_top,
        w_top,
        w - w_top,
        (rel + 1 + 8 * owner).astype(F32),
        send - send_quarter * geo.quarter,
        jnp.minimum(send_quarter, 15.0) + 16.0 * jnp.minimum(jnp.where(edge_key >= 0, swap_line, 0.0), 15.0),
        swap - swap_line * LANES,
    )
    key_value = jnp.where(valid & (spot < LANES), bucket, -1).astype(F32)
    bucket_cells = cells(buckets, step * LANES)
    total = jnp.zeros((FAST * buckets, LANES), F32)
    for i in range(0, lines, step):
        here = bucket_cells == bf(wide(key_value, i))
        stack = jnp.concatenate([jnp.where(here, bf(wide(v, i)), zero) for v in values], axis=0)
        place = jnp.where(lane_cells == bf(jnp.minimum(wide(spot, i), 255.0)), one, zero)
        total = total + nt_dot(stack, place)
    for f in range(FAST):
        plan_ref[f] = total[f * buckets : (f + 1) * buckets, :]

    sent = slabs * geo.quarter

    def position(rank, source, use):
        quarter = jnp.floor((rank + 0.5) * (1.0 / geo.quarter))
        place = quarter * sent + source.astype(F32) * geo.quarter + (rank - quarter * geo.quarter)
        return jnp.where(use, place, 4.0 * sent + 8.0)

    here_slot = slot_of - me * owned
    owned_lines = owned // LANES
    slot_line = jnp.where(owner == me, here_slot >> 7, -1).astype(F32)
    slot_lane = (here_slot & 127).astype(F32)
    fields = []
    for place in (position(recv1, home, owner == me), position(recv2, home + 1, edge)):
        high = jnp.floor(place * (1.0 / 64.0))
        fields += [high, place - 64.0 * high]
    slot_cells = cells(owned_lines, step * LANES)
    pad = -(4 * owned_lines) % 16
    placed = jnp.zeros((4 * owned_lines + pad, LANES), F32)
    for i in range(0, lines, step):
        here = jnp.broadcast_to(wide(slot_line, i), (owned_lines, step * LANES)) == iota((owned_lines, step * LANES), 0).astype(F32)
        stack = [jnp.where(here, wide(v, i), 0.0) for v in fields]
        if pad:
            stack.append(jnp.zeros((pad, step * LANES), F32))
        place = jnp.where(lane_cells == bf(wide(slot_lane, i)), one, zero)
        placed = placed + nt_dot(bf(jnp.concatenate(stack, axis=0)), place)
    for f in range(2):
        at = 2 * f * owned_lines
        slot_ref[f] = placed[at : at + owned_lines] * 64.0 + placed[at + owned_lines : at + 2 * owned_lines]

    depth = geo.rows * geo.probes
    spill = None
    batch = loads // 2
    for g in reversed(range(rounds)):
        for j in range(loads):
            load(g, j).wait()
        group = list(reversed(range(g * batch, (g + 1) * batch)))
        parts = []
        for b in group:
            block = jnp.concatenate([tiles[2 * b].reshape(depth, LANES), tiles[2 * b + 1].reshape(depth, LANES)], axis=1)
            parts.append(jnp.dot(block, bucket_table(plan_ref, b), preferred_element_type=F32))
        for b, part in zip(group, parts):
            value = part[:, :LANES]
            if spill is not None:
                value = value + spill
            spill = part[:, LANES:]
            fold[b] = value
            terms = [fold[b, pl.ds(k, geo.probes, stride=geo.rows), :] * x for k, x in enumerate(row_weights(geo, plan_ref, b))]
            value_ref[b] = functools.reduce(jnp.add, terms)


def bucket_table(plan_ref, b):
    near, low, high = (plan_ref[f, pl.ds(b, 1), :] for f in range(3))
    grid = cells(COLS, LANES)
    zero = jnp.zeros((), BF16)
    main = jnp.where(grid == bf(near), bf(low), jnp.where(grid == bf(near + 1.0), bf(high), zero))
    if isinstance(b, int) and b == 0:
        return jnp.concatenate([main, jnp.zeros((COLS, LANES), BF16)], axis=1)
    before = b - 1 if isinstance(b, int) else jnp.maximum(b - 1, 0)
    last, spill = (plan_ref[f, pl.ds(before, 1), :] for f in (0, 2))
    spill = jnp.where(last == COLS - 1.0, spill, 0.0)
    over = bf(jnp.where(iota((16, LANES), 0) == 0, spill, 0.0))
    over = jnp.concatenate([over, jnp.zeros((COLS - 16, LANES), BF16)], axis=0)
    return jnp.concatenate([main, over], axis=1)


def place_code(plan_ref, b):
    code = plan_ref[7, pl.ds(b, 1), :]
    owner = jnp.floor(code * 0.125)
    return owner, code - 8.0 * owner


def row_weights(geo, plan_ref, b):
    rf = plan_ref[3, pl.ds(b, 1), :] + plan_ref[4, pl.ds(b, 1), :]
    _, rel = place_code(plan_ref, b)
    return [jnp.where(rel == k + 2.0, 1.0 - rf, jnp.where(rel == k + 1.0, rf, 0.0)) for k in range(geo.rows)]


def exchange_kernel(geo, r_ref, c_ref, rf_ref, cf_ref, w_ref, order_ref, field_ref, adjoint_ref, arrived_ref, slot_ref, total_ref, ok_ref, plan_ref, flag_ref, value_ref, tiles, hots, ranks, fold, edges, places, shares, inbox, packed, sources, raised, traces, sums, load_sem, swap_send, swap_recv, owner_send, owner_recv, trace_send, trace_recv, sum_send, sum_recv):
    slabs, groups, probes, rows, quarter, buckets = geo.slabs, geo.groups, geo.probes, geo.rows, geo.quarter, geo.buckets
    me, mine = lax.axis_index("slab"), lax.axis_index("probe")
    lines = geo.edge_lines
    zero = jnp.zeros((), BF16)
    batch = 8

    def at(slab, probe):
        return dict(device_id=(slab, probe), device_id_type=pl.DeviceIdType.MESH)

    barrier = pltpu.get_barrier_semaphore()
    for k in range(1, slabs):
        pl.semaphore_signal(barrier, inc=1, **at(lax.rem(me + k, slabs), mine))
    for k in range(1, groups):
        pl.semaphore_signal(barrier, inc=1, **at(me, lax.rem(mine + k, groups)))

    observe(geo, me, r_ref, c_ref, rf_ref, cf_ref, w_ref, order_ref, field_ref, plan_ref, slot_ref, flag_ref, value_ref, tiles, hots, ranks, fold, load_sem)

    def columns(j):
        return slice(j * LANES, (j + 1) * LANES)

    def edge_fields(b):
        _, rel = place_code(plan_ref, b)
        line = jnp.floor(plan_ref[9, pl.ds(b, 1), :] * (1.0 / 16.0))
        lane = plan_ref[10, pl.ds(b, 1), :]
        return rel, line, lane

    def weight_of(b):
        return plan_ref[5, pl.ds(b, 1), :] + plan_ref[6, pl.ds(b, 1), :]

    share_rows = shares.shape[0]

    @pl.when(me == 0)
    def _():
        inbox[0] = jnp.zeros_like(inbox[0])

    @pl.when(me == slabs - 1)
    def _():
        inbox[1] = jnp.zeros_like(inbox[1])

    found = None
    for g in range(buckets // batch):
        stacks, spots = [], []
        for j in range(batch):
            b = g * batch + j
            rel, line, lane = edge_fields(b)
            low, high = rel == 1.0, rel == rows + 1.0
            spot = match(2 * LANES, jnp.where(low, lane, jnp.where(high, lane + LANES, -1.0)))
            value = value_ref[b]
            share = jnp.where((iota((share_rows, LANES), 0).astype(F32) == line) & high, weight_of(b), 0.0)
            stacks.append(jnp.concatenate([bf(jnp.where(line == float(l), value, 0.0)) for l in range(lines)] + [bf(share)], axis=0))
            spots.append(spot)
            places[b] = spot
        part = nt_dot(jnp.concatenate(stacks, axis=1), jnp.concatenate(spots, axis=1))
        found = part if found is None else found + part
    for side in range(2):
        edges[side] = found[: lines * probes, columns(side)]
    shares[...] = found[lines * probes :, columns(1)]

    pl.semaphore_wait(barrier, slabs + groups - 2)
    down, up = lax.rem(me + slabs - 1, slabs), lax.rem(me + 1, slabs)
    swaps = [
        pltpu.make_async_remote_copy(
            src_ref=edges.at[side], dst_ref=inbox.at[1 - side], send_sem=swap_send.at[side], recv_sem=swap_recv.at[side], **at(peer, mine)
        )
        for side, peer in ((0, down), (1, up))
    ]
    ends = (me > 0, me < slabs - 1)
    for side, copy in enumerate(swaps):
        pl.when(ends[side])(copy.start)

    packed[...] = jnp.zeros_like(packed)

    def pack(g, squares):
        hots, quads = [], []
        for j in range(batch):
            b = g * batch + j
            owner, rel = place_code(plan_ref, b)
            code = plan_ref[9, pl.ds(b, 1), :]
            fourth = code - 16.0 * jnp.floor(code * (1.0 / 16.0))
            row = jnp.where(rel > 0.0, owner * quarter + plan_ref[8, pl.ds(b, 1), :], -1.0)
            hots.append(match(slabs * quarter, row))
            value = value_ref[b]
            squares = squares + value * value * weight_of(b)
            quads.append(jnp.concatenate([bf(jnp.where(fourth == float(k), value, 0.0)) for k in range(4)], axis=0))
        part = nt_dot(jnp.concatenate(hots, axis=1), jnp.concatenate(quads, axis=1))
        packed[...] += part.reshape(packed.shape)
        return squares

    squares = lax.fori_loop(0, buckets // batch, pack, jnp.zeros((probes, LANES), F32))

    def owner_copy(k, source, peer):
        return pltpu.make_async_remote_copy(
            src_ref=packed.at[peer], dst_ref=arrived_ref.at[source], send_sem=owner_send.at[k], recv_sem=owner_recv.at[k], **at(peer, mine)
        )

    arrived_ref[me] = packed[me]

    for side, copy in enumerate(swaps):
        pl.when(ends[side])(copy.wait_send)
        pl.when(ends[1 - side])(copy.wait_recv)
    for l in range(lines):
        part = slice(l * probes, (l + 1) * probes)
        squares = squares + edges[1, part] * inbox[1, part] * (2.0 * shares[l : l + 1])
    folded = squares[:8]
    for d in range(8, probes, 8):
        folded = folded + squares[d : d + 8]
    traces[mine] = jnp.where(flag_ref[:1] > 0.0, jnp.inf, jnp.sum(folded, axis=0, keepdims=True))

    def trace_copy(k, source, peer):
        return pltpu.make_async_remote_copy(
            src_ref=traces.at[mine], dst_ref=traces.at[source], send_sem=trace_send.at[k], recv_sem=trace_recv.at[k], **at(me, peer)
        )

    for k in range(1, groups):
        trace_copy(k, mine, lax.rem(mine + k, groups)).start()

    for k in range(1, slabs):
        owner_copy(k, me, lax.rem(me + k, slabs)).start()
    both = bf(jnp.concatenate([inbox[0], inbox[1]], axis=1))
    sources[0] = jnp.zeros_like(sources[0])

    @pl.loop(0, buckets // batch)
    def _(g):
        spots = jnp.concatenate([places[g * batch + j] for j in range(batch)], axis=1)
        extra = jnp.dot(both, spots, preferred_element_type=F32)
        for j in range(batch):
            b = g * batch + j
            _, line, _ = edge_fields(b)
            full = value_ref[b]
            for l in range(lines):
                full = full + jnp.where(line == float(l), extra[l * probes : (l + 1) * probes, columns(j)], 0.0)
            spread = full * weight_of(b)
            for k, weight in enumerate(row_weights(geo, plan_ref, b)):
                raised[j, pl.ds(k, probes, stride=rows), :] = spread * weight
            sources[b + 1] = bf(raised[j])

    def spread_back(g):
        parts = []
        for j in range(batch):
            b = g * batch + j
            source = jnp.concatenate([sources[b + 1], sources[b]], axis=1)
            parts.append(nt_dot(source, bucket_table(plan_ref, b)))
        for j in range(batch):
            for t in range(2):
                adjoint_ref[2 * (g * batch + j) + t] = bf(parts[j][:, columns(t)]).reshape(probes, rows, LANES)

    rounds = buckets // batch
    early = max(1, rounds * EARLY // 4)
    pl.loop(0, early)(spread_back)
    for k in range(1, groups):
        source = lax.rem(mine + groups - k, groups)
        trace_copy(k, source, source).wait()
    sums[me] = jnp.sum(traces[...], axis=0)

    def sum_copy(k, source, peer):
        return pltpu.make_async_remote_copy(
            src_ref=sums.at[me], dst_ref=sums.at[source], send_sem=sum_send.at[k], recv_sem=sum_recv.at[k], **at(peer, mine)
        )

    for k in range(1, slabs):
        sum_copy(k, me, lax.rem(me + k, slabs)).start()

    if early < rounds:
        pl.loop(early, rounds)(spread_back)
    for k in range(1, slabs):
        source = lax.rem(me + slabs - k, slabs)
        owner_copy(k, source, source).wait()
    for k in range(1, slabs):
        source = lax.rem(me + slabs - k, slabs)
        sum_copy(k, source, source).wait()
    total = jnp.sum(sums[...], axis=0)
    total_ref[...] = total
    ok_ref[0] = jnp.max(jnp.where(total < jnp.inf, 0.0, 1.0)).astype(jnp.int32)


def deliver_kernel(geo, scale, adjoint_ref, arrived_ref, slot_ref, total_ref, out_ref, observed_ref, mean_ref, observed, sem):
    slabs, probes, quarter, owned = geo.slabs, geo.probes, geo.quarter, geo.owned
    loads = 8

    def store(t):
        return pltpu.make_async_copy(adjoint_ref.at[t], out_ref.at[:, t], sem.at[0])

    for t in range(geo.tiles):
        store(t).start()
    sent = slabs * quarter
    arrived = jnp.transpose(arrived_ref[...].reshape(sent, 4 * probes))
    lines = owned // LANES
    spots = [jnp.concatenate([slot_ref[f, l : l + 1, :] for l in range(lines)], axis=1) for f in range(2)]
    total = jnp.zeros((probes, owned), F32)
    for k in range(4):
        hot = match(sent, spots[0] - float(k * sent)) + match(sent, spots[1] - float(k * sent))
        total = total + jnp.dot(bf(arrived[k * probes : (k + 1) * probes]), hot, preferred_element_type=F32)
    observed[...] = total
    pltpu.make_async_copy(observed, observed_ref, sem.at[1]).start()
    mean_ref[...] = jnp.broadcast_to(jnp.sum(total_ref[...], axis=1, keepdims=True) * scale, mean_ref.shape)
    pltpu.make_async_copy(observed, observed_ref, sem.at[1]).wait()
    for t in range(geo.tiles):
        store(t).wait()


def geometry(slabs, groups, probe_fields, sensors):
    probes, rows, width = probe_fields.shape
    most = min(sensors, 4 * sensors // slabs)
    quarter = -(-(most // slabs + 32) // 32) * 8
    edge_lines = -(-5 * most // (4 * rows * LANES))
    buckets = width // COLS
    return Geo(rows, probes, slabs, groups, buckets, width // LANES, sensors // LANES, sensors // slabs, quarter, edge_lines, buckets + 2 * slabs + 16)


def body(slab_count, probe_groups, probe_fields, *vectors):
    sensors = vectors[0].shape[0]
    geo = geometry(slab_count, probe_groups, probe_fields, sensors)
    probes, rows, width = probe_fields.shape
    depth = probes * rows
    lines, buckets, tiles = geo.lines, geo.buckets, geo.tiles
    boxed = [x.reshape(lines, LANES) for x in vectors]
    field = probe_fields.reshape(probes, rows, tiles, LANES).transpose(0, 2, 1, 3)
    vmem = pl.BlockSpec(memory_space=VMEM)
    smem = pl.BlockSpec(memory_space=SMEM)
    hbm = pl.BlockSpec(memory_space=pltpu.HBM)
    dma = pltpu.SemaphoreType.DMA
    shape = jax.ShapeDtypeStruct
    edge_rows = geo.edge_lines * probes
    adjoint, arrived, slots, total, flag = pl.pallas_call(
        functools.partial(exchange_kernel, geo),
        out_shape=(
            shape((tiles, probes, rows, LANES), BF16),
            shape((slab_count, geo.quarter, 4 * probes), F32),
            shape((2, geo.owned // LANES, LANES), F32),
            shape((1, LANES), F32),
            shape((1,), jnp.int32),
        ),
        in_specs=[vmem] * 6 + [hbm],
        out_specs=(vmem, vmem, vmem, vmem, smem),
        scratch_shapes=[
            VMEM((FAST, buckets, LANES), F32),
            VMEM((8, LANES), F32),
            VMEM((buckets, probes, LANES), F32),
            VMEM((tiles, probes, rows, LANES), BF16),
            VMEM((lines * geo.kinds, LANES), BF16),
            VMEM((5, lines, LANES), F32),
            VMEM((buckets, depth, LANES), F32),
            VMEM((2, edge_rows, LANES), F32),
            VMEM((buckets, 2 * LANES, LANES), BF16),
            VMEM((-(-geo.edge_lines // 16) * 16, LANES), F32),
            VMEM((2, edge_rows, LANES), F32),
            VMEM((slab_count, geo.quarter, 4 * probes), F32),
            VMEM((buckets + 1, depth, LANES), BF16),
            VMEM((8, depth, LANES), F32),
            VMEM((probe_groups, 1, LANES), F32),
            VMEM((slab_count, 1, LANES), F32),
            dma((tiles // 8,)),
            dma((2,)),
            dma((2,)),
            dma((slab_count,)),
            dma((slab_count,)),
            dma((probe_groups,)),
            dma((probe_groups,)),
            dma((slab_count,)),
            dma((slab_count,)),
        ],
        compiler_params=pltpu.CompilerParams(collective_id=3, has_side_effects=True, vmem_limit_bytes=ROOM),
        name="exchange",
    )(*boxed, field)
    out, observed, mean = pl.pallas_call(
        functools.partial(deliver_kernel, geo, 1.0 / (probes * probe_groups * sensors)),
        out_shape=(
            shape((probes, tiles, rows, LANES), BF16),
            shape((probes, geo.owned), F32),
            shape((1, LANES), F32),
        ),
        in_specs=[vmem] * 4,
        out_specs=(hbm, hbm, vmem),
        scratch_shapes=[VMEM((probes, geo.owned), F32), dma((2,))],
        compiler_params=SMALL,
        name="deliver",
    )(adjoint, arrived, slots, total)
    out = out.transpose(0, 2, 1, 3).reshape(probes, rows, width)

    def again(state):
        out, observed, mean = general(slab_count, probe_groups, probe_fields, *vectors)
        return out, jnp.where(state[3] > 0, observed, state[1]), mean, state[3] * 0

    state = lax.while_loop(lambda state: state[3] != 0, again, (out, observed, mean[0, 0], flag[0]))
    return state[:3]


def solution(mesh):
    placed = (P("probe", "slab", None), P(), P(), P(), P(), P(), P())
    return jax.shard_map(
        functools.partial(body, mesh.shape["slab"], mesh.shape["probe"]),
        mesh=mesh,
        in_specs=placed,
        out_specs=(P("probe", "slab", None), P("probe", "slab"), P()),
        check_vma=False,
    )
```
